32 devices in a mesh: cp: 4 (over z), fsdp: 8 (over y, x, core).
Axes of the slice: x: 2, y: 2, z: 4, core: 2. Of those that a mesh axis runs over, the one named last changes fastest.
Arguments:
- tokens: int32 [256, 256], P('fsdp', 'cp')
- lengths: int32 [256], P('fsdp')
- embed_table: bfloat16 [33, 320], replicated
- layer_vecs: float32 [9, 320], P(None, 'fsdp')
- w_qkv: bfloat16 [320, 3, 20, 16], P('fsdp')
- w_out: bfloat16 [320, 320], P('fsdp')
- w_up: bfloat16 [320, 1280], P('fsdp')
- b_up: float32 [1280], P('fsdp')
- w_down: bfloat16 [1280, 320], P('fsdp')
- grad_out: bfloat16 [256, 256, 320], P('fsdp', 'cp')
Outputs:
- output 1: bfloat16 [256, 256, 320], P('fsdp', 'cp')
- output 2: float32 [33, 320], replicated
- output 3: float32 [9, 320], P(None, 'fsdp')
- output 4: float32 [320, 3, 20, 16], P('fsdp')
- output 5: float32 [320, 320], P('fsdp')
- output 6: float32 [320, 1280], P('fsdp')
- output 7: float32 [1280], P('fsdp')
- output 8: float32 [1280, 320], P('fsdp')
All inputs are finite; a program needn't handle non-finite values.
Results may differ from the reference program's by a relative error of at most 0.0103739.
Values are sent between devices in bfloat16 or wider.
A program may use at most 1 GiB of HBM per device.

```python
import jax
import jax.numpy as jnp
from jax import lax

NUM_SEQS = 256
SEQ_LEN = 256
MODEL_DIM = 320
NUM_HEADS = 20
FFN_DIM = 1280
VOCAB_SIZE = 33
BOS_ID = 0
PAD_ID = 1
EOS_ID = 2
MASK_ID = 32
HEAD_DIM = MODEL_DIM // NUM_HEADS
LN_EPS = 1e-5
ROPE_BASE = 10000.0
TRAIN_RATIO = 0.15 * 0.8
NEG_BIG = -1e30


def draw_tokens(rng_key):
    key_list = jax.random.split(rng_key, 4)
    lengths = jax.random.randint(key_list[0], (NUM_SEQS,), SEQ_LEN // 4, SEQ_LEN + 1)
    lengths = lengths.at[0].set(SEQ_LEN).at[1].set(SEQ_LEN // 4)
    positions = jnp.arange(SEQ_LEN)[None, :]
    len_col = lengths[:, None]
    residues = jax.random.randint(key_list[1], (NUM_SEQS, SEQ_LEN), 4, 31)
    win_start = jax.random.randint(key_list[2], (NUM_SEQS, 1), 0, SEQ_LEN)
    in_win = (positions >= win_start) & (positions < win_start + SEQ_LEN // 4)
    hit_draw = jax.random.randint(key_list[3], (NUM_SEQS, SEQ_LEN), 0, 100)
    is_mask = hit_draw < jnp.where(in_win, 45, 5)
    tokens = jnp.where(is_mask, MASK_ID, residues)
    tokens = jnp.where(positions >= len_col, PAD_ID, tokens)
    tokens = jnp.where(positions == len_col - 1, EOS_ID, tokens)
    tokens = jnp.where(positions == 0, BOS_ID, tokens)
    return tokens.astype(jnp.int32), lengths.astype(jnp.int32)


def setup_inputs(seed: int = 0) -> dict:
    key_list = jax.random.split(jax.random.key(seed), 9)
    tokens, lengths = draw_tokens(key_list[0])
    embed_table = jax.random.normal(key_list[1], (VOCAB_SIZE, MODEL_DIM), jnp.float32)
    row_scale = jnp.array([0.2, 0.3, 0.3, 0.3, SEQ_LEN ** -0.5, 0.3, 0.2, 0.3, 0.3], jnp.float32)
    row_shift = jnp.array([1.0, 0.0, 0.0, 0.0, 0.0, 0.0, 1.0, 0.0, 0.0], jnp.float32)
    layer_vecs = row_shift[:, None] + row_scale[:, None] * jax.random.normal(key_list[2], (9, MODEL_DIM), jnp.float32)
    w_qkv = jax.random.normal(key_list[3], (MODEL_DIM, 3, NUM_HEADS, HEAD_DIM), jnp.float32) * MODEL_DIM ** -0.5
    w_out = jax.random.normal(key_list[4], (MODEL_DIM, MODEL_DIM), jnp.float32) * (SEQ_LEN / (2.0 * MODEL_DIM)) ** 0.5
    w_up = jax.random.normal(key_list[5], (MODEL_DIM, FFN_DIM), jnp.float32) * MODEL_DIM ** -0.5
    b_up = 0.5 * jax.random.normal(key_list[6], (FFN_DIM,), jnp.float32)
    w_down = jax.random.normal(key_list[7], (FFN_DIM, MODEL_DIM), jnp.float32) * FFN_DIM ** -0.5
    grad_out = jax.random.normal(key_list[8], (NUM_SEQS, SEQ_LEN, MODEL_DIM), jnp.float32)
    return {
        'tokens': tokens,
        'lengths': lengths,
        'embed_table': embed_table.astype(jnp.bfloat16),
        'layer_vecs': layer_vecs,
        'w_qkv': w_qkv.astype(jnp.bfloat16),
        'w_out': w_out.astype(jnp.bfloat16),
        'w_up': w_up.astype(jnp.bfloat16),
        'b_up': b_up,
        'w_down': w_down.astype(jnp.bfloat16),
        'grad_out': grad_out.astype(jnp.bfloat16),
    }


def rounded(z_in):
    return z_in + lax.stop_gradient(z_in.astype(jnp.bfloat16).astype(jnp.float32) - z_in)


def layer_norm(z_in, ln_gain, ln_bias):
    row_mean = jnp.mean(z_in, axis=-1, keepdims=True)
    centered = z_in - row_mean
    row_var = jnp.mean(centered * centered, axis=-1, keepdims=True)
    return centered * lax.rsqrt(row_var + LN_EPS) * ln_gain + ln_bias


def rotate(z_in, cos_t, sin_t):
    lower_half, upper_half = jnp.split(z_in, 2, axis=-1)
    return jnp.concatenate([lower_half * cos_t - upper_half * sin_t, upper_half * cos_t + lower_half * sin_t], axis=-1)


def one_sequence(params, embed_f32, tok_row, len_row):
    layer_vecs, w_qkv, w_out, w_up, b_up, w_down = params
    positions = jnp.arange(SEQ_LEN)
    is_mask = tok_row == MASK_ID
    key_valid = positions < len_row
    n_mask = jnp.sum(is_mask.astype(jnp.float32))
    drop_scale = (1.0 - TRAIN_RATIO) / (1.0 - n_mask / len_row.astype(jnp.float32))
    keep_scale = jnp.where(is_mask | jnp.logical_not(key_valid), 0.0, drop_scale)
    embedded = embed_f32[tok_row] * keep_scale[:, None]
    norm_in = rounded(layer_norm(embedded, layer_vecs[0], layer_vecs[1]))
    qkv_lin = jnp.dot(norm_in, w_qkv.reshape(MODEL_DIM, 3 * MODEL_DIM)) + layer_vecs[2:5].reshape(3 * MODEL_DIM)
    qkv_lin = qkv_lin.reshape(SEQ_LEN, 3, NUM_HEADS, HEAD_DIM)
    inv_freq = 1.0 / (ROPE_BASE ** (jnp.arange(0, HEAD_DIM, 2, dtype=jnp.float32) / HEAD_DIM))
    angles = positions.astype(jnp.float32)[:, None] * inv_freq[None, :]
    cos_t = jnp.cos(angles)[:, None, :]
    sin_t = jnp.sin(angles)[:, None, :]
    q_heads = rounded(rotate(qkv_lin[:, 0] * HEAD_DIM ** -0.5, cos_t, sin_t))
    k_heads = rounded(rotate(qkv_lin[:, 1], cos_t, sin_t))
    v_heads = rounded(qkv_lin[:, 2])

    def one_head(head_in):
        q_h, k_h, v_h = head_in
        scores = jnp.dot(q_h, k_h.T)
        scores = jnp.where(key_valid[None, :], scores, NEG_BIG)
        return jnp.dot(jax.nn.softmax(scores, axis=-1), v_h)

    per_head = lax.map(jax.checkpoint(one_head), (q_heads.transpose(1, 0, 2), k_heads.transpose(1, 0, 2), v_heads.transpose(1, 0, 2)))
    attn_out = rounded(per_head.transpose(1, 0, 2).reshape(SEQ_LEN, MODEL_DIM))
    resid_mid = embedded + jnp.dot(attn_out, w_out) + layer_vecs[5]
    norm_mid = rounded(layer_norm(resid_mid, layer_vecs[6], layer_vecs[7]))
    gelu_out = rounded(jax.nn.gelu(jnp.dot(norm_mid, w_up) + b_up, approximate=False))
    return resid_mid + jnp.dot(gelu_out, w_down) + layer_vecs[8]


def reference(tokens, lengths, embed_table, layer_vecs, w_qkv, w_out, w_up, b_up, w_down, grad_out):
    params = (layer_vecs, w_qkv.astype(jnp.float32), w_out.astype(jnp.float32), w_up.astype(jnp.float32), b_up, w_down.astype(jnp.float32))
    seq_fn = jax.checkpoint(one_sequence)

    def forward(params_in, embed_f32):
        def per_row(seq_row):
            return seq_fn(params_in, embed_f32, seq_row[0], seq_row[1])
        return lax.map(per_row, (tokens, lengths))

    layer_out, pullback = jax.vjp(forward, params, embed_table.astype(jnp.float32))
    d_params, d_embed = pullback(grad_out.astype(jnp.float32))
    return (layer_out.astype(jnp.bfloat16), d_embed, d_params[0], d_params[1], d_params[2], d_params[3], d_params[4], d_params[5])
```

```python
import functools

import jax
import jax.numpy as jnp
from jax import lax
from jax.experimental import pallas as pl
from jax.experimental.pallas import tpu as pltpu
from jax.sharding import PartitionSpec as P

MASK_ID = 32
LN_EPS = 1e-5
ROPE_BASE = 10000.0
TRAIN_RATIO = 0.15 * 0.8
NEG_BIG = -1e30
VOCAB_PAD = 128
HEAD_DIM = 16
N_HEADS = 20
D = 320
F = 1280
SEQ = 256
LANES = 128
HEADS_PER_TILE = LANES // HEAD_DIM
N_TILES = -(-D // LANES)
HEAD_UNROLL = 4
QKV_HALF = 512
UO_PAD = 1664
SM_ROWS = 16
BF = jnp.bfloat16
F32 = jnp.float32
SQRT_HALF = 0.7071067811865476
INV_SQRT_2PI = 0.3989422804014327

NN = (((1,), (0,)), ((), ()))
NT = (((1,), (1,)), ((), ()))


def dot(a, b, dims=NN):
    return lax.dot_general(a, b, dims, preferred_element_type=F32)


def col(vecs_t, j):
    return vecs_t[:, j:j + 1]


def rope(z, cos_t, sin_t):
    z4 = z.reshape(N_HEADS, 2, HEAD_DIM // 2, SEQ)
    lower, upper = z4[:, 0], z4[:, 1]
    new_l = lower * cos_t - upper * sin_t
    new_u = upper * cos_t + lower * sin_t
    return jnp.stack([new_l, new_u], axis=1).reshape(D, SEQ)


def key_bias(shift_base, cp_size, seq_loc, length):
    row = lax.broadcasted_iota(jnp.int32, (SEQ, SEQ), 0)
    src = (shift_base - row // seq_loc + cp_size) % cp_size
    pos = src * seq_loc + row % seq_loc
    return jnp.where(pos < length, 0.0, NEG_BIG).astype(F32)


def store_token_major(dst_ref, z_t):
    for t in range(N_TILES):
        lo = t * LANES
        hi = min(lo + LANES, D)
        part = z_t[lo:hi]
        if hi - lo < LANES:
            part = jnp.concatenate([part, jnp.zeros((LANES - (hi - lo), z_t.shape[1]), F32)], axis=0)
        dst_ref[t] = part.T.astype(BF)


def head_rows(tile, slot):
    row = lax.broadcasted_iota(jnp.int32, tile.shape, 0)
    return jnp.where(row // HEAD_DIM == slot, tile, jnp.zeros_like(tile))


def token_scale(tok, length, seq_loc, cp_size, me):
    lane = lax.broadcasted_iota(jnp.int32, (1, SEQ), 1)
    src = (me - lane // seq_loc + cp_size) % cp_size
    pos = src * seq_loc + lane % seq_loc
    is_mask = tok == MASK_ID
    n_mask = jnp.sum(is_mask.astype(F32), axis=1, keepdims=True)
    drop = (1.0 - TRAIN_RATIO) / (1.0 - n_mask / length.astype(F32))
    return jnp.where(is_mask | (pos >= length), 0.0, drop)


def one_hot_rows(tok):
    row = lax.broadcasted_iota(jnp.int32, (VOCAB_PAD, SEQ), 0)
    return jnp.where(row == tok, 1.0, 0.0).astype(BF)


def join_rows(ref):
    return jnp.concatenate([ref[i].astype(F32) for i in range(ref.shape[0])], axis=0).astype(BF)


def wide(z):
    return jnp.concatenate([z, z], axis=1)


def fwd_kernel(cp_size, seq_loc, len_ref, me_ref, tok_ref, emb_ref, sm_ref, wqkv_ref, wout_ref, wup_ref, wdown_ref, cos_ref, sin_ref,
               o0_ref, o1_ref, o2_ref, o3_ref, h_ref, xhat1_ref, stat_ref, qkv_ref, lse_ref, attn_ref, xhat2_ref, a_ref, gelu_ref, dgelu_ref, gain_ref, wqkv_n, wout_n, wup_n,
               wqkv_t, wout_t, wup_t, wdown_t, k_tm, q_pad, bias, vec_b, bup_b):
    step = pl.program_id(0)

    @pl.when(step == 0)
    def _():
        for src, nat, tr in ((wqkv_ref, wqkv_n, wqkv_t), (wout_ref, wout_n, wout_t), (wup_ref, wup_n, wup_t)):
            joined = join_rows(src)
            nat[...] = joined
            tr[...] = joined.T
        wdown_t[...] = wdown_ref[...].T
        q_pad[...] = jnp.zeros_like(q_pad)
        pieces = sm_ref.shape[0]
        rows = D // pieces
        for i in range(pieces):
            sm_t = sm_ref[i].T
            gain_ref[i * rows:(i + 1) * rows] = sm_t[:rows]
            for j in range(9):
                vec_b[j, i * rows:(i + 1) * rows] = jnp.broadcast_to(sm_t[:rows, j:j + 1], (rows, LANES))
            for r in range(F // D):
                lo = i * (F // pieces) + r * rows
                bup_b[lo:lo + rows] = jnp.broadcast_to(sm_t[:rows, 9 + r:10 + r], (rows, LANES))

    length = len_ref[step]
    me = me_ref[0]
    tok = tok_ref[0]
    keep = token_scale(tok, length, seq_loc, cp_size, me)
    e = dot(emb_ref[...], one_hot_rows(tok)) * keep
    mean = jnp.mean(e, axis=0, keepdims=True)
    cent = e - mean
    var = jnp.mean(cent * cent, axis=0, keepdims=True)
    rstd1 = lax.rsqrt(var + LN_EPS)
    xhat1 = cent * rstd1
    xhat1_ref[0] = xhat1
    h = (xhat1 * wide(vec_b[0]) + wide(vec_b[1])).astype(BF)
    h_ref[0] = h
    cos_t, sin_t = cos_ref[...], sin_ref[...]
    q = (dot(wqkv_t[0:D], h) + wide(vec_b[2])) * HEAD_DIM ** -0.5
    q = rope(q, cos_t, sin_t).astype(BF)
    qkv_ref[0, 0:D] = q
    q_pad[0:D] = q
    k = rope(dot(wqkv_t[D:2 * D], h) + wide(vec_b[3]), cos_t, sin_t)
    qkv_ref[0, D:2 * D] = k.astype(BF)
    store_token_major(k_tm, k)
    qkv_ref[0, 2 * D:3 * D] = (dot(wqkv_t[2 * D:3 * D], h) + wide(vec_b[4])).astype(BF)
    bias[...] = key_bias(me, cp_size, seq_loc, length)

    def head_body(it, _):
        for u in range(HEAD_UNROLL):
            hd = it * HEAD_UNROLL + u
            tile = hd // HEADS_PER_TILE
            slot = hd % HEADS_PER_TILE
            q_t = q_pad[pl.ds(pl.multiple_of(tile * LANES, LANES), LANES), :]
            s = dot(k_tm[tile], head_rows(q_t, slot)) + bias[...]
            m = jnp.max(s, axis=0, keepdims=True)
            p = jnp.exp(s - m)
            l = jnp.sum(p, axis=0, keepdims=True)
            r0 = pl.multiple_of(hd * HEAD_DIM, HEAD_DIM)
            v_h = qkv_ref[0, pl.ds(pl.multiple_of(2 * D + hd * HEAD_DIM, HEAD_DIM), HEAD_DIM), :]
            attn_ref[0, pl.ds(r0, HEAD_DIM), :] = dot(v_h, p.astype(BF)) / l
            lse_ref[0, hd] = m + jnp.log(l)
        return 0

    lax.fori_loop(0, N_HEADS // HEAD_UNROLL, head_body, 0)

    o = attn_ref[0].astype(BF)
    x1 = e + dot(wout_t[...], o) + wide(vec_b[5])
    mean2 = jnp.mean(x1, axis=0, keepdims=True)
    cent2 = x1 - mean2
    var2 = jnp.mean(cent2 * cent2, axis=0, keepdims=True)
    rstd2 = lax.rsqrt(var2 + LN_EPS)
    xhat2 = cent2 * rstd2
    xhat2_ref[0] = xhat2
    a = (xhat2 * wide(vec_b[6]) + wide(vec_b[7])).astype(BF)
    a_ref[0] = a
    stat_ref[0] = jnp.concatenate([rstd1, rstd2, keep, jnp.zeros((5, SEQ), F32)], axis=0)
    out = x1 + wide(vec_b[8])
    for c in range(F // D):
        rows = slice(c * D, (c + 1) * D)
        u = dot(wup_t[rows], a) + wide(bup_b[rows])
        cdf = 0.5 * (1.0 + lax.erf(u * SQRT_HALF))
        g = (u * cdf).astype(BF)
        gelu_ref[0, rows] = g
        dgelu_ref[0, rows] = cdf + u * (INV_SQRT_2PI * jnp.exp(-0.5 * u * u))
    out = out + dot(wdown_t[...], gelu_ref[0])
    out_tm = to_token_major(out)
    for k_i, o_ref in enumerate((o0_ref, o1_ref, o2_ref, o3_ref)):
        o_ref[0] = out_tm[k_i * seq_loc:(k_i + 1) * seq_loc]


def to_token_major(z_t):
    parts = []
    for t in range(N_TILES):
        lo, hi = t * LANES, min((t + 1) * LANES, D)
        part = z_t[lo:hi]
        if hi - lo < LANES:
            part = jnp.concatenate([part, jnp.zeros((LANES - (hi - lo), SEQ), F32)], axis=0)
        parts.append(part.T.astype(BF))
    return jnp.concatenate(parts, axis=1)[:, :D]


def to_feature_major(z):
    z32 = z.astype(F32)
    pad = jnp.concatenate([z32, jnp.zeros((SEQ, N_TILES * LANES - D), F32)], axis=1)
    return jnp.concatenate([pad[:, t * LANES:(t + 1) * LANES].T for t in range(N_TILES)], axis=0)[:D]


def lane_part(z):
    return z[:, :LANES] + z[:, LANES:]


def ln_grad(dn, xhat, rstd, gain):
    dxh = dn * gain
    m1 = jnp.mean(dxh, axis=0, keepdims=True)
    m2 = jnp.mean(dxh * xhat, axis=0, keepdims=True)
    return rstd * (dxh - m1 - xhat * m2)


def row_sum(acc):
    return jnp.sum(acc.T, axis=0, keepdims=True)


def ffn_bwd_kernel(n_steps, seq_loc, g0_ref, g1_ref, g2_ref, g3_ref, vec_ref, wdown_ref, wup_ref, wout_ref, gelu_ref, dgelu_ref, a_ref, xhat2_ref, stat_ref, attn_ref,
                   dres_ref, dattn_ref, dwdown_ref, dwuo_ref, dbup_ref, dvec_ref,
                   acc_bup, acc_vec):
    step = pl.program_id(0)

    @pl.when(step == 0)
    def _():
        dwdown_ref[...] = jnp.zeros_like(dwdown_ref)
        dwuo_ref[...] = jnp.zeros_like(dwuo_ref)
        acc_bup[...] = jnp.zeros_like(acc_bup)
        acc_vec[...] = jnp.zeros_like(acc_vec)

    vecs = vec_ref[...]
    g = jnp.concatenate([g0_ref[0], g1_ref[0], g2_ref[0], g3_ref[0]], axis=0)
    g_t = to_feature_major(g)
    a = a_ref[0]
    dn2 = jnp.zeros((D, SEQ), F32)
    dup_parts = []
    for c in range(F // D):
        rows = slice(c * D, (c + 1) * D)
        dup = dot(wdown_ref[rows], g, NT) * dgelu_ref[0, rows]
        acc_bup[rows] += lane_part(dup)
        dup_parts.append(dup.astype(BF))
        dwdown_ref[rows] += dot(gelu_ref[0, rows], g)
    dup_b = jnp.concatenate(dup_parts, axis=0)
    dwuo_ref[:, 0:F] += dot(a, dup_b, NT)
    dn2 = dot(wup_ref[...], dup_b)
    xhat2 = xhat2_ref[0]
    rstd2 = stat_ref[0, 1:2]
    dres = g_t + ln_grad(dn2, xhat2, rstd2, col(vecs, 6))
    acc_vec[0] += lane_part(dres)
    acc_vec[1] += lane_part(dn2 * xhat2)
    acc_vec[2] += lane_part(dn2)
    acc_vec[3] += lane_part(g_t)
    dres_ref[0] = dres
    dres_b = dres.astype(BF)
    dwuo_ref[:, F:F + D] += dot(attn_ref[0].astype(BF), dres_b, NT)
    dattn_ref[0] = dot(wout_ref[...], dres_b)

    @pl.when(step == n_steps - 1)
    def _():
        dbup_ref[...] = row_sum(acc_bup[...])
        dvec_ref[...] = jnp.concatenate([row_sum(pad_rows(acc_vec[j])) for j in range(4)] + [jnp.zeros((4, N_TILES * LANES), F32)], axis=0)


def pad_rows(z):
    return jnp.concatenate([z, jnp.zeros((N_TILES * LANES - D, LANES), F32)], axis=0)


def attn_bwd_kernel(n_steps, cp_size, seq_loc, len_ref, me_ref, tok_ref, vec_ref, wqkv_ref, cos_ref, sin_ref, qkv_ref, lse_ref, attn_ref, dattn_ref, dres_ref, xhat1_ref, h_ref, stat_ref,
                    dwqa_ref, dwqb_ref, demb_ref, dvec_ref,
                    k_tm, v_tm, q_pad, do_pad, bias, dq_s, dk_s, dv_s, acc_b, acc_vec):
    step = pl.program_id(0)

    @pl.when(step == 0)
    def _():
        dwqa_ref[...] = jnp.zeros_like(dwqa_ref)
        dwqb_ref[...] = jnp.zeros_like(dwqb_ref)
        demb_ref[...] = jnp.zeros_like(demb_ref)
        acc_b[...] = jnp.zeros_like(acc_b)
        acc_vec[...] = jnp.zeros_like(acc_vec)
        q_pad[...] = jnp.zeros_like(q_pad)
        do_pad[...] = jnp.zeros_like(do_pad)

    length = len_ref[step]
    me = me_ref[0]
    vecs = vec_ref[...]
    q_pad[0:D] = qkv_ref[0, 0:D]
    do_pad[0:D] = dattn_ref[0].astype(BF)
    store_token_major(k_tm, qkv_ref[0, D:2 * D].astype(F32))
    store_token_major(v_tm, qkv_ref[0, 2 * D:3 * D].astype(F32))
    bias[...] = key_bias(me, cp_size, seq_loc, length)

    def head_body(it, _):
        for u in range(HEAD_UNROLL):
            hd = it * HEAD_UNROLL + u
            tile = hd // HEADS_PER_TILE
            slot = hd % HEADS_PER_TILE
            t0 = pl.ds(pl.multiple_of(tile * LANES, LANES), LANES)
            rows = pl.ds(pl.multiple_of(hd * HEAD_DIM, HEAD_DIM), HEAD_DIM)
            q_h = q_pad[rows, :]
            do_h = do_pad[rows, :]
            k_h = qkv_ref[0, pl.ds(pl.multiple_of(D + hd * HEAD_DIM, HEAD_DIM), HEAD_DIM), :]
            delta = jnp.sum(dattn_ref[0, rows, :] * attn_ref[0, rows, :], axis=0, keepdims=True)
            s = dot(k_tm[tile], head_rows(q_pad[t0, :], slot)) + bias[...]
            p = jnp.exp(s - lse_ref[0, hd])
            dp = dot(v_tm[tile], head_rows(do_pad[t0, :], slot))
            ds = (p * (dp - delta)).astype(BF)
            dq_s[rows, :] = dot(k_h, ds)
            dk_s[rows, :] = dot(q_h, ds, NT)
            dv_s[rows, :] = dot(do_h, p.astype(BF), NT)
        return 0

    lax.fori_loop(0, N_HEADS // HEAD_UNROLL, head_body, 0)

    cos_t, sin_t = cos_ref[...], sin_ref[...]
    h = h_ref[0]
    dq = rope(dq_s[...], cos_t, -sin_t) * HEAD_DIM ** -0.5
    dk = rope(dk_s[...], cos_t, -sin_t)
    dv = dv_s[...]
    dn1 = jnp.zeros((D, SEQ), F32)
    parts = []
    for j, dz in enumerate((dq, dk, dv)):
        acc_b[j] += lane_part(dz)
        parts.append(dz.astype(BF))
    dz_b = jnp.concatenate(parts, axis=0)
    dwqa_ref[...] += dot(h, dz_b[:QKV_HALF], NT)
    dwqb_ref[:, :3 * D - QKV_HALF] += dot(h, dz_b[QKV_HALF:], NT)
    dn1 = dot(wqkv_ref[...], dz_b)
    xhat1 = xhat1_ref[0]
    acc_vec[0] += lane_part(dn1 * xhat1)
    acc_vec[1] += lane_part(dn1)
    de = dres_ref[0] + ln_grad(dn1, xhat1, stat_ref[0, 0:1], col(vecs, 0))
    de = (de * stat_ref[0, 2:3]).astype(BF)
    demb_ref[...] += dot(one_hot_rows(tok_ref[0]), de, NT)

    @pl.when(step == n_steps - 1)
    def _():
        rows = [row_sum(pad_rows(acc_vec[j])) for j in range(2)] + [row_sum(pad_rows(acc_b[j])) for j in range(3)]
        dvec_ref[...] = jnp.concatenate(rows + [jnp.zeros((3, N_TILES * LANES), F32)], axis=0)


def per_seq(*shape):
    return pl.BlockSpec((1,) + shape, lambda b: (b,) + (0,) * len(shape))


def whole(*shape):
    return pl.BlockSpec(shape, lambda b: (0,) * len(shape))


SMEM = pl.BlockSpec(memory_space=pltpu.SMEM)


def sds(shape, dtype):
    return jax.ShapeDtypeStruct(shape, dtype)


def call(kernel, grid, in_specs, out_specs, out_shape, scratch, flops, name):
    return pl.pallas_call(
        kernel, grid=(grid,), in_specs=in_specs, out_specs=out_specs, out_shape=out_shape, scratch_shapes=scratch, name=name,
        cost_estimate=pl.CostEstimate(flops=flops, bytes_accessed=50_000_000, transcendentals=10_000_000),
        compiler_params=pltpu.CompilerParams(dimension_semantics=('arbitrary',), vmem_limit_bytes=58 * 1024 * 1024))


MESH = pl.DeviceIdType.MESH


def place(fs):
    return fs // 4, (fs // 2) % 2, fs % 2


def device(cp, fs):
    return {'cp': cp, 'fsdp': fs}


def enter(peers):
    barrier = pltpu.get_barrier_semaphore()
    for peer in peers:
        pl.semaphore_signal(barrier, inc=1, device_id=peer, device_id_type=MESH)
    pl.semaphore_wait(barrier, len(peers))


def remote(src, dst, send_sem, recv_sem, peer):
    return pltpu.make_async_remote_copy(src_ref=src, dst_ref=dst, send_sem=send_sem, recv_sem=recv_sem, device_id=peer, device_id_type=MESH)


def gather_kernel(cp_size, n_arr, *refs):
    ins, tok_in = refs[:n_arr], refs[n_arr]
    outs, tok_out = refs[n_arr + 1:2 * n_arr + 1], refs[2 * n_arr + 1]
    send, recv, tok_send, tok_recv = refs[2 * n_arr + 2:]
    me = lax.axis_index('cp')
    fs = lax.axis_index('fsdp')
    y, x, c = place(fs)
    near, xn, yn = fs + 1 - 2 * c, fs + 2 - 4 * x, fs + 4 - 8 * y
    dg = xn + 4 - 8 * y
    first = xn * (1 - c) + yn * c
    other = yn * (1 - c) + xn * c
    cps = [lax.rem(me + k, cp_size) for k in range(1, cp_size)]
    enter([device(me, near), device(me, xn), device(me, yn)] + [device(z, fs) for z in cps])

    sent = []

    def push(a, src, slot, peer, lane):
        copy = remote(src, outs[a].at[slot], send.at[a, lane], recv.at[a, slot], device(me, peer))
        copy.start()
        sent.append(copy)

    def arrived(a, slot):
        remote(ins[a], outs[a].at[slot], send.at[a, 0], recv.at[a, slot], device(me, near)).wait_recv()

    for k in range(1, cp_size):
        copy = remote(tok_in.at[cps[k - 1]], tok_out.at[k], tok_send.at[k], tok_recv.at[k], device(cps[k - 1], fs))
        copy.start()
        sent.append(copy)
    for a in range(n_arr):
        push(a, ins[a], fs, xn, 0)
        push(a, ins[a], fs, yn, 1)
        push(a, ins[a], fs, near, 2)
    for a in range(n_arr):
        outs[a][fs] = ins[a][...]
    tok_out[0] = tok_in[me]
    for a in range(n_arr):
        arrived(a, first)
        push(a, outs[a].at[first], first, other, 3)
        push(a, outs[a].at[first], first, near, 4)
    for a in range(n_arr):
        arrived(a, other)
        push(a, outs[a].at[other], other, near, 5)
    for a in range(n_arr):
        arrived(a, dg)
        push(a, outs[a].at[dg], dg, near, 6)
    for a in range(n_arr):
        arrived(a, near)
        for slot in (xn, yn, dg):
            arrived(a, slot + 1 - 2 * c)
    for k in range(1, cp_size):
        remote(tok_in.at[0], tok_out.at[k], tok_send.at[k], tok_recv.at[k], device(me, near)).wait_recv()
    for copy in sent:
        copy.wait_send()


def gather_call(cp_size, arrays, tok):
    n_arr = len(arrays)
    pieces = 8
    vmem = pl.BlockSpec(memory_space=pltpu.VMEM)
    dma = pltpu.SemaphoreType.DMA
    return pl.pallas_call(
        functools.partial(gather_kernel, cp_size, n_arr),
        out_shape=[sds((pieces,) + arr.shape, arr.dtype) for arr in arrays] + [sds(tok.shape, tok.dtype)],
        in_specs=[vmem] * (n_arr + 1), out_specs=[vmem] * (n_arr + 1),
        scratch_shapes=[dma((n_arr, 7)), dma((n_arr, pieces)), dma((cp_size,)), dma((cp_size,))],
        compiler_params=pltpu.CompilerParams(collective_id=0, has_side_effects=True, vmem_limit_bytes=48 * 1024 * 1024),
        name='gather',
    )(*arrays, tok)


def piece_of(ref, spec, p):
    axis, size, stride = spec
    start = pl.multiple_of(p * stride, stride)
    return ref.at[pl.ds(start, size), :] if axis == 0 else ref.at[:, pl.ds(start, size)]


def reduce_kernel(cp_size, specs, *refs):
    n = len(specs)
    big, small = refs[:n], refs[n]
    outs, small_out = refs[n + 1:2 * n + 1], refs[2 * n + 1]
    rest = refs[2 * n + 2:]
    r0, acc, r1, r2, rz, rg = (rest[i * n:(i + 1) * n] for i in range(6))
    es, er, ez, s0, v0, s1, v1, s2, v2, sz, vz, sg, vg, se, ve, sez, vez = rest[6 * n:]
    me = lax.axis_index('cp')
    fs = lax.axis_index('fsdp')
    y, x, c = place(fs)
    near, xn, yn = fs + 1 - 2 * c, fs + 2 - 4 * x, fs + 4 - 8 * y
    cps = [lax.rem(me + k, cp_size) for k in range(1, cp_size)]
    hops = (device(me, near), device(me, xn), device(me, yn))
    enter(list(hops) + [device(z, fs) for z in cps])

    def start(copies):
        for copy in copies:
            copy.start()

    def finish(copies):
        for copy in copies:
            copy.wait()

    def small_hop(i, src):
        copy = remote(src, er.at[i], se.at[i], ve.at[i], hops[i])
        copy.start()
        return copy

    first = [[remote(b.at[2 * j + 1 - c], r0[i].at[j], s0.at[i, j], v0.at[i, j], hops[0]) for j in range(4)] for i, b in enumerate(big)]
    for group in first:
        start(group)
    hop = small_hop(0, small)
    second = []
    for i, (path, _) in enumerate(specs):
        finish(first[i])
        for j in range(4):
            acc[i][j] = big[i][2 * j + c] + r0[i][j]
        group = []
        for k in range(2):
            give = 2 * k + 1 - x if path == 'xy' else 2 * (1 - y) + k
            group.append(remote(acc[i].at[give], r1[i].at[k], s1.at[i, k], v1.at[i, k], hops[1] if path == 'xy' else hops[2]))
        start(group)
        second.append(group)
    hop.wait()
    es[0] = small[...] + er[0]
    hop = small_hop(1, es.at[0])
    third = []
    for i, (path, _) in enumerate(specs):
        finish(second[i])
        for k in range(2):
            keep = 2 * k + x if path == 'xy' else 2 * y + k
            r1[i][k] = acc[i][keep] + r1[i][k]
        give = 1 - y if path == 'xy' else 1 - x
        copy = remote(r1[i].at[give], r2[i], s2.at[i], v2.at[i], hops[2] if path == 'xy' else hops[1])
        copy.start()
        third.append(copy)
    hop.wait()
    es[1] = es[0] + er[1]
    hop = small_hop(2, es.at[1])
    fourth = []
    for i, (path, spec) in enumerate(specs):
        third[i].wait()
        keep = y if path == 'xy' else x
        outs[i][...] = r1[i][keep] + r2[i][...]
        group = [remote(piece_of(outs[i], spec, cps[k]), rz[i].at[k], sz.at[i, k], vz.at[i, k], device(cps[k], fs)) for k in range(cp_size - 1)]
        start(group)
        fourth.append(group)
    hop.wait()
    ez[me] = es[1] + er[2]
    last = [remote(ez.at[me], ez.at[me], sez.at[k], vez.at[k], device(cps[k], fs)) for k in range(cp_size - 1)]
    start(last)
    fifth = []
    for i, (path, spec) in enumerate(specs):
        finish(fourth[i])
        rg[i][me] = ((piece_of(outs[i], spec, me)[...] + rz[i][0]) + rz[i][1]) + rz[i][2]
        group = [remote(rg[i].at[me], rg[i].at[me], sg.at[i, k], vg.at[i, k], device(cps[k], fs)) for k in range(cp_size - 1)]
        start(group)
        fifth.append(group)
    finish(last)
    small_out[...] = ((ez[0] + ez[1]) + ez[2]) + ez[3]
    for i, (path, spec) in enumerate(specs):
        finish(fifth[i])
        for p in range(cp_size):
            axis, size, stride = spec
            lo = p * stride
            if axis == 0:
                outs[i][lo:lo + size, :] = rg[i][p]
            else:
                outs[i][:, lo:lo + size] = rg[i][p]


def reduce_call(cp_size, arrays, small):
    vmem = pl.BlockSpec(memory_space=pltpu.VMEM)
    dma = pltpu.SemaphoreType.DMA
    n = len(arrays)
    specs = tuple((path, spec) for _, path, spec in arrays)
    shapes = [arr.shape[1:] for arr, _, _ in arrays]
    cut = [((size, sh[1]) if axis == 0 else (sh[0], size)) for sh, (_, (axis, size, _)) in zip(shapes, specs)]
    scratch = [pltpu.VMEM((4,) + sh, F32) for sh in shapes] * 2 + [pltpu.VMEM((2,) + sh, F32) for sh in shapes] + [pltpu.VMEM(sh, F32) for sh in shapes]
    scratch += [pltpu.VMEM((cp_size - 1,) + sh, F32) for sh in cut] + [pltpu.VMEM((cp_size,) + sh, F32) for sh in cut]
    scratch += [pltpu.VMEM((2,) + small.shape, F32), pltpu.VMEM((3,) + small.shape, F32), pltpu.VMEM((cp_size,) + small.shape, F32)]
    for shape in ((n, 4), (n, 2), (n,), (n, cp_size - 1), (n, cp_size - 1), (3,), (cp_size - 1,)):
        scratch += [dma(shape), dma(shape)]
    return pl.pallas_call(
        functools.partial(reduce_kernel, cp_size, specs),
        out_shape=[sds(sh, F32) for sh in shapes] + [sds(small.shape, F32)],
        in_specs=[vmem] * (n + 1), out_specs=[vmem] * (n + 1), scratch_shapes=scratch,
        compiler_params=pltpu.CompilerParams(collective_id=1, has_side_effects=True, vmem_limit_bytes=48 * 1024 * 1024),
        name='reduce',
    )(*[arr for arr, _, _ in arrays], small)


def solution(mesh):
    cp_size = mesh.shape['cp']
    fs_size = mesh.shape['fsdp']

    def shift(k):
        return [(i, (i + k) % cp_size) for i in range(cp_size)]

    def local_step(tokens, lengths, embed_table, layer_vecs, w_qkv, w_out, w_up, b_up, w_down, grad_out):
        n_loc, seq_loc = tokens.shape
        n_seq = n_loc // cp_size
        me = lax.axis_index('cp')
        fs = lax.axis_index('fsdp')

        def to_whole(arr):
            blocks = []
            for k in range(cp_size):
                dest = (me + k) % cp_size
                blk = lax.dynamic_slice_in_dim(arr, dest * n_seq, n_seq, 0)
                blocks.append(lax.ppermute(blk, 'cp', shift(k)) if k else blk)
            return blocks

        g_blocks = to_whole(grad_out)
        len_w = lax.dynamic_slice_in_dim(lengths, me * n_seq, n_seq, 0)
        small = jnp.concatenate([layer_vecs, b_up.reshape(F // D, D // fs_size)], axis=0)
        small = jnp.pad(small, ((0, SM_ROWS - small.shape[0]), (0, LANES - small.shape[1])))
        qkv_p, out_p, up_p, down_p, small_p, tok_p = gather_call(cp_size, [w_qkv.reshape(-1, 3 * D), w_out, w_up, w_down, small], tokens.reshape(cp_size, n_seq, seq_loc))
        down_w = down_p.reshape(F, D)
        tok_w = tok_p.transpose(1, 0, 2).reshape(n_seq, 1, SEQ)
        emb_t = jnp.pad(embed_table, ((0, VOCAB_PAD - embed_table.shape[0]), (0, 0))).T

        lane = jnp.arange(SEQ)
        positions = ((me - lane // seq_loc + cp_size) % cp_size) * seq_loc + lane % seq_loc
        inv_freq = 1.0 / (ROPE_BASE ** (jnp.arange(0, HEAD_DIM, 2, dtype=F32) / HEAD_DIM))
        angles = inv_freq[:, None] * positions.astype(F32)[None, :]
        cos_t, sin_t = jnp.cos(angles), jnp.sin(angles)
        me_arr = me.reshape(1).astype(jnp.int32)

        S = SEQ
        blk_spec = per_seq(seq_loc, D)
        outs = call(
            functools.partial(fwd_kernel, cp_size, seq_loc), n_seq,
            [SMEM, SMEM, per_seq(1, S), whole(D, VOCAB_PAD), whole(*small_p.shape), whole(*qkv_p.shape), whole(*out_p.shape), whole(*up_p.shape), whole(F, D), whole(8, S), whole(8, S)],
            [blk_spec] * 4 + [per_seq(D, S), per_seq(D, S), per_seq(8, S), per_seq(3 * D, S), per_seq(N_HEADS, 1, S), per_seq(D, S), per_seq(D, S), per_seq(D, S), per_seq(F, S), per_seq(F, S), whole(D, SM_ROWS), whole(D, 3 * D), whole(D, D), whole(D, F)],
            [sds((n_seq, seq_loc, D), BF)] * 4 + [sds((n_seq, D, S), BF), sds((n_seq, D, S), F32), sds((n_seq, 8, S), F32), sds((n_seq, 3 * D, S), BF), sds((n_seq, N_HEADS, 1, S), F32), sds((n_seq, D, S), F32), sds((n_seq, D, S), F32), sds((n_seq, D, S), BF), sds((n_seq, F, S), BF), sds((n_seq, F, S), F32), sds((D, SM_ROWS), F32), sds((D, 3 * D), BF), sds((D, D), BF), sds((D, F), BF)],
            [pltpu.VMEM((3 * D, D), BF), pltpu.VMEM((D, D), BF), pltpu.VMEM((F, D), BF), pltpu.VMEM((D, F), BF), pltpu.VMEM((N_TILES, S, LANES), BF), pltpu.VMEM((N_TILES * LANES, S), BF), pltpu.VMEM((S, S), F32), pltpu.VMEM((9, D, LANES), F32), pltpu.VMEM((F, LANES), F32)],
            9_000_000_000, 'fwd',
        )(len_w, me_arr, tok_w, emb_t, small_p, qkv_p, out_p, up_p, down_w, cos_t, sin_t)
        out_blocks = outs[:4]
        h, xhat1, stat, qkv, lse, attn, xhat2, a, gelu, dgelu, vecs_t, qkv_w, out_w, up_w = outs[4:]

        dres, dattn, dw_down, dw_uo, db_up, dvec2 = call(
            functools.partial(ffn_bwd_kernel, n_seq, seq_loc), n_seq,
            [blk_spec] * 4 + [whole(D, SM_ROWS), whole(F, D), whole(D, F), whole(D, D), per_seq(F, S), per_seq(F, S), per_seq(D, S), per_seq(D, S), per_seq(8, S), per_seq(D, S)],
            [per_seq(D, S), per_seq(D, S), whole(F, D), whole(D, UO_PAD), whole(1, F), whole(8, N_TILES * LANES)],
            [sds((n_seq, D, S), F32), sds((n_seq, D, S), F32), sds((F, D), F32), sds((D, UO_PAD), F32), sds((1, F), F32), sds((8, N_TILES * LANES), F32)],
            [pltpu.VMEM((F, LANES), F32), pltpu.VMEM((4, D, LANES), F32)],
            9_000_000_000, 'ffn_bwd',
        )(*g_blocks, vecs_t, down_w, up_w, out_w, gelu, dgelu, a, xhat2, stat, attn)

        dw_qa, dw_qb, d_emb, dvec1 = call(
            functools.partial(attn_bwd_kernel, n_seq, cp_size, seq_loc), n_seq,
            [SMEM, SMEM, per_seq(1, S), whole(D, SM_ROWS), whole(D, 3 * D), whole(8, S), whole(8, S), per_seq(3 * D, S), per_seq(N_HEADS, 1, S), per_seq(D, S), per_seq(D, S), per_seq(D, S), per_seq(D, S), per_seq(D, S), per_seq(8, S)],
            [whole(D, QKV_HALF), whole(D, QKV_HALF), whole(VOCAB_PAD, D), whole(8, N_TILES * LANES)],
            [sds((D, QKV_HALF), F32), sds((D, QKV_HALF), F32), sds((VOCAB_PAD, D), F32), sds((8, N_TILES * LANES), F32)],
            [pltpu.VMEM((N_TILES, S, LANES), BF), pltpu.VMEM((N_TILES, S, LANES), BF), pltpu.VMEM((N_TILES * LANES, S), BF), pltpu.VMEM((N_TILES * LANES, S), BF), pltpu.VMEM((S, S), F32),
             pltpu.VMEM((D, S), F32), pltpu.VMEM((D, S), F32), pltpu.VMEM((D, S), F32), pltpu.VMEM((3, D, LANES), F32), pltpu.VMEM((2, D, LANES), F32)],
            9_000_000_000, 'attn_bwd',
        )(len_w, me_arr, tok_w, vecs_t, qkv_w, cos_t, sin_t, qkv, lse, attn, dattn, dres, xhat1, h, stat)

        layer_out = jnp.zeros((n_loc, seq_loc, D), BF)
        for k in range(cp_size):
            back = lax.ppermute(out_blocks[k], 'cp', shift(-k)) if k else out_blocks[0]
            layer_out = lax.dynamic_update_slice_in_dim(layer_out, back, ((me + k) % cp_size) * n_seq, 0)

        vocab = embed_table.shape[0]
        packed = jnp.concatenate([d_emb[:vocab], dvec1[:5, :D], dvec2[:4, :D], db_up.reshape(F // D, D)], axis=0)
        packed = jnp.pad(packed, ((0, 48 - packed.shape[0]), (0, N_TILES * LANES - D)))

        def pieces(arr):
            return arr.reshape(fs_size, arr.shape[0] // fs_size, arr.shape[1])

        r_down, r_uo, r_qa, r_qb, packed = reduce_call(cp_size, [(pieces(dw_down), 'xy', (0, 40, 40)), (pieces(dw_uo), 'yx', (1, 512, 384)), (pieces(dw_qa), 'xy', (1, 128, 128)), (pieces(dw_qb), 'yx', (1, 128, 128))], packed)
        packed = packed[:, :D]
        d_vecs = lax.dynamic_slice_in_dim(packed[vocab:vocab + 9], fs * (D // fs_size), D // fs_size, 1)
        d_bup = lax.dynamic_slice_in_dim(packed[vocab + 9:vocab + 13].reshape(F), fs * (F // fs_size), F // fs_size, 0)
        d_qkv = jnp.concatenate([r_qa, r_qb], axis=1)[:, :3 * D].reshape(w_qkv.shape)
        return (layer_out, packed[:vocab], d_vecs, d_qkv, r_uo[:, F:F + D], r_uo[:, :F], d_bup, r_down)

    in_specs = (P('fsdp', 'cp'), P('fsdp'), P(), P(None, 'fsdp'), P('fsdp', None, None, None), P('fsdp', None), P('fsdp', None), P('fsdp'), P('fsdp', None), P('fsdp', 'cp', None))
    out_specs = (P('fsdp', 'cp', None), P(), P(None, 'fsdp'), P('fsdp', None, None, None), P('fsdp', None), P('fsdp', None), P('fsdp'), P('fsdp', None))
    return jax.shard_map(local_step, mesh=mesh, in_specs=in_specs, out_specs=out_specs, check_vma=False)
```

```python
import functools

import jax
import jax.numpy as jnp
from jax import lax
from jax.experimental import pallas as pl
from jax.experimental.pallas import tpu as pltpu
from jax.sharding import PartitionSpec as P

MASK_ID = 32
LN_EPS = 1e-5
ROPE_BASE = 10000.0
TRAIN_RATIO = 0.15 * 0.8
NEG_BIG = -1e30
VOCAB_PAD = 128
HEAD_DIM = 16
N_HEADS = 20
D = 320
F = 1280
SEQ = 256
LANES = 128
HEADS_PER_TILE = LANES // HEAD_DIM
N_TILES = -(-D // LANES)
HEAD_UNROLL = 4
QKV_HALF = 512
UO_PAD = 1664
SM_ROWS = 16
BF = jnp.bfloat16
F32 = jnp.float32
SQRT_HALF = 0.7071067811865476
INV_SQRT_2PI = 0.3989422804014327

NN = (((1,), (0,)), ((), ()))
NT = (((1,), (1,)), ((), ()))


def dot(a, b, dims=NN):
    return lax.dot_general(a, b, dims, preferred_element_type=F32)


def col(vecs_t, j):
    return vecs_t[:, j:j + 1]


def rope(z, cos_t, sin_t):
    z4 = z.reshape(N_HEADS, 2, HEAD_DIM // 2, SEQ)
    lower, upper = z4[:, 0], z4[:, 1]
    new_l = lower * cos_t - upper * sin_t
    new_u = upper * cos_t + lower * sin_t
    return jnp.stack([new_l, new_u], axis=1).reshape(D, SEQ)


def key_bias(shift_base, cp_size, seq_loc, length):
    row = lax.broadcasted_iota(jnp.int32, (SEQ, SEQ), 0)
    src = (shift_base - row // seq_loc + cp_size) % cp_size
    pos = src * seq_loc + row % seq_loc
    return jnp.where(pos < length, 0.0, NEG_BIG).astype(F32)


def store_token_major(dst_ref, z_t):
    for t in range(N_TILES):
        lo = t * LANES
        hi = min(lo + LANES, D)
        part = z_t[lo:hi]
        if hi - lo < LANES:
            part = jnp.concatenate([part, jnp.zeros((LANES - (hi - lo), z_t.shape[1]), F32)], axis=0)
        dst_ref[t] = part.T.astype(BF)


def head_rows(tile, slot):
    row = lax.broadcasted_iota(jnp.int32, tile.shape, 0)
    return jnp.where(row // HEAD_DIM == slot, tile, jnp.zeros_like(tile))


def token_scale(tok, length, seq_loc, cp_size, me):
    lane = lax.broadcasted_iota(jnp.int32, (1, SEQ), 1)
    src = (me - lane // seq_loc + cp_size) % cp_size
    pos = src * seq_loc + lane % seq_loc
    is_mask = tok == MASK_ID
    n_mask = jnp.sum(is_mask.astype(F32), axis=1, keepdims=True)
    drop = (1.0 - TRAIN_RATIO) / (1.0 - n_mask / length.astype(F32))
    return jnp.where(is_mask | (pos >= length), 0.0, drop)


def one_hot_rows(tok):
    row = lax.broadcasted_iota(jnp.int32, (VOCAB_PAD, SEQ), 0)
    return jnp.where(row == tok, 1.0, 0.0).astype(BF)


def join_rows(ref):
    return jnp.concatenate([ref[i].astype(F32) for i in range(ref.shape[0])], axis=0).astype(BF)


def wide(z):
    return jnp.concatenate([z, z], axis=1)


def fwd_kernel(cp_size, seq_loc, len_ref, me_ref, tok_ref, emb_ref, sm_ref, wqkv_ref, wout_ref, wup_ref, wdown_ref, cos_ref, sin_ref,
               o0_ref, o1_ref, o2_ref, o3_ref, h_ref, xhat1_ref, stat_ref, qkv_ref, lse_ref, attn_ref, xhat2_ref, a_ref, gelu_ref, dgelu_ref, gain_ref, wqkv_n, wout_n, wup_n,
               wqkv_t, wout_t, wup_t, wdown_t, k_tm, q_pad, bias, vec_b, bup_b):
    step = pl.program_id(0)

    @pl.when(step == 0)
    def _():
        for src, nat, tr in ((wqkv_ref, wqkv_n, wqkv_t), (wout_ref, wout_n, wout_t), (wup_ref, wup_n, wup_t)):
            joined = join_rows(src)
            nat[...] = joined
            tr[...] = joined.T
        wdown_t[...] = wdown_ref[...].T
        q_pad[...] = jnp.zeros_like(q_pad)
        pieces = sm_ref.shape[0]
        rows = D // pieces
        for i in range(pieces):
            sm_t = sm_ref[i].T
            gain_ref[i * rows:(i + 1) * rows] = sm_t[:rows]
            for j in range(9):
                vec_b[j, i * rows:(i + 1) * rows] = jnp.broadcast_to(sm_t[:rows, j:j + 1], (rows, LANES))
            for r in range(F // D):
                lo = i * (F // pieces) + r * rows
                bup_b[lo:lo + rows] = jnp.broadcast_to(sm_t[:rows, 9 + r:10 + r], (rows, LANES))

    length = len_ref[step]
    me = me_ref[0]
    tok = tok_ref[0]
    keep = token_scale(tok, length, seq_loc, cp_size, me)
    e = dot(emb_ref[...], one_hot_rows(tok)) * keep
    mean = jnp.mean(e, axis=0, keepdims=True)
    cent = e - mean
    var = jnp.mean(cent * cent, axis=0, keepdims=True)
    rstd1 = lax.rsqrt(var + LN_EPS)
    xhat1 = cent * rstd1
    xhat1_ref[0] = xhat1
    h = (xhat1 * wide(vec_b[0]) + wide(vec_b[1])).astype(BF)
    h_ref[0] = h
    cos_t, sin_t = cos_ref[...], sin_ref[...]
    q = (dot(wqkv_t[0:D], h) + wide(vec_b[2])) * HEAD_DIM ** -0.5
    q = rope(q, cos_t, sin_t).astype(BF)
    qkv_ref[0, 0:D] = q
    q_pad[0:D] = q
    k = rope(dot(wqkv_t[D:2 * D], h) + wide(vec_b[3]), cos_t, sin_t)
    qkv_ref[0, D:2 * D] = k.astype(BF)
    store_token_major(k_tm, k)
    qkv_ref[0, 2 * D:3 * D] = (dot(wqkv_t[2 * D:3 * D], h) + wide(vec_b[4])).astype(BF)
    bias[...] = key_bias(me, cp_size, seq_loc, length)

    def head_body(it, _):
        for u in range(HEAD_UNROLL):
            hd = it * HEAD_UNROLL + u
            tile = hd // HEADS_PER_TILE
            slot = hd % HEADS_PER_TILE
            q_t = q_pad[pl.ds(pl.multiple_of(tile * LANES, LANES), LANES), :]
            s = dot(k_tm[tile], head_rows(q_t, slot)) + bias[...]
            m = jnp.max(s, axis=0, keepdims=True)
            p = jnp.exp(s - m)
            l = jnp.sum(p, axis=0, keepdims=True)
            r0 = pl.multiple_of(hd * HEAD_DIM, HEAD_DIM)
            v_h = qkv_ref[0, pl.ds(pl.multiple_of(2 * D + hd * HEAD_DIM, HEAD_DIM), HEAD_DIM), :]
            attn_ref[0, pl.ds(r0, HEAD_DIM), :] = dot(v_h, p.astype(BF)) / l
            lse_ref[0, hd] = m + jnp.log(l)
        return 0

    lax.fori_loop(0, N_HEADS // HEAD_UNROLL, head_body, 0)

    o = attn_ref[0].astype(BF)
    x1 = e + dot(wout_t[...], o) + wide(vec_b[5])
    mean2 = jnp.mean(x1, axis=0, keepdims=True)
    cent2 = x1 - mean2
    var2 = jnp.mean(cent2 * cent2, axis=0, keepdims=True)
    rstd2 = lax.rsqrt(var2 + LN_EPS)
    xhat2 = cent2 * rstd2
    xhat2_ref[0] = xhat2
    a = (xhat2 * wide(vec_b[6]) + wide(vec_b[7])).astype(BF)
    a_ref[0] = a
    stat_ref[0] = jnp.concatenate([rstd1, rstd2, keep, jnp.zeros((5, SEQ), F32)], axis=0)
    out = x1 + wide(vec_b[8])
    for c in range(F // D):
        rows = slice(c * D, (c + 1) * D)
        u = dot(wup_t[rows], a) + wide(bup_b[rows])
        cdf = 0.5 * (1.0 + lax.erf(u * SQRT_HALF))
        g = (u * cdf).astype(BF)
        gelu_ref[0, rows] = g
        dgelu_ref[0, rows] = cdf + u * (INV_SQRT_2PI * jnp.exp(-0.5 * u * u))
    out = out + dot(wdown_t[...], gelu_ref[0])
    out_tm = to_token_major(out)
    for k_i, o_ref in enumerate((o0_ref, o1_ref, o2_ref, o3_ref)):
        o_ref[0] = out_tm[k_i * seq_loc:(k_i + 1) * seq_loc]


def to_token_major(z_t):
    parts = []
    for t in range(N_TILES):
        lo, hi = t * LANES, min((t + 1) * LANES, D)
        part = z_t[lo:hi]
        if hi - lo < LANES:
            part = jnp.concatenate([part, jnp.zeros((LANES - (hi - lo), SEQ), F32)], axis=0)
        parts.append(part.T.astype(BF))
    return jnp.concatenate(parts, axis=1)[:, :D]


def to_feature_major(z):
    z32 = z.astype(F32)
    pad = jnp.concatenate([z32, jnp.zeros((SEQ, N_TILES * LANES - D), F32)], axis=1)
    return jnp.concatenate([pad[:, t * LANES:(t + 1) * LANES].T for t in range(N_TILES)], axis=0)[:D]


def lane_part(z):
    return z[:, :LANES] + z[:, LANES:]


def ln_grad(dn, xhat, rstd, gain):
    dxh = dn * gain
    m1 = jnp.mean(dxh, axis=0, keepdims=True)
    m2 = jnp.mean(dxh * xhat, axis=0, keepdims=True)
    return rstd * (dxh - m1 - xhat * m2)


def row_sum(acc):
    return jnp.sum(acc.T, axis=0, keepdims=True)


def ffn_bwd_kernel(n_steps, seq_loc, g0_ref, g1_ref, g2_ref, g3_ref, vec_ref, wdown_ref, wup_ref, wout_ref, gelu_ref, dgelu_ref, a_ref, xhat2_ref, stat_ref, attn_ref,
                   dres_ref, dattn_ref, dwdown_ref, dwuo_ref, dvec_ref,
                   acc_bup, acc_vec):
    step = pl.program_id(0)

    @pl.when(step == 0)
    def _():
        dwdown_ref[...] = jnp.zeros_like(dwdown_ref)
        dwuo_ref[...] = jnp.zeros_like(dwuo_ref)
        acc_bup[...] = jnp.zeros_like(acc_bup)
        acc_vec[...] = jnp.zeros_like(acc_vec)

    vecs = vec_ref[...]
    g = jnp.concatenate([g0_ref[0], g1_ref[0], g2_ref[0], g3_ref[0]], axis=0)
    g_t = to_feature_major(g)
    a = a_ref[0]
    dn2 = jnp.zeros((D, SEQ), F32)
    dup_parts = []
    for c in range(F // D):
        rows = slice(c * D, (c + 1) * D)
        dup = dot(wdown_ref[rows], g, NT) * dgelu_ref[0, rows]
        acc_bup[rows] += lane_part(dup)
        dup_parts.append(dup.astype(BF))
        dwdown_ref[rows] += dot(gelu_ref[0, rows], g)
    dup_b = jnp.concatenate(dup_parts, axis=0)
    dwuo_ref[:, 0:F] += dot(a, dup_b, NT)
    dn2 = dot(wup_ref[...], dup_b)
    xhat2 = xhat2_ref[0]
    rstd2 = stat_ref[0, 1:2]
    dres = g_t + ln_grad(dn2, xhat2, rstd2, col(vecs, 6))
    acc_vec[0] += lane_part(dres)
    acc_vec[1] += lane_part(dn2 * xhat2)
    acc_vec[2] += lane_part(dn2)
    acc_vec[3] += lane_part(g_t)
    dres_ref[0] = dres
    dres_b = dres.astype(BF)
    dwuo_ref[:, F:F + D] += dot(attn_ref[0].astype(BF), dres_b, NT)
    dattn_ref[0] = dot(wout_ref[...], dres_b)

    @pl.when(step == n_steps - 1)
    def _():
        rows = [row_sum(pad_rows(acc_vec[j])) for j in range(4)] + [row_sum(pad_rows(acc_bup[j * D:(j + 1) * D])) for j in range(F // D)]
        dvec_ref[...] = jnp.concatenate(rows, axis=0)


def pad_rows(z):
    return jnp.concatenate([z, jnp.zeros((N_TILES * LANES - D, LANES), F32)], axis=0)


def attn_bwd_kernel(n_steps, cp_size, seq_loc, len_ref, me_ref, tok_ref, vec_ref, wqkv_ref, cos_ref, sin_ref, qkv_ref, lse_ref, attn_ref, dattn_ref, dres_ref, xhat1_ref, h_ref, stat_ref, dwdown_ref, dwuo_ref, dvec2_ref,
                    rdown_ref, ruo_ref, rqa_ref, rqb_ref, rsmall_ref,
                    k_tm, v_tm, q_pad, do_pad, bias, dq_s, dk_s, dv_s, acc_b, acc_vec, acc_qa, acc_qb, acc_emb, *red):
    step = pl.program_id(0)
    summer = GradSum(cp_size, (dwdown_ref, dwuo_ref, acc_qa, acc_qb), (rdown_ref, ruo_ref, rqa_ref, rqb_ref), rsmall_ref, red)

    @pl.when(step == 0)
    def _():
        summer.enter()
        for i in (0, 1):
            summer.start(0, i)
        acc_qa[...] = jnp.zeros_like(acc_qa)
        acc_qb[...] = jnp.zeros_like(acc_qb)
        acc_emb[...] = jnp.zeros_like(acc_emb)
        acc_b[...] = jnp.zeros_like(acc_b)
        acc_vec[...] = jnp.zeros_like(acc_vec)
        q_pad[...] = jnp.zeros_like(q_pad)
        do_pad[...] = jnp.zeros_like(do_pad)

    for phase, at in enumerate(PHASE_STEPS):
        @pl.when(step == at)
        def _(phase=phase):
            for i in (0, 1):
                summer.finish(phase, i)
                summer.start(phase + 1, i)

    length = len_ref[step]
    me = me_ref[0]
    vecs = vec_ref[...]
    q_pad[0:D] = qkv_ref[0, 0:D]
    do_pad[0:D] = dattn_ref[0].astype(BF)
    store_token_major(k_tm, qkv_ref[0, D:2 * D].astype(F32))
    store_token_major(v_tm, qkv_ref[0, 2 * D:3 * D].astype(F32))
    bias[...] = key_bias(me, cp_size, seq_loc, length)

    def head_body(it, _):
        for u in range(HEAD_UNROLL):
            hd = it * HEAD_UNROLL + u
            tile = hd // HEADS_PER_TILE
            slot = hd % HEADS_PER_TILE
            t0 = pl.ds(pl.multiple_of(tile * LANES, LANES), LANES)
            rows = pl.ds(pl.multiple_of(hd * HEAD_DIM, HEAD_DIM), HEAD_DIM)
            q_h = q_pad[rows, :]
            do_h = do_pad[rows, :]
            k_h = qkv_ref[0, pl.ds(pl.multiple_of(D + hd * HEAD_DIM, HEAD_DIM), HEAD_DIM), :]
            delta = jnp.sum(dattn_ref[0, rows, :] * attn_ref[0, rows, :], axis=0, keepdims=True)
            s = dot(k_tm[tile], head_rows(q_pad[t0, :], slot)) + bias[...]
            p = jnp.exp(s - lse_ref[0, hd])
            dp = dot(v_tm[tile], head_rows(do_pad[t0, :], slot))
            ds = (p * (dp - delta)).astype(BF)
            dq_s[rows, :] = dot(k_h, ds)
            dk_s[rows, :] = dot(q_h, ds, NT)
            dv_s[rows, :] = dot(do_h, p.astype(BF), NT)
        return 0

    lax.fori_loop(0, N_HEADS // HEAD_UNROLL, head_body, 0)

    cos_t, sin_t = cos_ref[...], sin_ref[...]
    h = h_ref[0]
    dq = rope(dq_s[...], cos_t, -sin_t) * HEAD_DIM ** -0.5
    dk = rope(dk_s[...], cos_t, -sin_t)
    dv = dv_s[...]
    dn1 = jnp.zeros((D, SEQ), F32)
    parts = []
    for j, dz in enumerate((dq, dk, dv)):
        acc_b[j] += lane_part(dz)
        parts.append(dz.astype(BF))
    dz_b = jnp.concatenate(parts, axis=0)
    acc_qa[...] += dot(h, dz_b[:QKV_HALF], NT).reshape(acc_qa.shape)
    acc_qb[:, :, :3 * D - QKV_HALF] += dot(h, dz_b[QKV_HALF:], NT).reshape(acc_qb.shape[0], acc_qb.shape[1], 3 * D - QKV_HALF)
    dn1 = dot(wqkv_ref[...], dz_b)
    xhat1 = xhat1_ref[0]
    acc_vec[0] += lane_part(dn1 * xhat1)
    acc_vec[1] += lane_part(dn1)
    de = dres_ref[0] + ln_grad(dn1, xhat1, stat_ref[0, 0:1], col(vecs, 0))
    de = (de * stat_ref[0, 2:3]).astype(BF)
    acc_emb[...] += dot(one_hot_rows(tok_ref[0]), de, NT)

    @pl.when(step == n_steps - 1)
    def _():
        for i in (2, 3):
            summer.start(0, i)
        rows = [row_sum(pad_rows(acc_vec[j])) for j in range(2)] + [row_sum(pad_rows(acc_b[j])) for j in range(3)]
        small = summer.small
        small[0:EMB_ROWS, 0:D] = acc_emb[0:EMB_ROWS]
        small[0:EMB_ROWS, D:] = jnp.zeros((EMB_ROWS, N_TILES * LANES - D), F32)
        small[EMB_ROWS:EMB_ROWS + 8] = jnp.concatenate(rows + [jnp.zeros((3, N_TILES * LANES), F32)], axis=0)
        small[EMB_ROWS + 8:EMB_ROWS + 16] = dvec2_ref[...]
        small[EMB_ROWS + 16:SMALL_ROWS] = jnp.zeros((SMALL_ROWS - EMB_ROWS - 16, N_TILES * LANES), F32)
        summer.start_small(0)
        for phase in range(5):
            for i in (2, 3):
                summer.finish(phase, i)
                if phase < 4:
                    summer.start(phase + 1, i)
            summer.finish_small(phase)
            if phase < 4:
                summer.start_small(phase + 1)
        for i in (0, 1):
            summer.finish(4, i)


MESH = pl.DeviceIdType.MESH
EMB_ROWS = 40
SMALL_ROWS = 64
PHASE_STEPS = (1, 3, 4, 6)
STREAMS = (('xy', (0, 40, 40)), ('yx', (1, 512, 384)), ('xy', (1, 128, 128)), ('yx', (1, 128, 128)))
SMALL_SPEC = (0, SMALL_ROWS // 4, SMALL_ROWS // 4)


def place(fs):
    return fs // 4, (fs // 2) % 2, fs % 2


def device(cp, fs):
    return {'cp': cp, 'fsdp': fs}


def enter(peers):
    barrier = pltpu.get_barrier_semaphore()
    for peer in peers:
        pl.semaphore_signal(barrier, inc=1, device_id=peer, device_id_type=MESH)
    pl.semaphore_wait(barrier, len(peers))


def remote(src, dst, send_sem, recv_sem, peer):
    return pltpu.make_async_remote_copy(src_ref=src, dst_ref=dst, send_sem=send_sem, recv_sem=recv_sem, device_id=peer, device_id_type=MESH)


def piece_of(ref, spec, p):
    axis, size, stride = spec
    start = pl.multiple_of(p * stride, stride)
    return ref.at[pl.ds(start, size), :] if axis == 0 else ref.at[:, pl.ds(start, size)]


class GradSum:
    def __init__(self, cp_size, big, outs, small_out, refs):
        n = len(STREAMS)
        self.cp_size, self.big, self.outs, self.small_out = cp_size, big, outs, small_out
        self.r0, self.acc, self.r1, self.r2, self.rz, self.rg = (refs[i * n:(i + 1) * n] for i in range(6))
        self.small, self.er, self.ez, self.eg = refs[6 * n:6 * n + 4]
        sems = refs[6 * n + 4:]
        self.sends, self.recvs = sems[0:5], sems[5:10]
        self.small_send, self.small_recv = sems[10], sems[11]
        self.me = lax.axis_index('cp')
        self.fs = lax.axis_index('fsdp')
        self.y, self.x, self.c = place(self.fs)
        fs, y, x, c = self.fs, self.y, self.x, self.c
        self.cps = [lax.rem(self.me + k, cp_size) for k in range(1, cp_size)]
        self.hops = [device(self.me, f) for f in (fs + 1 - 2 * c, fs + 2 - 4 * x, fs + 4 - 8 * y)]
        self.peers = [device(z, fs) for z in self.cps]

    def enter(self):
        enter(self.hops + self.peers)

    def copies(self, phase, i):
        path, spec = STREAMS[i]
        xy = path == 'xy'
        s, v = self.sends[phase], self.recvs[phase]
        x, y, c, me = self.x, self.y, self.c, self.me
        if phase == 0:
            return [remote(self.big[i].at[2 * j + 1 - c], self.r0[i].at[j], s.at[i, j], v.at[i, j], self.hops[0]) for j in range(4)]
        if phase == 1:
            give = [2 * k + 1 - x if xy else 2 * (1 - y) + k for k in range(2)]
            return [remote(self.acc[i].at[give[k]], self.r1[i].at[k], s.at[i, k], v.at[i, k], self.hops[1 if xy else 2]) for k in range(2)]
        if phase == 2:
            return [remote(self.r1[i].at[1 - y if xy else 1 - x], self.r2[i], s.at[i, 0], v.at[i, 0], self.hops[2 if xy else 1])]
        if phase == 3:
            return [remote(piece_of(self.outs[i], spec, self.cps[k]), self.rz[i].at[k], s.at[i, k], v.at[i, k], self.peers[k]) for k in range(self.cp_size - 1)]
        return [remote(self.rg[i].at[me], self.rg[i].at[me], s.at[i, k], v.at[i, k], self.peers[k]) for k in range(self.cp_size - 1)]

    def start(self, phase, i):
        for copy in self.copies(phase, i):
            copy.start()

    def finish(self, phase, i):
        for copy in self.copies(phase, i):
            copy.wait()
        path, spec = STREAMS[i]
        xy = path == 'xy'
        big, r0, acc, r1, r2, out = self.big[i], self.r0[i], self.acc[i], self.r1[i], self.r2[i], self.outs[i]
        rz, rg = self.rz[i], self.rg[i]
        if phase == 0:
            for j in range(4):
                acc[j] = big[2 * j + self.c] + r0[j]
        elif phase == 1:
            for k in range(2):
                r1[k] = acc[2 * k + self.x if xy else 2 * self.y + k] + r1[k]
        elif phase == 2:
            out[...] = r1[self.y if xy else self.x] + r2[...]
        elif phase == 3:
            rg[self.me] = ((piece_of(out, spec, self.me)[...] + rz[0]) + rz[1]) + rz[2]
        else:
            axis, size, stride = spec
            for p in range(self.cp_size):
                lo = p * stride
                if axis == 0:
                    out[lo:lo + size, :] = rg[p]
                else:
                    out[:, lo:lo + size] = rg[p]

    def small_copies(self, phase):
        s, v = self.small_send, self.small_recv
        if phase < 3:
            return [remote(self.small, self.er.at[phase], s.at[phase], v.at[phase], self.hops[phase])]
        if phase == 3:
            return [remote(piece_of(self.small, SMALL_SPEC, self.cps[k]), self.ez.at[k], s.at[3 + k], v.at[3 + k], self.peers[k]) for k in range(self.cp_size - 1)]
        return [remote(self.eg.at[self.me], self.eg.at[self.me], s.at[6 + k], v.at[6 + k], self.peers[k]) for k in range(self.cp_size - 1)]

    def start_small(self, phase):
        for copy in self.small_copies(phase):
            copy.start()

    def finish_small(self, phase):
        for copy in self.small_copies(phase):
            copy.wait()
        if phase < 3:
            self.small[...] += self.er[phase]
        elif phase == 3:
            self.eg[self.me] = ((piece_of(self.small, SMALL_SPEC, self.me)[...] + self.ez[0]) + self.ez[1]) + self.ez[2]
        else:
            size = SMALL_SPEC[1]
            for p in range(self.cp_size):
                self.small_out[p * size:(p + 1) * size, :] = self.eg[p]


def sum_scratch(cp_size, shapes, small_shape):
    dma = pltpu.SemaphoreType.DMA
    n = len(shapes)
    cut = [((size, sh[1]) if axis == 0 else (sh[0], size)) for sh, (_, (axis, size, _)) in zip(shapes, STREAMS)]
    lanes = small_shape[1]
    scratch = [pltpu.VMEM((4,) + sh, F32) for sh in shapes] * 2 + [pltpu.VMEM((2,) + sh, F32) for sh in shapes] + [pltpu.VMEM(sh, F32) for sh in shapes]
    scratch += [pltpu.VMEM((cp_size - 1,) + sh, F32) for sh in cut] + [pltpu.VMEM((cp_size,) + sh, F32) for sh in cut]
    scratch += [pltpu.VMEM(small_shape, F32), pltpu.VMEM((3,) + small_shape, F32), pltpu.VMEM((cp_size - 1, SMALL_SPEC[1], lanes), F32), pltpu.VMEM((cp_size, SMALL_SPEC[1], lanes), F32)]
    scratch += [dma(shape) for shape in ((n, 4), (n, 2), (n, 1), (n, cp_size - 1), (n, cp_size - 1))] * 2 + [dma((3 + 2 * (cp_size - 1),))] * 2
    return scratch


def per_seq(*shape):
    return pl.BlockSpec((1,) + shape, lambda b: (b,) + (0,) * len(shape))


def whole(*shape):
    return pl.BlockSpec(shape, lambda b: (0,) * len(shape))


SMEM = pl.BlockSpec(memory_space=pltpu.SMEM)


def sds(shape, dtype):
    return jax.ShapeDtypeStruct(shape, dtype)


def call(kernel, grid, in_specs, out_specs, out_shape, scratch, flops, name, **params):
    return pl.pallas_call(
        kernel, grid=(grid,), in_specs=in_specs, out_specs=out_specs, out_shape=out_shape, scratch_shapes=scratch, name=name,
        cost_estimate=pl.CostEstimate(flops=flops, bytes_accessed=50_000_000, transcendentals=10_000_000),
        compiler_params=pltpu.CompilerParams(dimension_semantics=('arbitrary',), vmem_limit_bytes=58 * 1024 * 1024, **params))


def gather_kernel(cp_size, n_arr, *refs):
    ins, tok_in = refs[:n_arr], refs[n_arr]
    outs, tok_out = refs[n_arr + 1:2 * n_arr + 1], refs[2 * n_arr + 1]
    send, recv, tok_send, tok_recv = refs[2 * n_arr + 2:]
    me = lax.axis_index('cp')
    fs = lax.axis_index('fsdp')
    y, x, c = place(fs)
    near, xn, yn = fs + 1 - 2 * c, fs + 2 - 4 * x, fs + 4 - 8 * y
    dg = xn + 4 - 8 * y
    first = xn * (1 - c) + yn * c
    other = yn * (1 - c) + xn * c
    cps = [lax.rem(me + k, cp_size) for k in range(1, cp_size)]
    enter([device(me, near), device(me, xn), device(me, yn)] + [device(z, fs) for z in cps])

    sent = []

    def push(a, src, slot, peer, lane):
        copy = remote(src, outs[a].at[slot], send.at[a, lane], recv.at[a, slot], device(me, peer))
        copy.start()
        sent.append(copy)

    def arrived(a, slot):
        remote(ins[a], outs[a].at[slot], send.at[a, 0], recv.at[a, slot], device(me, near)).wait_recv()

    for k in range(1, cp_size):
        copy = remote(tok_in.at[cps[k - 1]], tok_out.at[k], tok_send.at[k], tok_recv.at[k], device(cps[k - 1], fs))
        copy.start()
        sent.append(copy)
    for a in range(n_arr):
        push(a, ins[a], fs, xn, 0)
        push(a, ins[a], fs, yn, 1)
        push(a, ins[a], fs, near, 2)
    for a in range(n_arr):
        outs[a][fs] = ins[a][...]
    tok_out[0] = tok_in[me]
    for a in range(n_arr):
        arrived(a, first)
        push(a, outs[a].at[first], first, other, 3)
        push(a, outs[a].at[first], first, near, 4)
    for a in range(n_arr):
        arrived(a, other)
        push(a, outs[a].at[other], other, near, 5)
    for a in range(n_arr):
        arrived(a, dg)
        push(a, outs[a].at[dg], dg, near, 6)
    for a in range(n_arr):
        arrived(a, near)
        for slot in (xn, yn, dg):
            arrived(a, slot + 1 - 2 * c)
    for k in range(1, cp_size):
        remote(tok_in.at[0], tok_out.at[k], tok_send.at[k], tok_recv.at[k], device(me, near)).wait_recv()
    for copy in sent:
        copy.wait_send()


def gather_call(cp_size, arrays, tok):
    n_arr = len(arrays)
    pieces = 8
    vmem = pl.BlockSpec(memory_space=pltpu.VMEM)
    dma = pltpu.SemaphoreType.DMA
    return pl.pallas_call(
        functools.partial(gather_kernel, cp_size, n_arr),
        out_shape=[sds((pieces,) + arr.shape, arr.dtype) for arr in arrays] + [sds(tok.shape, tok.dtype)],
        in_specs=[vmem] * (n_arr + 1), out_specs=[vmem] * (n_arr + 1),
        scratch_shapes=[dma((n_arr, 7)), dma((n_arr, pieces)), dma((cp_size,)), dma((cp_size,))],
        compiler_params=pltpu.CompilerParams(collective_id=0, has_side_effects=True, vmem_limit_bytes=48 * 1024 * 1024),
        name='gather',
    )(*arrays, tok)


def solution(mesh):
    cp_size = mesh.shape['cp']
    fs_size = mesh.shape['fsdp']

    def shift(k):
        return [(i, (i + k) % cp_size) for i in range(cp_size)]

    def local_step(tokens, lengths, embed_table, layer_vecs, w_qkv, w_out, w_up, b_up, w_down, grad_out):
        n_loc, seq_loc = tokens.shape
        n_seq = n_loc // cp_size
        me = lax.axis_index('cp')
        fs = lax.axis_index('fsdp')

        def to_whole(arr):
            blocks = []
            for k in range(cp_size):
                dest = (me + k) % cp_size
                blk = lax.dynamic_slice_in_dim(arr, dest * n_seq, n_seq, 0)
                blocks.append(lax.ppermute(blk, 'cp', shift(k)) if k else blk)
            return blocks

        g_blocks = to_whole(grad_out)
        len_w = lax.dynamic_slice_in_dim(lengths, me * n_seq, n_seq, 0)
        small = jnp.concatenate([layer_vecs, b_up.reshape(F // D, D // fs_size)], axis=0)
        small = jnp.pad(small, ((0, SM_ROWS - small.shape[0]), (0, LANES - small.shape[1])))
        qkv_p, out_p, up_p, down_p, small_p, tok_p = gather_call(cp_size, [w_qkv.reshape(-1, 3 * D), w_out, w_up, w_down, small], tokens.reshape(cp_size, n_seq, seq_loc))
        down_w = down_p.reshape(F, D)
        tok_w = tok_p.transpose(1, 0, 2).reshape(n_seq, 1, SEQ)
        emb_t = jnp.pad(embed_table, ((0, VOCAB_PAD - embed_table.shape[0]), (0, 0))).T

        lane = jnp.arange(SEQ)
        positions = ((me - lane // seq_loc + cp_size) % cp_size) * seq_loc + lane % seq_loc
        inv_freq = 1.0 / (ROPE_BASE ** (jnp.arange(0, HEAD_DIM, 2, dtype=F32) / HEAD_DIM))
        angles = inv_freq[:, None] * positions.astype(F32)[None, :]
        cos_t, sin_t = jnp.cos(angles), jnp.sin(angles)
        me_arr = me.reshape(1).astype(jnp.int32)

        S = SEQ
        blk_spec = per_seq(seq_loc, D)
        outs = call(
            functools.partial(fwd_kernel, cp_size, seq_loc), n_seq,
            [SMEM, SMEM, per_seq(1, S), whole(D, VOCAB_PAD), whole(*small_p.shape), whole(*qkv_p.shape), whole(*out_p.shape), whole(*up_p.shape), whole(F, D), whole(8, S), whole(8, S)],
            [blk_spec] * 4 + [per_seq(D, S), per_seq(D, S), per_seq(8, S), per_seq(3 * D, S), per_seq(N_HEADS, 1, S), per_seq(D, S), per_seq(D, S), per_seq(D, S), per_seq(F, S), per_seq(F, S), whole(D, SM_ROWS), whole(D, 3 * D), whole(D, D), whole(D, F)],
            [sds((n_seq, seq_loc, D), BF)] * 4 + [sds((n_seq, D, S), BF), sds((n_seq, D, S), F32), sds((n_seq, 8, S), F32), sds((n_seq, 3 * D, S), BF), sds((n_seq, N_HEADS, 1, S), F32), sds((n_seq, D, S), F32), sds((n_seq, D, S), F32), sds((n_seq, D, S), BF), sds((n_seq, F, S), BF), sds((n_seq, F, S), F32), sds((D, SM_ROWS), F32), sds((D, 3 * D), BF), sds((D, D), BF), sds((D, F), BF)],
            [pltpu.VMEM((3 * D, D), BF), pltpu.VMEM((D, D), BF), pltpu.VMEM((F, D), BF), pltpu.VMEM((D, F), BF), pltpu.VMEM((N_TILES, S, LANES), BF), pltpu.VMEM((N_TILES * LANES, S), BF), pltpu.VMEM((S, S), F32), pltpu.VMEM((9, D, LANES), F32), pltpu.VMEM((F, LANES), F32)],
            9_000_000_000, 'fwd',
        )(len_w, me_arr, tok_w, emb_t, small_p, qkv_p, out_p, up_p, down_w, cos_t, sin_t)
        out_blocks = outs[:4]
        h, xhat1, stat, qkv, lse, attn, xhat2, a, gelu, dgelu, vecs_t, qkv_w, out_w, up_w = outs[4:]

        dres, dattn, dw_down, dw_uo, dvec2 = call(
            functools.partial(ffn_bwd_kernel, n_seq, seq_loc), n_seq,
            [blk_spec] * 4 + [whole(D, SM_ROWS), whole(F, D), whole(D, F), whole(D, D), per_seq(F, S), per_seq(F, S), per_seq(D, S), per_seq(D, S), per_seq(8, S), per_seq(D, S)],
            [per_seq(D, S), per_seq(D, S), whole(F, D), whole(D, UO_PAD), whole(8, N_TILES * LANES)],
            [sds((n_seq, D, S), F32), sds((n_seq, D, S), F32), sds((F, D), F32), sds((D, UO_PAD), F32), sds((8, N_TILES * LANES), F32)],
            [pltpu.VMEM((F, LANES), F32), pltpu.VMEM((4, D, LANES), F32)],
            9_000_000_000, 'ffn_bwd',
        )(*g_blocks, vecs_t, down_w, up_w, out_w, gelu, dgelu, a, xhat2, stat, attn)

        rows = D // fs_size
        shapes = [(F // fs_size, D), (rows, UO_PAD), (rows, QKV_HALF), (rows, QKV_HALF)]
        small_shape = (SMALL_ROWS, N_TILES * LANES)
        acc_q = pltpu.VMEM((fs_size, rows, QKV_HALF), F32)
        r_down, r_uo, r_qa, r_qb, packed = call(
            functools.partial(attn_bwd_kernel, n_seq, cp_size, seq_loc), n_seq,
            [SMEM, SMEM, per_seq(1, S), whole(D, SM_ROWS), whole(D, 3 * D), whole(8, S), whole(8, S), per_seq(3 * D, S), per_seq(N_HEADS, 1, S), per_seq(D, S), per_seq(D, S), per_seq(D, S), per_seq(D, S), per_seq(D, S), per_seq(8, S),
             whole(fs_size, *shapes[0]), whole(fs_size, *shapes[1]), whole(8, N_TILES * LANES)],
            [whole(*sh) for sh in shapes] + [whole(*small_shape)],
            [sds(sh, F32) for sh in shapes] + [sds(small_shape, F32)],
            [pltpu.VMEM((N_TILES, S, LANES), BF), pltpu.VMEM((N_TILES, S, LANES), BF), pltpu.VMEM((N_TILES * LANES, S), BF), pltpu.VMEM((N_TILES * LANES, S), BF), pltpu.VMEM((S, S), F32),
             pltpu.VMEM((D, S), F32), pltpu.VMEM((D, S), F32), pltpu.VMEM((D, S), F32), pltpu.VMEM((3, D, LANES), F32), pltpu.VMEM((2, D, LANES), F32), acc_q, acc_q, pltpu.VMEM((VOCAB_PAD, D), F32)] + sum_scratch(cp_size, shapes, small_shape),
            9_000_000_000, 'attn_bwd', collective_id=1, has_side_effects=True,
        )(len_w, me_arr, tok_w, vecs_t, qkv_w, cos_t, sin_t, qkv, lse, attn, dattn, dres, xhat1, h, stat, dw_down.reshape(fs_size, *shapes[0]), dw_uo.reshape(fs_size, *shapes[1]), dvec2)

        layer_out = jnp.zeros((n_loc, seq_loc, D), BF)
        for k in range(cp_size):
            back = lax.ppermute(out_blocks[k], 'cp', shift(-k)) if k else out_blocks[0]
            layer_out = lax.dynamic_update_slice_in_dim(layer_out, back, ((me + k) % cp_size) * n_seq, 0)

        vocab = embed_table.shape[0]
        d_vecs = jnp.concatenate([packed[EMB_ROWS:EMB_ROWS + 5], packed[EMB_ROWS + 8:EMB_ROWS + 12]], axis=0)
        d_vecs = lax.dynamic_slice_in_dim(d_vecs, fs * (D // fs_size), D // fs_size, 1)
        d_bup = packed[EMB_ROWS + 12:EMB_ROWS + 16, :D].reshape(F)
        d_bup = lax.dynamic_slice_in_dim(d_bup, fs * (F // fs_size), F // fs_size, 0)
        d_qkv = jnp.concatenate([r_qa, r_qb], axis=1)[:, :3 * D].reshape(w_qkv.shape)
        return (layer_out, packed[:vocab, :D], d_vecs, d_qkv, r_uo[:, F:F + D], r_uo[:, :F], d_bup, r_down)

    in_specs = (P('fsdp', 'cp'), P('fsdp'), P(), P(None, 'fsdp'), P('fsdp', None, None, None), P('fsdp', None), P('fsdp', None), P('fsdp'), P('fsdp', None), P('fsdp', 'cp', None))
    out_specs = (P('fsdp', 'cp', None), P(), P(None, 'fsdp'), P('fsdp', None, None, None), P('fsdp', None), P('fsdp', None), P('fsdp'), P('fsdp', None))
    return jax.shard_map(local_step, mesh=mesh, in_specs=in_specs, out_specs=out_specs, check_vma=False)
```

```python
import functools

import jax
import jax.numpy as jnp
from jax import lax
from jax.experimental import pallas as pl
from jax.experimental.pallas import tpu as pltpu
from jax.sharding import PartitionSpec as P

MASK_ID = 32
LN_EPS = 1e-5
ROPE_BASE = 10000.0
TRAIN_RATIO = 0.15 * 0.8
NEG_BIG = -1e30
VOCAB_PAD = 128
HEAD_DIM = 16
N_HEADS = 20
D = 320
F = 1280
SEQ = 256
LANES = 128
HEADS_PER_TILE = LANES // HEAD_DIM
N_TILES = -(-D // LANES)
HEAD_UNROLL = 4
QKV_HALF = 512
UO_PAD = 1664
SM_ROWS = 16
BF = jnp.bfloat16
F32 = jnp.float32
SQRT_HALF = 0.7071067811865476
INV_SQRT_2PI = 0.3989422804014327

NN = (((1,), (0,)), ((), ()))
NT = (((1,), (1,)), ((), ()))


def stack_rows(parts):
    return jnp.concatenate(parts, axis=0)


def col_sum(z):
    return jnp.sum(z, axis=0, keepdims=True)


def col_mean(z):
    return jnp.mean(z, axis=0, keepdims=True)


def dot(a, b, dims=NN):
    return lax.dot_general(a, b, dims, preferred_element_type=F32)


def col(vecs_t, j):
    return vecs_t[:, j:j + 1]


def rope(z, cos_t, sin_t):
    z4 = z.reshape(N_HEADS, 2, HEAD_DIM // 2, SEQ)
    lower, upper = z4[:, 0], z4[:, 1]
    new_l = lower * cos_t - upper * sin_t
    new_u = upper * cos_t + lower * sin_t
    return jnp.stack([new_l, new_u], axis=1).reshape(D, SEQ)


def key_bias(shift_base, cp_size, seq_loc, length):
    row = lax.broadcasted_iota(jnp.int32, (SEQ, LANES), 0)
    src = (shift_base - row // seq_loc + cp_size) % cp_size
    pos = src * seq_loc + row % seq_loc
    return jnp.where(pos < length, 0.0, NEG_BIG).astype(F32)


def feature_tiles(z_t):
    pad = stack_rows([z_t, jnp.zeros((N_TILES * LANES - D, SEQ), F32)])
    return [pad[t * LANES:(t + 1) * LANES].T.astype(BF) for t in range(N_TILES)]


def store_token_major(dst_ref, z_t):
    for t, part in enumerate(feature_tiles(z_t)):
        dst_ref[t] = part


def head_rows(tile, slot):
    row = lax.broadcasted_iota(jnp.int32, tile.shape, 0)
    return jnp.where(row // HEAD_DIM == slot, tile, jnp.zeros_like(tile))


def pipeline(n, stages):
    held = {}
    for turn in range(n + len(stages) - 1):
        for j in reversed(range(len(stages))):
            i = turn - j
            if 0 <= i < n:
                held[i] = stages[j](held[i], i) if j else stages[j](i)


def token_scale(tok, length, seq_loc, cp_size, me):
    lane = lax.broadcasted_iota(jnp.int32, (1, SEQ), 1)
    src = (me - lane // seq_loc + cp_size) % cp_size
    pos = src * seq_loc + lane % seq_loc
    is_mask = tok == MASK_ID
    n_mask = jnp.sum(is_mask.astype(F32), axis=1, keepdims=True)
    drop = (1.0 - TRAIN_RATIO) / (1.0 - n_mask / length.astype(F32))
    return jnp.where(is_mask | (pos >= length), 0.0, drop)


def one_hot_rows(tok):
    row = lax.broadcasted_iota(jnp.int32, (VOCAB_PAD, SEQ), 0)
    return jnp.where(row == tok, 1.0, 0.0).astype(BF)


def join_rows(ref):
    return stack_rows([ref[i].astype(F32) for i in range(ref.shape[0])]).astype(BF)


def wide(z):
    return jnp.concatenate([z, z], axis=1)


def spread_vectors(sm_ref, rows_of, dst_ref):
    pieces = sm_ref.shape[0]
    rows = D // pieces
    for i in range(pieces):
        sm_t = sm_ref[i].T
        for n, j in enumerate(rows_of):
            dst_ref[n, i * rows:(i + 1) * rows] = jnp.broadcast_to(sm_t[:rows, j:j + 1], (rows, LANES))


def normalize(z):
    cent = z - col_mean(z)
    rstd = lax.rsqrt(col_mean(cent * cent) + LN_EPS)
    return cent * rstd, rstd


class Gather:
    def __init__(self, cp_size, n_seq, ins, outs, tok_in, tok_out, g_in, g_out, sems):
        self.ins, self.outs, self.tok_in, self.tok_out, self.g_in, self.g_out = ins, outs, tok_in, tok_out, g_in, g_out
        self.send, self.recv, self.tok_send, self.tok_recv, self.g_send, self.g_recv, self.own = sems
        self.cp_size, self.n_seq = cp_size, n_seq
        self.me = lax.axis_index('cp')
        fs = self.fs = lax.axis_index('fsdp')
        y, x, c = place(fs)
        self.near, self.xn, self.yn = neighbours(fs)
        self.dg = neighbours(self.xn)[2]
        self.first = self.xn * (1 - c) + self.yn * c
        self.other = self.yn * (1 - c) + self.xn * c
        self.flip = 1 - 2 * c
        self.cps = [lax.rem(self.me + k, cp_size) for k in range(1, cp_size)]

    def enter(self):
        enter([device(self.me, f) for f in (self.near, self.xn, self.yn)] + [device(z, self.fs) for z in self.cps])

    def routes(self):
        return [(self.fs, self.xn), (self.fs, self.yn), (self.fs, self.near), (self.first, self.other), (self.first, self.near), (self.other, self.near), (self.dg, self.near)]

    def copy(self, a, lane):
        slot, peer = self.routes()[lane]
        src = self.ins[a] if lane < 3 else self.outs[a].at[slot]
        return remote(src, self.outs[a].at[slot], self.send.at[a, lane], self.recv.at[a, slot], device(self.me, peer))

    def push(self, arrays, lanes):
        for a in arrays:
            for lane in lanes:
                self.copy(a, lane).start()

    def arrived(self, arrays, slots):
        for a in arrays:
            for slot in slots:
                remote(self.ins[a], self.outs[a].at[slot], self.send.at[a, 0], self.recv.at[a, slot], device(self.me, self.near)).wait_recv()

    def begin(self, arrays):
        self.push(arrays, (0, 1, 2))
        for a in arrays:
            self.outs[a][self.fs] = self.ins[a][...]

    def relay(self, arrays):
        self.arrived(arrays, [self.first])
        self.push(arrays, (3, 4))
        self.arrived(arrays, [self.other])
        self.push(arrays, (5,))

    def relay_last(self, arrays):
        self.arrived(arrays, [self.dg])
        self.push(arrays, (6,))

    def complete(self, arrays):
        self.arrived(arrays, [self.near] + [slot + self.flip for slot in (self.xn, self.yn, self.dg)])

    def sent(self, arrays):
        for a in arrays:
            for lane in range(7):
                self.copy(a, lane).wait_send()

    def blocks(self, z):
        return self.g_in.at[pl.ds(z * self.n_seq, self.n_seq)]

    def tok_copy(self, k):
        z = self.cps[k - 1]
        return remote(self.tok_in.at[z], self.tok_out.at[k], self.tok_send.at[k], self.tok_recv.at[k], device(z, self.fs))

    def g_copy(self, k):
        z = self.cps[k - 1]
        return remote(self.blocks(z), self.g_out.at[k], self.g_send.at[k], self.g_recv.at[k], device(z, self.fs))

    def own_block(self):
        return pltpu.make_async_copy(self.blocks(self.me), self.g_out.at[0], self.own)


def attn_fwd_kernel(n_steps, cp_size, seq_loc, n_arr, len_ref, emb_ref, cos_ref, sin_ref, tok_in, g_in, *refs):
    ins, refs = refs[:n_arr], refs[n_arr:]
    saved, refs = refs[:n_arr - 1], refs[n_arr - 1:]
    tok_ref, g_out, gain_ref, wqkv_n, h_ref, xhat1_ref, stat_ref, qkv_ref, lse_ref, attn_ref, wqkv_t, k_tm, q_pad, bias, vec_b, tok_s, save_sem, *refs = refs
    outs = refs[:n_arr]
    gather = Gather(cp_size, n_steps, ins, outs, tok_in, tok_s, g_in, g_out, refs[n_arr:])
    kept = outs[:1] + outs[2:]
    saves = [pltpu.make_async_copy(src, dst, save_sem.at[i]) for i, (src, dst) in enumerate(zip(kept, saved))]
    early, late = (0, 1), tuple(range(2, n_arr))
    step = pl.program_id(0)
    me = lax.axis_index('cp')

    @pl.when(step == 0)
    def _():
        gather.enter()
        for k in range(1, cp_size):
            gather.tok_copy(k).start()
        gather.begin(early)
        for k in range(1, cp_size):
            gather.g_copy(k).start()
        gather.own_block().start()
        tok_s[0] = tok_in[me]
        q_pad[...] = jnp.zeros_like(q_pad)
        gather.relay(early)
        gather.begin(late)
        gather.relay_last(early)
        gather.complete(early)
        joined = join_rows(outs[1])
        wqkv_n[...] = joined
        wqkv_t[...] = joined.T
        pieces = outs[0].shape[0]
        rows = D // pieces
        for i in range(pieces):
            gain_ref[i * rows:(i + 1) * rows] = outs[0][i].T[:rows]
        spread_vectors(outs[0], range(5), vec_b)
        for k in range(1, cp_size):
            gather.tok_copy(k).wait()

    @pl.when(step == 2)
    def _():
        gather.relay(late)

    @pl.when(step == 4)
    def _():
        gather.relay_last(late)

    @pl.when(step == 6)
    def _():
        gather.complete(late)
        for copy in saves:
            copy.start()

    length = len_ref[step]
    tok = jnp.concatenate([tok_s[k, pl.ds(step, 1), :] for k in range(cp_size)], axis=1)
    tok_ref[0] = tok
    keep = token_scale(tok, length, seq_loc, cp_size, me)
    e = dot(emb_ref[...], one_hot_rows(tok)) * keep
    xhat1, rstd1 = normalize(e)
    xhat1_ref[0] = xhat1
    h = (xhat1 * wide(vec_b[0]) + wide(vec_b[1])).astype(BF)
    h_ref[0] = h
    stat_ref[0] = stack_rows([rstd1, keep, jnp.zeros((6, SEQ), F32)])
    cos_t, sin_t = cos_ref[...], sin_ref[...]
    q = (dot(wqkv_t[0:D], h) + wide(vec_b[2])) * HEAD_DIM ** -0.5
    q = rope(q, cos_t, sin_t).astype(BF)
    qkv_ref[0, 0:D] = q
    q_pad[0:D] = q
    k = rope(dot(wqkv_t[D:2 * D], h) + wide(vec_b[3]), cos_t, sin_t)
    qkv_ref[0, D:2 * D] = k.astype(BF)
    store_token_major(k_tm, k)
    qkv_ref[0, 2 * D:3 * D] = (dot(wqkv_t[2 * D:3 * D], h) + wide(vec_b[4])).astype(BF)
    bias[...] = key_bias(me, cp_size, seq_loc, length)

    def scores(hd):
        tile, slot = hd // HEADS_PER_TILE, hd % HEADS_PER_TILE
        return dot(k_tm[tile], head_rows(q_pad[tile * LANES:(tile + 1) * LANES, :], slot))

    def weights(s, hd):
        s = s + wide(bias[...])
        m = jnp.max(s, axis=0, keepdims=True)
        p = jnp.exp(s - m)
        l = col_sum(p)
        lse_ref[0, hd] = m + jnp.log(l)
        return p.astype(BF), l

    def attend(pair, hd):
        p, l = pair
        lo = hd * HEAD_DIM
        attn_ref[0, lo:lo + HEAD_DIM] = dot(qkv_ref[0, 2 * D + lo:2 * D + lo + HEAD_DIM, :], p) / l

    pipeline(N_HEADS, (scores, weights, attend))

    @pl.when(step == n_steps - 1)
    def _():
        gather.sent(early + late)
        for copy in saves:
            copy.wait()
        for k in range(1, cp_size):
            gather.g_copy(k).wait()
        gather.own_block().wait()


def to_token_major(z_t):
    return jnp.concatenate(feature_tiles(z_t), axis=1)[:, :D]


def to_feature_major(z):
    z32 = z.astype(F32)
    pad = jnp.concatenate([z32, jnp.zeros((SEQ, N_TILES * LANES - D), F32)], axis=1)
    return stack_rows([pad[:, t * LANES:(t + 1) * LANES].T for t in range(N_TILES)])[:D]


def lane_part(z):
    return z[:, :LANES] + z[:, LANES:]


def ln_grad(dn, xhat, rstd, gain):
    dxh = dn * gain
    m1 = col_mean(dxh)
    m2 = col_mean(dxh * xhat)
    return rstd * (dxh - m1 - xhat * m2)


def row_sum(acc):
    return col_sum(acc.T)


class Homeward:
    def __init__(self, n_seq, seq_loc, buf, out, send, recv):
        self.n_seq, self.seq_loc, self.buf, self.out, self.send, self.recv = n_seq, seq_loc, buf, out, send, recv
        self.cp_size = n_pieces(out, n_seq)
        self.me = lax.axis_index('cp')
        self.fs = lax.axis_index('fsdp')
        self.others = range(1, self.cp_size)

    def enter(self):
        enter([device(lax.rem(self.me + k, self.cp_size), self.fs) for k in self.others])

    def copy(self, step, k):
        src = self.buf.at[lax.rem(step, 2), pl.ds(k * self.seq_loc, self.seq_loc)]
        dst = self.out.at[self.me * self.n_seq + step]
        if k == 0:
            return pltpu.make_async_copy(src, dst, self.send.at[step, k])
        return remote(src, dst, self.send.at[step, k], self.recv.at[step, k], device(lax.rem(self.me + self.cp_size - k, self.cp_size), self.fs))

    def start(self, step):
        for k in range(self.cp_size):
            self.copy(step, k).start()

    def sent(self, step):
        self.copy(step, 0).wait()
        for k in self.others:
            self.copy(step, k).wait_send()

    def arrived(self):
        for step in range(self.n_seq):
            for k in self.others:
                self.copy(step, k).wait_recv()


def n_pieces(out, n_seq):
    return out.shape[0] // n_seq


def ffn_kernel(n_steps, seq_loc, tok_ref, stat_ref, attn_ref, g_ref, emb_ref, sm_ref, wout_ref, wup_ref, wdown_ref,
               out_ref, dres_ref, dattn_ref, dwdown_ref, dwuo_ref, dvec_ref,
               wout_n, wup_n, wout_t, wup_t, wdown_t, vec_b, bup_b, dup_s, gelu_s, acc_bup, acc_vec, out_s, out_send, out_recv):
    step = pl.program_id(0)
    home = Homeward(n_steps, seq_loc, out_s, out_ref, out_send, out_recv)

    @pl.when(step == 0)
    def _():
        home.enter()
        for src, nat, tr in ((wout_ref, wout_n, wout_t), (wup_ref, wup_n, wup_t)):
            joined = join_rows(src)
            nat[...] = joined
            tr[...] = joined.T
        wdown_t[...] = wdown_ref[...].T
        spread_vectors(sm_ref, range(5, 9), vec_b)
        pieces = sm_ref.shape[0]
        rows = D // pieces
        for i in range(pieces):
            sm_t = sm_ref[i].T
            for r in range(F // D):
                lo = i * (F // pieces) + r * rows
                bup_b[lo:lo + rows] = jnp.broadcast_to(sm_t[:rows, 9 + r:10 + r], (rows, LANES))
        for acc in (dwdown_ref, dwuo_ref, acc_bup, acc_vec):
            acc[...] = jnp.zeros_like(acc)

    e = dot(emb_ref[...], one_hot_rows(tok_ref[0])) * stat_ref[0, 1:2]
    o = attn_ref[0].astype(BF)
    x1 = e + dot(wout_t[...], o) + wide(vec_b[0])
    xhat2, rstd2 = normalize(x1)
    a = (xhat2 * wide(vec_b[1]) + wide(vec_b[2])).astype(BF)
    g = stack_rows([g_ref[k, 0] for k in range(g_ref.shape[0])])
    for c in range(F // D):
        rows = slice(c * D, (c + 1) * D)
        u = dot(wup_t[rows], a) + wide(bup_b[rows])
        cdf = 0.5 * (1.0 + lax.erf(u * SQRT_HALF))
        gelu = (u * cdf).astype(BF)
        gelu_s[rows] = gelu
        dup = dot(wdown_ref[rows], g, NT) * (cdf + u * (INV_SQRT_2PI * jnp.exp(-0.5 * u * u)))
        acc_bup[rows] += lane_part(dup)
        dup_s[rows] = dup.astype(BF)
        dwdown_ref[rows] += dot(gelu, g)
    @pl.when(step >= 2)
    def _():
        home.sent(step - 2)

    out_s[lax.rem(step, 2)] = to_token_major(x1 + wide(vec_b[3]) + dot(wdown_t[...], gelu_s[...]))
    home.start(step)
    dup_b = dup_s[...]
    dwuo_ref[:, 0:F] += dot(a, dup_b, NT)
    dn2 = dot(wup_n[...], dup_b)
    g_t = to_feature_major(g)
    dres = g_t + ln_grad(dn2, xhat2, rstd2, wide(vec_b[1]))
    for j, part in enumerate((dres, dn2 * xhat2, dn2, g_t)):
        acc_vec[j] += lane_part(part)
    dres_ref[0] = dres
    dres_b = dres.astype(BF)
    dwuo_ref[:, F:F + D] += dot(o, dres_b, NT)
    dattn_ref[0] = dot(wout_n[...], dres_b)

    @pl.when(step == n_steps - 1)
    def _():
        rows = [row_sum(pad_rows(acc_vec[j])) for j in range(4)] + [row_sum(pad_rows(acc_bup[j * D:(j + 1) * D])) for j in range(F // D)]
        dvec_ref[...] = stack_rows(rows)
        home.sent(step - 1)
        home.sent(step)
        home.arrived()


def pad_rows(z):
    return stack_rows([z, jnp.zeros((N_TILES * LANES - D, LANES), F32)])


def attn_bwd_kernel(n_steps, cp_size, seq_loc, len_ref, me_ref, tok_ref, vec_ref, wqkv_ref, cos_ref, sin_ref, qkv_ref, lse_ref, attn_ref, dattn_ref, dres_ref, xhat1_ref, h_ref, stat_ref, dwdown_ref, dwuo_ref, dvec2_ref,
                    rdown_ref, ruo_ref, rqa_ref, rqb_ref, rsmall_ref,
                    k_tm, v_tm, q_pad, do_pad, bias, dq_s, dk_s, dv_s, acc_b, acc_vec, acc_qa, acc_qb, acc_emb, *red):
    step = pl.program_id(0)
    summer = GradSum(cp_size, (dwdown_ref, dwuo_ref, acc_qa, acc_qb), (rdown_ref, ruo_ref, rqa_ref, rqb_ref), rsmall_ref, red)

    @pl.when(step == 0)
    def _():
        summer.enter()
        for i in (0, 1):
            summer.start(0, i)
        acc_qa[...] = jnp.zeros_like(acc_qa)
        acc_qb[...] = jnp.zeros_like(acc_qb)
        acc_emb[...] = jnp.zeros_like(acc_emb)
        acc_b[...] = jnp.zeros_like(acc_b)
        acc_vec[...] = jnp.zeros_like(acc_vec)
        q_pad[...] = jnp.zeros_like(q_pad)
        do_pad[...] = jnp.zeros_like(do_pad)

    for phase, at in enumerate(PHASE_STEPS):
        @pl.when(step == at)
        def _(phase=phase):
            for i in (0, 1):
                summer.finish(phase, i)
                summer.start(phase + 1, i)

    length = len_ref[step]
    me = me_ref[0]
    vecs = vec_ref[...]
    q_pad[0:D] = qkv_ref[0, 0:D]
    do_pad[0:D] = dattn_ref[0].astype(BF)
    store_token_major(k_tm, qkv_ref[0, D:2 * D].astype(F32))
    store_token_major(v_tm, qkv_ref[0, 2 * D:3 * D].astype(F32))
    bias[...] = key_bias(me, cp_size, seq_loc, length)

    def products(hd):
        tile, slot = hd // HEADS_PER_TILE, hd % HEADS_PER_TILE
        t0 = slice(tile * LANES, (tile + 1) * LANES)
        return dot(k_tm[tile], head_rows(q_pad[t0, :], slot)), dot(v_tm[tile], head_rows(do_pad[t0, :], slot))

    def weights(pair, hd):
        s, dp = pair
        rows = slice(hd * HEAD_DIM, (hd + 1) * HEAD_DIM)
        delta = col_sum(dattn_ref[0, rows, :] * attn_ref[0, rows, :])
        p = jnp.exp((s + wide(bias[...])) - lse_ref[0, hd])
        return p.astype(BF), (p * (dp - delta)).astype(BF)

    def gradients(pair, hd):
        p, ds = pair
        rows = slice(hd * HEAD_DIM, (hd + 1) * HEAD_DIM)
        dq_s[rows, :] = dot(qkv_ref[0, D + hd * HEAD_DIM:D + (hd + 1) * HEAD_DIM, :], ds)
        dk_s[rows, :] = dot(q_pad[rows, :], ds, NT)
        dv_s[rows, :] = dot(do_pad[rows, :], p, NT)

    pipeline(N_HEADS, (products, weights, gradients))

    cos_t, sin_t = cos_ref[...], sin_ref[...]
    h = h_ref[0]
    dq = rope(dq_s[...], cos_t, -sin_t) * HEAD_DIM ** -0.5
    dk = rope(dk_s[...], cos_t, -sin_t)
    dv = dv_s[...]
    dn1 = jnp.zeros((D, SEQ), F32)
    parts = []
    for j, dz in enumerate((dq, dk, dv)):
        acc_b[j] += lane_part(dz)
        parts.append(dz.astype(BF))
    dz_b = stack_rows(parts)
    acc_qa[...] += dot(h, dz_b[:QKV_HALF], NT).reshape(acc_qa.shape)
    acc_qb[:, :, :3 * D - QKV_HALF] += dot(h, dz_b[QKV_HALF:], NT).reshape(acc_qb.shape[0], acc_qb.shape[1], 3 * D - QKV_HALF)
    dn1 = dot(wqkv_ref[...], dz_b)
    xhat1 = xhat1_ref[0]
    acc_vec[0] += lane_part(dn1 * xhat1)
    acc_vec[1] += lane_part(dn1)
    de = dres_ref[0] + ln_grad(dn1, xhat1, stat_ref[0, 0:1], col(vecs, 0))
    de = (de * stat_ref[0, 1:2]).astype(BF)
    acc_emb[...] += dot(one_hot_rows(tok_ref[0]), de, NT)

    @pl.when(step == n_steps - 1)
    def _():
        for i in (2, 3):
            summer.start(0, i)
        rows = [row_sum(pad_rows(acc_vec[j])) for j in range(2)] + [row_sum(pad_rows(acc_b[j])) for j in range(3)]
        small = summer.small
        small[...] = jnp.zeros_like(small)
        small[:EMB_ROWS, :D] = acc_emb[:EMB_ROWS]
        small[EMB_ROWS:EMB_ROWS + len(rows)] = stack_rows(rows)
        small[EMB_ROWS + 8:EMB_ROWS + 16] = dvec2_ref[...]
        summer.start_small(0)
        for phase in range(5):
            for i in (2, 3):
                summer.finish(phase, i)
                if phase < 4:
                    summer.start(phase + 1, i)
            summer.finish_small(phase)
            if phase < 4:
                summer.start_small(phase + 1)
        for i in (0, 1):
            summer.finish(4, i)


MESH = pl.DeviceIdType.MESH
EMB_ROWS = 40
SMALL_ROWS = 64
PHASE_STEPS = (1, 3, 4, 6)
STREAMS = (('xy', (0, 40, 40)), ('yx', (1, 512, 384)), ('xy', (1, 128, 128)), ('yx', (1, 128, 128)))
SMALL_SPEC = (0, SMALL_ROWS // 4, SMALL_ROWS // 4)


def neighbours(fs):
    y, x, c = place(fs)
    return fs + 1 - 2 * c, fs + 2 - 4 * x, fs + 4 - 8 * y


def place(fs):
    return fs // 4, (fs // 2) % 2, fs % 2


def device(cp, fs):
    return {'cp': cp, 'fsdp': fs}


def enter(peers):
    barrier = pltpu.get_barrier_semaphore()
    for peer in peers:
        pl.semaphore_signal(barrier, inc=1, device_id=peer, device_id_type=MESH)
    pl.semaphore_wait(barrier, len(peers))


def remote(src, dst, send_sem, recv_sem, peer):
    return pltpu.make_async_remote_copy(src_ref=src, dst_ref=dst, send_sem=send_sem, recv_sem=recv_sem, device_id=peer, device_id_type=MESH)


def piece_of(ref, spec, p):
    axis, size, stride = spec
    start = pl.multiple_of(p * stride, stride)
    return ref.at[pl.ds(start, size), :] if axis == 0 else ref.at[:, pl.ds(start, size)]


class GradSum:
    def __init__(self, cp_size, big, outs, small_out, refs):
        n = len(STREAMS)
        self.cp_size, self.big, self.outs, self.small_out = cp_size, big, outs, small_out
        self.r0, self.acc, self.r1, self.r2, self.rz, self.rg = (refs[i * n:(i + 1) * n] for i in range(6))
        self.small, self.er, self.ez, self.eg = refs[6 * n:6 * n + 4]
        sems = refs[6 * n + 4:]
        self.sends, self.recvs = sems[0:5], sems[5:10]
        self.small_send, self.small_recv = sems[10], sems[11]
        self.me = lax.axis_index('cp')
        self.fs = lax.axis_index('fsdp')
        self.y, self.x, self.c = place(self.fs)
        fs, y, x, c = self.fs, self.y, self.x, self.c
        self.cps = [lax.rem(self.me + k, cp_size) for k in range(1, cp_size)]
        self.hops = [device(self.me, f) for f in neighbours(fs)]
        self.peers = [device(z, fs) for z in self.cps]

    def enter(self):
        enter(self.hops + self.peers)

    def copies(self, phase, i):
        path, spec = STREAMS[i]
        xy = path == 'xy'
        s, v = self.sends[phase], self.recvs[phase]
        x, y, c, me = self.x, self.y, self.c, self.me
        if phase == 0:
            return [remote(self.big[i].at[2 * j + 1 - c], self.r0[i].at[j], s.at[i, j], v.at[i, j], self.hops[0]) for j in range(4)]
        if phase == 1:
            give = [2 * k + 1 - x if xy else 2 * (1 - y) + k for k in range(2)]
            return [remote(self.acc[i].at[give[k]], self.r1[i].at[k], s.at[i, k], v.at[i, k], self.hops[1 if xy else 2]) for k in range(2)]
        if phase == 2:
            return [remote(self.r1[i].at[1 - y if xy else 1 - x], self.r2[i], s.at[i, 0], v.at[i, 0], self.hops[2 if xy else 1])]
        if phase == 3:
            return [remote(piece_of(self.outs[i], spec, self.cps[k]), self.rz[i].at[k], s.at[i, k], v.at[i, k], self.peers[k]) for k in range(self.cp_size - 1)]
        return [remote(self.rg[i].at[me], self.rg[i].at[me], s.at[i, k], v.at[i, k], self.peers[k]) for k in range(self.cp_size - 1)]

    def start(self, phase, i):
        for copy in self.copies(phase, i):
            copy.start()

    def finish(self, phase, i):
        for copy in self.copies(phase, i):
            copy.wait()
        path, spec = STREAMS[i]
        xy = path == 'xy'
        big, r0, acc, r1, r2, out = self.big[i], self.r0[i], self.acc[i], self.r1[i], self.r2[i], self.outs[i]
        rz, rg = self.rz[i], self.rg[i]
        if phase == 0:
            for j in range(4):
                acc[j] = big[2 * j + self.c] + r0[j]
        elif phase == 1:
            for k in range(2):
                r1[k] = acc[2 * k + self.x if xy else 2 * self.y + k] + r1[k]
        elif phase == 2:
            out[...] = r1[self.y if xy else self.x] + r2[...]
        elif phase == 3:
            rg[self.me] = ((piece_of(out, spec, self.me)[...] + rz[0]) + rz[1]) + rz[2]
        else:
            axis, size, stride = spec
            for p in range(self.cp_size):
                lo = p * stride
                if axis == 0:
                    out[lo:lo + size, :] = rg[p]
                else:
                    out[:, lo:lo + size] = rg[p]

    def small_copies(self, phase):
        s, v = self.small_send, self.small_recv
        if phase < 3:
            return [remote(self.small, self.er.at[phase], s.at[phase], v.at[phase], self.hops[phase])]
        if phase == 3:
            return [remote(piece_of(self.small, SMALL_SPEC, self.cps[k]), self.ez.at[k], s.at[3 + k], v.at[3 + k], self.peers[k]) for k in range(self.cp_size - 1)]
        return [remote(self.eg.at[self.me], self.eg.at[self.me], s.at[6 + k], v.at[6 + k], self.peers[k]) for k in range(self.cp_size - 1)]

    def start_small(self, phase):
        for copy in self.small_copies(phase):
            copy.start()

    def finish_small(self, phase):
        for copy in self.small_copies(phase):
            copy.wait()
        if phase < 3:
            self.small[...] += self.er[phase]
        elif phase == 3:
            self.eg[self.me] = ((piece_of(self.small, SMALL_SPEC, self.me)[...] + self.ez[0]) + self.ez[1]) + self.ez[2]
        else:
            size = SMALL_SPEC[1]
            for p in range(self.cp_size):
                self.small_out[p * size:(p + 1) * size, :] = self.eg[p]


def sum_scratch(cp_size, shapes, small_shape):
    dma = pltpu.SemaphoreType.DMA
    n = len(shapes)
    cut = [((size, sh[1]) if axis == 0 else (sh[0], size)) for sh, (_, (axis, size, _)) in zip(shapes, STREAMS)]
    lanes = small_shape[1]
    scratch = [pltpu.VMEM((4,) + sh, F32) for sh in shapes] * 2 + [pltpu.VMEM((2,) + sh, F32) for sh in shapes] + [pltpu.VMEM(sh, F32) for sh in shapes]
    scratch += [pltpu.VMEM((cp_size - 1,) + sh, F32) for sh in cut] + [pltpu.VMEM((cp_size,) + sh, F32) for sh in cut]
    scratch += [pltpu.VMEM(small_shape, F32), pltpu.VMEM((3,) + small_shape, F32), pltpu.VMEM((cp_size - 1, SMALL_SPEC[1], lanes), F32), pltpu.VMEM((cp_size, SMALL_SPEC[1], lanes), F32)]
    scratch += [dma(shape) for shape in ((n, 4), (n, 2), (n, 1), (n, cp_size - 1), (n, cp_size - 1))] * 2 + [dma((3 + 2 * (cp_size - 1),))] * 2
    return scratch


def per_seq(*shape):
    return pl.BlockSpec((1,) + shape, lambda b: (b,) + (0,) * len(shape))


def whole(*shape):
    return pl.BlockSpec(shape, lambda b: (0,) * len(shape))


SMEM = pl.BlockSpec(memory_space=pltpu.SMEM)


def sds(shape, dtype):
    return jax.ShapeDtypeStruct(shape, dtype)


def call(kernel, grid, in_specs, out_specs, out_shape, scratch, flops, name, **params):
    return pl.pallas_call(
        kernel, grid=(grid,), in_specs=in_specs, out_specs=out_specs, out_shape=out_shape, scratch_shapes=scratch, name=name,
        cost_estimate=pl.CostEstimate(flops=flops, bytes_accessed=50_000_000, transcendentals=10_000_000),
        compiler_params=pltpu.CompilerParams(dimension_semantics=('arbitrary',), vmem_limit_bytes=58 * 1024 * 1024, **params))


def solution(mesh):
    cp_size = mesh.shape['cp']
    fs_size = mesh.shape['fsdp']

    def local_step(tokens, lengths, embed_table, layer_vecs, w_qkv, w_out, w_up, b_up, w_down, grad_out):
        n_loc, seq_loc = tokens.shape
        n_seq = n_loc // cp_size
        me = lax.axis_index('cp')
        fs = lax.axis_index('fsdp')

        len_w = lax.dynamic_slice_in_dim(lengths, me * n_seq, n_seq, 0)
        small = stack_rows([layer_vecs, b_up.reshape(F // D, D // fs_size)])
        small = jnp.pad(small, ((0, SM_ROWS - small.shape[0]), (0, LANES - small.shape[1])))
        shards = [small, w_qkv.reshape(-1, 3 * D), w_out, w_up, w_down]
        full = [(fs_size,) + arr.shape for arr in shards]
        emb_t = jnp.pad(embed_table, ((0, VOCAB_PAD - embed_table.shape[0]), (0, 0))).T

        lane = jnp.arange(SEQ)
        positions = ((me - lane // seq_loc + cp_size) % cp_size) * seq_loc + lane % seq_loc
        inv_freq = 1.0 / (ROPE_BASE ** (jnp.arange(0, HEAD_DIM, 2, dtype=F32) / HEAD_DIM))
        angles = inv_freq[:, None] * positions.astype(F32)[None, :]
        cos_t, sin_t = jnp.cos(angles), jnp.sin(angles)
        me_arr = me.reshape(1).astype(jnp.int32)

        S = SEQ
        dma = pltpu.SemaphoreType.DMA
        vmem = pl.BlockSpec(memory_space=pltpu.VMEM)
        hbm = pl.BlockSpec(memory_space=pl.ANY)
        n_arr = len(shards)
        kept = [0] + list(range(2, n_arr))
        g_shape = (cp_size, n_seq, seq_loc, D)
        per_feature = per_seq(D, S)
        tok = tokens.reshape(cp_size, n_seq, seq_loc)
        outs = call(
            functools.partial(attn_fwd_kernel, n_seq, cp_size, seq_loc, n_arr), n_seq,
            [SMEM, whole(D, VOCAB_PAD), whole(8, S), whole(8, S), vmem, hbm] + [vmem] * n_arr,
            [hbm] * len(kept) + [per_seq(1, S), hbm, whole(D, SM_ROWS), whole(D, 3 * D), per_feature, per_feature, per_seq(8, S), per_seq(3 * D, S), per_seq(N_HEADS, 1, S), per_feature],
            [sds(full[i], shards[i].dtype) for i in kept] + [sds((n_seq, 1, S), jnp.int32), sds(g_shape, BF), sds((D, SM_ROWS), F32), sds((D, 3 * D), BF), sds((n_seq, D, S), BF), sds((n_seq, D, S), F32), sds((n_seq, 8, S), F32), sds((n_seq, 3 * D, S), BF), sds((n_seq, N_HEADS, 1, S), F32), sds((n_seq, D, S), F32)],
            [pltpu.VMEM((3 * D, D), BF), pltpu.VMEM((N_TILES, S, LANES), BF), pltpu.VMEM((N_TILES * LANES, S), BF), pltpu.VMEM((S, LANES), F32), pltpu.VMEM((5, D, LANES), F32), pltpu.VMEM(tok.shape, jnp.int32), dma((len(kept),))] + [pltpu.VMEM(sh, arr.dtype) for sh, arr in zip(full, shards)] + [
             dma((n_arr, 7)), dma((n_arr, fs_size)), dma((cp_size,)), dma((cp_size,)), dma((cp_size,)), dma((cp_size,)), dma],
            4_000_000_000, 'attn_fwd', collective_id=0, has_side_effects=True,
        )(len_w, emb_t, cos_t, sin_t, tok, grad_out, *shards)
        small_p, out_p, up_p, down_p, tok_w, g_w, vecs_t, qkv_w, h, xhat1, stat, qkv, lse, attn = outs

        outs = call(
            functools.partial(ffn_kernel, n_seq, seq_loc), n_seq,
            [per_seq(1, S), per_seq(8, S), per_feature, pl.BlockSpec((cp_size, 1, seq_loc, D), lambda b: (0, b, 0, 0)), whole(D, VOCAB_PAD), whole(*full[0]), whole(*full[2]), whole(*full[3]), whole(F, D)],
            [hbm, per_feature, per_feature, whole(F, D), whole(D, UO_PAD), whole(8, N_TILES * LANES)],
            [sds(grad_out.shape, BF), sds((n_seq, D, S), F32), sds((n_seq, D, S), F32), sds((F, D), F32), sds((D, UO_PAD), F32), sds((8, N_TILES * LANES), F32)],
            [pltpu.VMEM((D, D), BF), pltpu.VMEM((D, F), BF), pltpu.VMEM((D, D), BF), pltpu.VMEM((F, D), BF), pltpu.VMEM((D, F), BF), pltpu.VMEM((4, D, LANES), F32), pltpu.VMEM((F, LANES), F32),
             pltpu.VMEM((F, S), BF), pltpu.VMEM((F, S), BF), pltpu.VMEM((F, LANES), F32), pltpu.VMEM((4, D, LANES), F32), pltpu.VMEM((2, S, D), BF), dma((n_seq, cp_size)), dma((n_seq, cp_size))],
            9_000_000_000, 'ffn', collective_id=2, has_side_effects=True,
        )(tok_w, stat, attn, g_w, emb_t, small_p, out_p, up_p, down_p.reshape(F, D))
        layer_out, dres, dattn, dw_down, dw_uo, dvec2 = outs

        rows = D // fs_size
        shapes = [(F // fs_size, D), (rows, UO_PAD), (rows, QKV_HALF), (rows, QKV_HALF)]
        small_shape = (SMALL_ROWS, N_TILES * LANES)
        acc_q = pltpu.VMEM((fs_size, rows, QKV_HALF), F32)
        r_down, r_uo, r_qa, r_qb, packed = call(
            functools.partial(attn_bwd_kernel, n_seq, cp_size, seq_loc), n_seq,
            [SMEM, SMEM, per_seq(1, S), whole(D, SM_ROWS), whole(D, 3 * D), whole(8, S), whole(8, S), per_seq(3 * D, S), per_seq(N_HEADS, 1, S), per_seq(D, S), per_seq(D, S), per_seq(D, S), per_seq(D, S), per_seq(D, S), per_seq(8, S),
             whole(fs_size, *shapes[0]), whole(fs_size, *shapes[1]), whole(8, N_TILES * LANES)],
            [whole(*sh) for sh in shapes] + [whole(*small_shape)],
            [sds(sh, F32) for sh in shapes] + [sds(small_shape, F32)],
            [pltpu.VMEM((N_TILES, S, LANES), BF), pltpu.VMEM((N_TILES, S, LANES), BF), pltpu.VMEM((N_TILES * LANES, S), BF), pltpu.VMEM((N_TILES * LANES, S), BF), pltpu.VMEM((S, LANES), F32),
             pltpu.VMEM((D, S), F32), pltpu.VMEM((D, S), F32), pltpu.VMEM((D, S), F32), pltpu.VMEM((3, D, LANES), F32), pltpu.VMEM((2, D, LANES), F32), acc_q, acc_q, pltpu.VMEM((VOCAB_PAD, D), F32)] + sum_scratch(cp_size, shapes, small_shape),
            9_000_000_000, 'attn_bwd', collective_id=1, has_side_effects=True,
        )(len_w, me_arr, tok_w, vecs_t, qkv_w, cos_t, sin_t, qkv, lse, attn, dattn, dres, xhat1, h, stat, dw_down.reshape(fs_size, *shapes[0]), dw_uo.reshape(fs_size, *shapes[1]), dvec2)

        vocab = embed_table.shape[0]
        d_vecs = stack_rows([packed[EMB_ROWS:EMB_ROWS + 5], packed[EMB_ROWS + 8:EMB_ROWS + 12]])
        d_vecs = lax.dynamic_slice_in_dim(d_vecs, fs * (D // fs_size), D // fs_size, 1)
        d_bup = packed[EMB_ROWS + 12:EMB_ROWS + 16, :D].reshape(F)
        d_bup = lax.dynamic_slice_in_dim(d_bup, fs * (F // fs_size), F // fs_size, 0)
        d_qkv = jnp.concatenate([r_qa, r_qb], axis=1)[:, :3 * D].reshape(w_qkv.shape)
        return (layer_out, packed[:vocab, :D], d_vecs, d_qkv, r_uo[:, F:F + D], r_uo[:, :F], d_bup, r_down)

    in_specs = (P('fsdp', 'cp'), P('fsdp'), P(), P(None, 'fsdp'), P('fsdp', None, None, None), P('fsdp', None), P('fsdp', None), P('fsdp'), P('fsdp', None), P('fsdp', 'cp', None))
    out_specs = (P('fsdp', 'cp', None), P(), P(None, 'fsdp'), P('fsdp', None, None, None), P('fsdp', None), P('fsdp', None), P('fsdp'), P('fsdp', None))
    return jax.shard_map(local_step, mesh=mesh, in_specs=in_specs, out_specs=out_specs, check_vma=False)
```

```python
import functools

import jax
import jax.numpy as jnp
from jax import lax
from jax.experimental import pallas as pl
from jax.experimental.pallas import tpu as pltpu
from jax.sharding import PartitionSpec as P

MASK_ID = 32
LN_EPS = 1e-5
ROPE_BASE = 10000.0
TRAIN_RATIO = 0.15 * 0.8
NEG_BIG = -1e30
VOCAB_PAD = 128
HEAD_DIM = 16
N_HEADS = 20
D = 320
F = 1280
SEQ = 256
LANES = 128
HEADS_PER_TILE = LANES // HEAD_DIM
N_TILES = -(-D // LANES)
HEAD_UNROLL = 4
QKV_HALF = 512
UO_PAD = 1664
EARLY_SEQS = 5
FLOPS = 9_000_000_000
SM_ROWS = 16
BF = jnp.bfloat16
F32 = jnp.float32
SQRT_HALF = 0.7071067811865476
INV_SQRT_2PI = 0.3989422804014327

NN = (((1,), (0,)), ((), ()))
NT = (((1,), (1,)), ((), ()))


def stack_rows(parts):
    return jnp.concatenate(parts, axis=0)


def col_sum(z):
    return jnp.sum(z, axis=0, keepdims=True)


def col_mean(z):
    return jnp.mean(z, axis=0, keepdims=True)


def dot(a, b, dims=NN):
    return lax.dot_general(a, b, dims, preferred_element_type=F32)


def col(vecs_t, j):
    return vecs_t[:, j:j + 1]


def rope(z, cos_t, sin_t):
    z4 = z.reshape(N_HEADS, 2, HEAD_DIM // 2, SEQ)
    lower, upper = z4[:, 0], z4[:, 1]
    new_l = lower * cos_t - upper * sin_t
    new_u = upper * cos_t + lower * sin_t
    return jnp.stack([new_l, new_u], axis=1).reshape(D, SEQ)


def key_bias(shift_base, cp_size, seq_loc, length):
    row = lax.broadcasted_iota(jnp.int32, (SEQ, LANES), 0)
    src = (shift_base - row // seq_loc + cp_size) % cp_size
    pos = src * seq_loc + row % seq_loc
    return jnp.where(pos < length, 0.0, NEG_BIG).astype(F32)


def feature_tiles(z_t):
    pad = stack_rows([z_t, jnp.zeros((N_TILES * LANES - D, SEQ), F32)])
    return [pad[t * LANES:(t + 1) * LANES].T.astype(BF) for t in range(N_TILES)]


def store_token_major(dst_ref, z_t):
    for t, part in enumerate(feature_tiles(z_t)):
        dst_ref[t] = part


def head_rows(tile, slot):
    row = lax.broadcasted_iota(jnp.int32, tile.shape, 0)
    return jnp.where(row // HEAD_DIM == slot, tile, jnp.zeros_like(tile))


def pipeline(n, stages):
    held = {}
    for turn in range(n + len(stages) - 1):
        for j in reversed(range(len(stages))):
            i = turn - j
            if 0 <= i < n:
                held[i] = stages[j](held[i], i) if j else stages[j](i)


def token_scale(tok, length, seq_loc, cp_size, me):
    lane = lax.broadcasted_iota(jnp.int32, (1, SEQ), 1)
    src = (me - lane // seq_loc + cp_size) % cp_size
    pos = src * seq_loc + lane % seq_loc
    is_mask = tok == MASK_ID
    n_mask = jnp.sum(is_mask.astype(F32), axis=1, keepdims=True)
    drop = (1.0 - TRAIN_RATIO) / (1.0 - n_mask / length.astype(F32))
    return jnp.where(is_mask | (pos >= length), 0.0, drop)


def one_hot_rows(tok):
    row = lax.broadcasted_iota(jnp.int32, (VOCAB_PAD, SEQ), 0)
    return jnp.where(row == tok, 1.0, 0.0).astype(BF)


def join_rows(ref):
    return stack_rows([ref[i].astype(F32) for i in range(ref.shape[0])]).astype(BF)


def wide(z):
    return jnp.concatenate([z, z], axis=1)


def spread_vectors(sm_ref, rows_of, dst_ref):
    pieces = sm_ref.shape[0]
    rows = D // pieces
    for i in range(pieces):
        sm_t = sm_ref[i].T
        for n, j in enumerate(rows_of):
            dst_ref[n, i * rows:(i + 1) * rows] = jnp.broadcast_to(sm_t[:rows, j:j + 1], (rows, LANES))


def normalize(z):
    cent = z - col_mean(z)
    rstd = lax.rsqrt(col_mean(cent * cent) + LN_EPS)
    return cent * rstd, rstd


class Gather:
    def __init__(self, cp_size, n_seq, ins, outs, tok_in, tok_out, g_in, g_out, sems):
        self.ins, self.outs, self.tok_in, self.tok_out, self.g_in, self.g_out = ins, outs, tok_in, tok_out, g_in, g_out
        self.send, self.recv, self.tok_send, self.tok_recv, self.g_send, self.g_recv, self.own = sems
        self.cp_size, self.n_seq = cp_size, n_seq
        self.me = lax.axis_index('cp')
        fs = self.fs = lax.axis_index('fsdp')
        y, x, c = place(fs)
        self.near, self.xn, self.yn = neighbours(fs)
        self.dg = neighbours(self.xn)[2]
        self.first = self.xn * (1 - c) + self.yn * c
        self.other = self.yn * (1 - c) + self.xn * c
        self.flip = 1 - 2 * c
        self.cps = [lax.rem(self.me + k, cp_size) for k in range(1, cp_size)]

    def enter(self):
        enter([device(self.me, f) for f in (self.near, self.xn, self.yn)] + [device(z, self.fs) for z in self.cps])

    def routes(self):
        return [(self.fs, self.xn), (self.fs, self.yn), (self.fs, self.near), (self.first, self.other), (self.first, self.near), (self.other, self.near), (self.dg, self.near)]

    def copy(self, a, lane):
        slot, peer = self.routes()[lane]
        src = self.ins[a] if lane < 3 else self.outs[a].at[slot]
        return remote(src, self.outs[a].at[slot], self.send.at[a, lane], self.recv.at[a, slot], device(self.me, peer))

    def push(self, arrays, lanes):
        for a in arrays:
            for lane in lanes:
                self.copy(a, lane).start()

    def arrived(self, arrays, slots):
        for a in arrays:
            for slot in slots:
                remote(self.ins[a], self.outs[a].at[slot], self.send.at[a, 0], self.recv.at[a, slot], device(self.me, self.near)).wait_recv()

    def begin(self, arrays):
        self.push(arrays, (0, 1, 2))
        for a in arrays:
            self.outs[a][self.fs] = self.ins[a][...]

    def relay(self, arrays):
        self.arrived(arrays, [self.first])
        self.push(arrays, (3, 4))
        self.arrived(arrays, [self.other])
        self.push(arrays, (5,))

    def relay_last(self, arrays):
        self.arrived(arrays, [self.dg])
        self.push(arrays, (6,))

    def complete(self, arrays):
        self.arrived(arrays, [self.near] + [slot + self.flip for slot in (self.xn, self.yn, self.dg)])

    def sent(self, arrays):
        for a in arrays:
            for lane in range(7):
                self.copy(a, lane).wait_send()

    def blocks(self, z):
        return self.g_in.at[pl.ds(z * self.n_seq, self.n_seq)]

    def tok_copy(self, k):
        z = self.cps[k - 1]
        return remote(self.tok_in.at[z], self.tok_out.at[k], self.tok_send.at[k], self.tok_recv.at[k], device(z, self.fs))

    def g_copy(self, k):
        z = self.cps[k - 1]
        return remote(self.blocks(z), self.g_out.at[k], self.g_send.at[k], self.g_recv.at[k], device(z, self.fs))

    def own_block(self):
        return pltpu.make_async_copy(self.blocks(self.me), self.g_out.at[0], self.own)


def attn_fwd_kernel(n_steps, cp_size, seq_loc, n_arr, len_ref, emb_ref, cos_ref, sin_ref, tok_in, g_in, *refs):
    ins, refs = refs[:n_arr], refs[n_arr:]
    saved, refs = refs[:n_arr - 1], refs[n_arr - 1:]
    tok_ref, g_out, gain_ref, wqkv_n, h_ref, xhat1_ref, stat_ref, qkv_ref, lse_ref, attn_ref, wqkv_t, k_tm, q_pad, bias, vec_b, tok_s, save_sem, *refs = refs
    outs = refs[:n_arr]
    gather = Gather(cp_size, n_steps, ins, outs, tok_in, tok_s, g_in, g_out, refs[n_arr:])
    kept = outs[:1] + outs[2:]
    saves = [pltpu.make_async_copy(src, dst, save_sem.at[i]) for i, (src, dst) in enumerate(zip(kept, saved))]
    early, late = (0, 1), tuple(range(2, n_arr))
    others = range(1, cp_size)
    step = pl.program_id(0)
    me = lax.axis_index('cp')

    @pl.when(step == 0)
    def _():
        gather.enter()
        for k in others:
            gather.tok_copy(k).start()
        gather.begin(early)
        for k in others:
            gather.g_copy(k).start()
        gather.own_block().start()
        tok_s[0] = tok_in[me]
        q_pad[...] = jnp.zeros_like(q_pad)
        gather.relay(early)
        gather.begin(late)
        gather.relay_last(early)
        gather.complete(early)
        joined = join_rows(outs[1])
        wqkv_n[...] = joined
        wqkv_t[...] = joined.T
        pieces = outs[0].shape[0]
        rows = D // pieces
        for i in range(pieces):
            gain_ref[i * rows:(i + 1) * rows] = outs[0][i].T[:rows]
        spread_vectors(outs[0], range(5), vec_b)
        for k in others:
            gather.tok_copy(k).wait()

    @pl.when(step == 2)
    def _():
        gather.relay(late)

    @pl.when(step == 4)
    def _():
        gather.relay_last(late)

    @pl.when(step == 6)
    def _():
        gather.complete(late)
        for copy in saves:
            copy.start()

    length = len_ref[lax.axis_index('cp') * n_steps + step]
    tok = jnp.concatenate([tok_s[k, pl.ds(step, 1), :] for k in range(cp_size)], axis=1)
    tok_ref[0] = tok
    keep = token_scale(tok, length, seq_loc, cp_size, me)
    e = dot(emb_ref[...], one_hot_rows(tok)) * keep
    xhat1, rstd1 = normalize(e)
    xhat1_ref[0] = xhat1
    h = (xhat1 * wide(vec_b[0]) + wide(vec_b[1])).astype(BF)
    h_ref[0] = h
    stat_ref[0] = stack_rows([rstd1, keep, jnp.zeros((6, SEQ), F32)])
    cos_t, sin_t = cos_ref[...], sin_ref[...]
    q = (dot(wqkv_t[0:D], h) + wide(vec_b[2])) * HEAD_DIM ** -0.5
    q = rope(q, cos_t, sin_t).astype(BF)
    qkv_ref[0, 0:D] = q
    q_pad[0:D] = q
    k = rope(dot(wqkv_t[D:2 * D], h) + wide(vec_b[3]), cos_t, sin_t)
    qkv_ref[0, D:2 * D] = k.astype(BF)
    store_token_major(k_tm, k)
    qkv_ref[0, 2 * D:3 * D] = (dot(wqkv_t[2 * D:3 * D], h) + wide(vec_b[4])).astype(BF)
    bias[...] = key_bias(me, cp_size, seq_loc, length)

    def scores(hd):
        tile, slot = hd // HEADS_PER_TILE, hd % HEADS_PER_TILE
        return dot(k_tm[tile], head_rows(q_pad[tile * LANES:(tile + 1) * LANES, :], slot))

    def weights(s, hd):
        s = s + wide(bias[...])
        m = jnp.max(s, axis=0, keepdims=True)
        p = jnp.exp(s - m)
        l = col_sum(p)
        lse_ref[0, hd] = m + jnp.log(l)
        return p.astype(BF), l

    def attend(pair, hd):
        p, l = pair
        lo = hd * HEAD_DIM
        attn_ref[0, lo:lo + HEAD_DIM] = dot(qkv_ref[0, 2 * D + lo:2 * D + lo + HEAD_DIM, :], p) / l

    pipeline(N_HEADS, (scores, weights, attend))

    @pl.when(step == n_steps - 1)
    def _():
        gather.sent(early + late)
        for copy in saves:
            copy.wait()
        for k in others:
            gather.g_copy(k).wait()
        gather.own_block().wait()


def to_token_major(z_t):
    return jnp.concatenate(feature_tiles(z_t), axis=1)[:, :D]


def to_feature_major(z):
    z32 = z.astype(F32)
    pad = jnp.concatenate([z32, jnp.zeros((SEQ, N_TILES * LANES - D), F32)], axis=1)
    return stack_rows([pad[:, t * LANES:(t + 1) * LANES].T for t in range(N_TILES)])[:D]


def lane_part(z):
    return z[:, :LANES] + z[:, LANES:]


def ln_grad(dn, xhat, rstd, gain):
    dxh = dn * gain
    m1 = col_mean(dxh)
    m2 = col_mean(dxh * xhat)
    return rstd * (dxh - m1 - xhat * m2)


def row_sum(acc):
    return col_sum(acc.T)


class Homeward:
    def __init__(self, cp_size, seq_loc, send, recv):
        self.cp_size, self.seq_loc, self.send, self.recv = cp_size, seq_loc, send, recv
        self.me = lax.axis_index('cp')
        self.fs = lax.axis_index('fsdp')
        self.others = range(1, cp_size)

    def enter(self):
        enter([device(lax.rem(self.me + k, self.cp_size), self.fs) for k in self.others])

    def block(self, k):
        return pl.ds(k * self.seq_loc, self.seq_loc)

    def copies(self, item, srcs, dst):
        local = pltpu.make_async_copy(srcs[0], dst, self.send.at[item, 0])
        return [local] + [remote(srcs[k], dst, self.send.at[item, k], self.recv.at[item, k], device(lax.rem(self.me + self.cp_size - k, self.cp_size), self.fs)) for k in self.others]


def ffn_kernel(n_steps, cp_size, seq_loc, tok_ref, stat_ref, attn_ref, g_ref, emb_ref, sm_ref, wout_ref, wup_ref, wdown_ref,
               out_ref, rest_ref, dres_ref, dattn_ref, dwdown_ref, dwuo_ref, dvec_ref,
               wout_n, wup_n, wout_t, wup_t, wdown_t, vec_b, bup_b, dup_s, gelu_s, acc_bup, acc_vec, out_s, out_send, out_recv):
    step = pl.program_id(0)
    home = Homeward(cp_size, seq_loc, out_send, out_recv)

    def leaving(item):
        return home.copies(item, [out_s.at[item, home.block(k)] for k in range(cp_size)], out_ref.at[home.me, item])


    @pl.when(step == 0)
    def _():
        home.enter()
        for src, nat, tr in ((wout_ref, wout_n, wout_t), (wup_ref, wup_n, wup_t)):
            joined = join_rows(src)
            nat[...] = joined
            tr[...] = joined.T
        wdown_t[...] = wdown_ref[...].T
        spread_vectors(sm_ref, range(5, 9), vec_b)
        pieces = sm_ref.shape[0]
        rows = D // pieces
        for i in range(pieces):
            sm_t = sm_ref[i].T
            for r in range(F // D):
                lo = i * (F // pieces) + r * rows
                bup_b[lo:lo + rows] = jnp.broadcast_to(sm_t[:rows, 9 + r:10 + r], (rows, LANES))
        for acc in (dwdown_ref, dwuo_ref, acc_bup, acc_vec):
            acc[...] = jnp.zeros_like(acc)

    e = dot(emb_ref[...], one_hot_rows(tok_ref[0])) * stat_ref[0, 1:2]
    o = attn_ref[0].astype(BF)
    x1 = e + dot(wout_t[...], o) + wide(vec_b[0])
    xhat2, rstd2 = normalize(x1)
    a = (xhat2 * wide(vec_b[1]) + wide(vec_b[2])).astype(BF)
    g = stack_rows([g_ref[k, 0] for k in range(g_ref.shape[0])])
    for c in range(F // D):
        rows = slice(c * D, (c + 1) * D)
        u = dot(wup_t[rows], a) + wide(bup_b[rows])
        cdf = 0.5 * (1.0 + lax.erf(u * SQRT_HALF))
        gelu = (u * cdf).astype(BF)
        gelu_s[rows] = gelu
        dup = dot(wdown_ref[rows], g, NT) * (cdf + u * (INV_SQRT_2PI * jnp.exp(-0.5 * u * u)))
        acc_bup[rows] += lane_part(dup)
        dup_s[rows] = dup.astype(BF)
        dwdown_ref[rows] += dot(gelu, g)
    out_tm = to_token_major(x1 + wide(vec_b[3]) + dot(wdown_t[...], gelu_s[...]))
    rest_ref[0] = out_tm

    @pl.when(step < EARLY_SEQS)
    def _():
        out_s[step] = out_tm
        for copy in leaving(step):
            copy.start()

    dup_b = dup_s[...]
    dwuo_ref[:, 0:F] += dot(a, dup_b, NT)
    dn2 = dot(wup_n[...], dup_b)
    g_t = to_feature_major(g)
    dres = g_t + ln_grad(dn2, xhat2, rstd2, wide(vec_b[1]))
    for j, part in enumerate((dres, dn2 * xhat2, dn2, g_t)):
        acc_vec[j] += lane_part(part)
    dres_ref[0] = dres
    dres_b = dres.astype(BF)
    dwuo_ref[:, F:F + D] += dot(o, dres_b, NT)
    dattn_ref[0] = dot(wout_n[...], dres_b)

    @pl.when(step == n_steps - 1)
    def _():
        rows = [row_sum(pad_rows(acc_vec[j])) for j in range(4)] + [row_sum(pad_rows(acc_bup[j * D:(j + 1) * D])) for j in range(F // D)]
        dvec_ref[...] = stack_rows(rows)
        for item in range(EARLY_SEQS):
            for copy in leaving(item):
                copy.wait()


def pad_rows(z):
    return stack_rows([z, jnp.zeros((N_TILES * LANES - D, LANES), F32)])


def attn_bwd_kernel(n_steps, cp_size, seq_loc, len_ref, me_ref, tok_ref, vec_ref, wqkv_ref, cos_ref, sin_ref, qkv_ref, lse_ref, attn_ref, dattn_ref, dres_ref, xhat1_ref, h_ref, stat_ref, dwdown_ref, dwuo_ref, dvec2_ref, rest_ref,
                    rdown_ref, rup_ref, rout_ref, rqkv_ref, rsmall_ref, outb_ref,
                    ruo_ref, rqa_ref, rqb_ref, out_send, out_recv, k_tm, v_tm, q_pad, do_pad, bias, dq_s, dk_s, dv_s, acc_b, acc_vec, acc_qa, acc_qb, acc_emb, *red):
    step = pl.program_id(0)
    summer = GradSum(cp_size, (dwdown_ref, dwuo_ref, acc_qa, acc_qb), (rdown_ref, ruo_ref, rqa_ref, rqb_ref), rsmall_ref, red)

    home = Homeward(cp_size, seq_loc, out_send, out_recv)
    leaving = home.copies(0, [rest_ref.at[:, home.block(k)] for k in range(cp_size)], outb_ref.at[home.me])

    @pl.when(step == 0)
    def _():
        summer.enter()
        for copy in leaving:
            copy.start()
        for i in (0, 1):
            summer.start(0, i)
        acc_qa[...] = jnp.zeros_like(acc_qa)
        acc_qb[...] = jnp.zeros_like(acc_qb)
        acc_emb[...] = jnp.zeros_like(acc_emb)
        acc_b[...] = jnp.zeros_like(acc_b)
        acc_vec[...] = jnp.zeros_like(acc_vec)
        q_pad[...] = jnp.zeros_like(q_pad)
        do_pad[...] = jnp.zeros_like(do_pad)

    for phase, at in enumerate(PHASE_STEPS):
        @pl.when(step == at)
        def _(phase=phase):
            for i in (0, 1):
                summer.finish(phase, i)
                summer.start(phase + 1, i)

    length = len_ref[lax.axis_index('cp') * n_steps + step]
    me = me_ref[0]
    vecs = vec_ref[...]
    q_pad[0:D] = qkv_ref[0, 0:D]
    do_pad[0:D] = dattn_ref[0].astype(BF)
    store_token_major(k_tm, qkv_ref[0, D:2 * D].astype(F32))
    store_token_major(v_tm, qkv_ref[0, 2 * D:3 * D].astype(F32))
    bias[...] = key_bias(me, cp_size, seq_loc, length)

    def products(hd):
        tile, slot = hd // HEADS_PER_TILE, hd % HEADS_PER_TILE
        t0 = slice(tile * LANES, (tile + 1) * LANES)
        return dot(k_tm[tile], head_rows(q_pad[t0, :], slot)), dot(v_tm[tile], head_rows(do_pad[t0, :], slot))

    def weights(pair, hd):
        s, dp = pair
        rows = slice(hd * HEAD_DIM, (hd + 1) * HEAD_DIM)
        delta = col_sum(dattn_ref[0, rows, :] * attn_ref[0, rows, :])
        p = jnp.exp((s + wide(bias[...])) - lse_ref[0, hd])
        return p.astype(BF), (p * (dp - delta)).astype(BF)

    def gradients(pair, hd):
        p, ds = pair
        rows = slice(hd * HEAD_DIM, (hd + 1) * HEAD_DIM)
        dq_s[rows, :] = dot(qkv_ref[0, D + hd * HEAD_DIM:D + (hd + 1) * HEAD_DIM, :], ds)
        dk_s[rows, :] = dot(q_pad[rows, :], ds, NT)
        dv_s[rows, :] = dot(do_pad[rows, :], p, NT)

    pipeline(N_HEADS, (products, weights, gradients))

    cos_t, sin_t = cos_ref[...], sin_ref[...]
    h = h_ref[0]
    dq = rope(dq_s[...], cos_t, -sin_t) * HEAD_DIM ** -0.5
    dk = rope(dk_s[...], cos_t, -sin_t)
    dv = dv_s[...]
    dn1 = jnp.zeros((D, SEQ), F32)
    parts = []
    for j, dz in enumerate((dq, dk, dv)):
        acc_b[j] += lane_part(dz)
        parts.append(dz.astype(BF))
    dz_b = stack_rows(parts)
    acc_qa[...] += dot(h, dz_b[:QKV_HALF], NT).reshape(acc_qa.shape)
    acc_qb[:, :, :3 * D - QKV_HALF] += dot(h, dz_b[QKV_HALF:], NT).reshape(acc_qb.shape[0], acc_qb.shape[1], 3 * D - QKV_HALF)
    dn1 = dot(wqkv_ref[...], dz_b)
    xhat1 = xhat1_ref[0]
    acc_vec[0] += lane_part(dn1 * xhat1)
    acc_vec[1] += lane_part(dn1)
    de = dres_ref[0] + ln_grad(dn1, xhat1, stat_ref[0, 0:1], col(vecs, 0))
    de = (de * stat_ref[0, 1:2]).astype(BF)
    acc_emb[...] += dot(one_hot_rows(tok_ref[0]), de, NT)

    @pl.when(step == n_steps - 1)
    def _():
        for i in (2, 3):
            summer.start(0, i)
        rows = [row_sum(pad_rows(acc_vec[j])) for j in range(2)] + [row_sum(pad_rows(acc_b[j])) for j in range(3)]
        small = summer.small
        small[...] = jnp.zeros_like(small)
        small[:EMB_ROWS, :D] = acc_emb[:EMB_ROWS]
        small[EMB_ROWS:EMB_ROWS + len(rows)] = stack_rows(rows)
        small[EMB_ROWS + 8:EMB_ROWS + 16] = dvec2_ref[...]
        summer.start_small(0)
        for phase in range(5):
            for i in (2, 3):
                summer.finish(phase, i)
                if phase < 4:
                    summer.start(phase + 1, i)
            summer.finish_small(phase)
            if phase < 4:
                summer.start_small(phase + 1)
        for i in (0, 1):
            summer.finish(4, i)
        rup_ref[...] = ruo_ref[:, :F]
        rout_ref[...] = ruo_ref[:, F:F + D]
        rqkv_ref[:, :QKV_HALF] = rqa_ref[...]
        rqkv_ref[:, QKV_HALF:] = rqb_ref[:, :3 * D - QKV_HALF]
        for copy in leaving:
            copy.wait()


MESH = pl.DeviceIdType.MESH
EMB_ROWS = 40
SMALL_ROWS = 64
PHASE_STEPS = (1, 3, 4, 7)
STREAMS = (('xy', (0, 40, 40)), ('yx', (1, 512, 384)), ('xy', (1, 128, 128)), ('yx', (1, 128, 128)))
SMALL_SPEC = (0, SMALL_ROWS // 4, SMALL_ROWS // 4)


def neighbours(fs):
    y, x, c = place(fs)
    return fs + 1 - 2 * c, fs + 2 - 4 * x, fs + 4 - 8 * y


def place(fs):
    return fs // 4, (fs // 2) % 2, fs % 2


def device(cp, fs):
    return {'cp': cp, 'fsdp': fs}


def enter(peers):
    barrier = pltpu.get_barrier_semaphore()
    for peer in peers:
        pl.semaphore_signal(barrier, inc=1, device_id=peer, device_id_type=MESH)
    pl.semaphore_wait(barrier, len(peers))


def remote(src, dst, send_sem, recv_sem, peer):
    return pltpu.make_async_remote_copy(src_ref=src, dst_ref=dst, send_sem=send_sem, recv_sem=recv_sem, device_id=peer, device_id_type=MESH)


def piece_of(ref, spec, p):
    axis, size, stride = spec
    start = pl.multiple_of(p * stride, stride)
    return ref.at[pl.ds(start, size), :] if axis == 0 else ref.at[:, pl.ds(start, size)]


class GradSum:
    def __init__(self, cp_size, big, outs, small_out, refs):
        n = len(STREAMS)
        self.cp_size, self.big, self.outs, self.small_out = cp_size, big, outs, small_out
        self.r0, self.acc, self.r1, self.r2, self.rz, self.rg = (refs[i * n:(i + 1) * n] for i in range(6))
        self.small, self.er, self.ez, self.eg = refs[6 * n:6 * n + 4]
        sems = refs[6 * n + 4:]
        self.sends, self.recvs = sems[0:5], sems[5:10]
        self.small_send, self.small_recv = sems[10], sems[11]
        self.me = lax.axis_index('cp')
        self.fs = lax.axis_index('fsdp')
        self.y, self.x, self.c = place(self.fs)
        fs, y, x, c = self.fs, self.y, self.x, self.c
        self.cps = [lax.rem(self.me + k, cp_size) for k in range(1, cp_size)]
        self.hops = [device(self.me, f) for f in neighbours(fs)]
        self.peers = [device(z, fs) for z in self.cps]

    def enter(self):
        enter(self.hops + self.peers)

    def copies(self, phase, i):
        path, spec = STREAMS[i]
        xy = path == 'xy'
        s, v = self.sends[phase], self.recvs[phase]
        x, y, c, me = self.x, self.y, self.c, self.me
        if phase == 0:
            return [remote(self.big[i].at[2 * j + 1 - c], self.r0[i].at[j], s.at[i, j], v.at[i, j], self.hops[0]) for j in range(4)]
        if phase == 1:
            give = [2 * k + 1 - x if xy else 2 * (1 - y) + k for k in range(2)]
            return [remote(self.acc[i].at[give[k]], self.r1[i].at[k], s.at[i, k], v.at[i, k], self.hops[1 if xy else 2]) for k in range(2)]
        if phase == 2:
            return [remote(self.r1[i].at[1 - y if xy else 1 - x], self.r2[i], s.at[i, 0], v.at[i, 0], self.hops[2 if xy else 1])]
        if phase == 3:
            return [remote(piece_of(self.outs[i], spec, self.cps[k]), self.rz[i].at[k], s.at[i, k], v.at[i, k], self.peers[k]) for k in range(self.cp_size - 1)]
        return [remote(self.rg[i].at[me], self.rg[i].at[me], s.at[i, k], v.at[i, k], self.peers[k]) for k in range(self.cp_size - 1)]

    def start(self, phase, i):
        for copy in self.copies(phase, i):
            copy.start()

    def finish(self, phase, i):
        for copy in self.copies(phase, i):
            copy.wait()
        path, spec = STREAMS[i]
        xy = path == 'xy'
        big, r0, acc, r1, r2, out = self.big[i], self.r0[i], self.acc[i], self.r1[i], self.r2[i], self.outs[i]
        rz, rg = self.rz[i], self.rg[i]
        if phase == 0:
            for j in range(4):
                acc[j] = big[2 * j + self.c] + r0[j]
        elif phase == 1:
            for k in range(2):
                r1[k] = acc[2 * k + self.x if xy else 2 * self.y + k] + r1[k]
        elif phase == 2:
            out[...] = r1[self.y if xy else self.x] + r2[...]
        elif phase == 3:
            rg[self.me] = ((piece_of(out, spec, self.me)[...] + rz[0]) + rz[1]) + rz[2]
        else:
            axis, size, stride = spec
            for p in range(self.cp_size):
                lo = p * stride
                if axis == 0:
                    out[lo:lo + size, :] = rg[p]
                else:
                    out[:, lo:lo + size] = rg[p]

    def small_copies(self, phase):
        s, v = self.small_send, self.small_recv
        if phase < 3:
            return [remote(self.small, self.er.at[phase], s.at[phase], v.at[phase], self.hops[phase])]
        if phase == 3:
            return [remote(piece_of(self.small, SMALL_SPEC, self.cps[k]), self.ez.at[k], s.at[3 + k], v.at[3 + k], self.peers[k]) for k in range(self.cp_size - 1)]
        return [remote(self.eg.at[self.me], self.eg.at[self.me], s.at[6 + k], v.at[6 + k], self.peers[k]) for k in range(self.cp_size - 1)]

    def start_small(self, phase):
        for copy in self.small_copies(phase):
            copy.start()

    def finish_small(self, phase):
        for copy in self.small_copies(phase):
            copy.wait()
        if phase < 3:
            self.small[...] += self.er[phase]
        elif phase == 3:
            self.eg[self.me] = ((piece_of(self.small, SMALL_SPEC, self.me)[...] + self.ez[0]) + self.ez[1]) + self.ez[2]
        else:
            size = SMALL_SPEC[1]
            for p in range(self.cp_size):
                self.small_out[p * size:(p + 1) * size, :] = self.eg[p]


def sum_scratch(cp_size, shapes, small_shape):
    dma = pltpu.SemaphoreType.DMA
    n = len(shapes)
    cut = [((size, sh[1]) if axis == 0 else (sh[0], size)) for sh, (_, (axis, size, _)) in zip(shapes, STREAMS)]
    lanes = small_shape[1]
    scratch = [pltpu.VMEM((4,) + sh, F32) for sh in shapes] * 2 + [pltpu.VMEM((2,) + sh, F32) for sh in shapes] + [pltpu.VMEM(sh, F32) for sh in shapes]
    scratch += [pltpu.VMEM((cp_size - 1,) + sh, F32) for sh in cut] + [pltpu.VMEM((cp_size,) + sh, F32) for sh in cut]
    scratch += [pltpu.VMEM(small_shape, F32), pltpu.VMEM((3,) + small_shape, F32), pltpu.VMEM((cp_size - 1, SMALL_SPEC[1], lanes), F32), pltpu.VMEM((cp_size, SMALL_SPEC[1], lanes), F32)]
    scratch += [dma(shape) for shape in ((n, 4), (n, 2), (n, 1), (n, cp_size - 1), (n, cp_size - 1))] * 2 + [dma((3 + 2 * (cp_size - 1),))] * 2
    return scratch


def per_seq(*shape):
    return pl.BlockSpec((1,) + shape, lambda b: (b,) + (0,) * len(shape))


def whole(*shape):
    return pl.BlockSpec(shape, lambda b: (0,) * len(shape))


SMEM = pl.BlockSpec(memory_space=pltpu.SMEM)


def sds(shape, dtype):
    return jax.ShapeDtypeStruct(shape, dtype)


def call(kernel, grid, in_specs, out_specs, out_shape, scratch, flops, name, **params):
    return pl.pallas_call(
        kernel, grid=(grid,), in_specs=in_specs, out_specs=out_specs, out_shape=out_shape, scratch_shapes=scratch, name=name,
        cost_estimate=pl.CostEstimate(flops=flops, bytes_accessed=50_000_000, transcendentals=10_000_000),
        compiler_params=pltpu.CompilerParams(dimension_semantics=('arbitrary',), vmem_limit_bytes=58 * 1024 * 1024, **params))


def solution(mesh):
    cp_size = mesh.shape['cp']
    fs_size = mesh.shape['fsdp']

    def local_step(tokens, lengths, embed_table, layer_vecs, w_qkv, w_out, w_up, b_up, w_down, grad_out):
        n_loc, seq_loc = tokens.shape
        n_seq = n_loc // cp_size
        me = lax.axis_index('cp')
        fs = lax.axis_index('fsdp')

        small = stack_rows([layer_vecs, b_up.reshape(F // D, D // fs_size)])
        small = jnp.pad(small, ((0, SM_ROWS - small.shape[0]), (0, LANES - small.shape[1])))
        shards = [small, w_qkv.reshape(-1, 3 * D), w_out, w_up, w_down]
        full = [(fs_size,) + arr.shape for arr in shards]
        emb_t = jnp.pad(embed_table, ((0, VOCAB_PAD - embed_table.shape[0]), (0, 0))).T

        lane = jnp.arange(SEQ)
        positions = ((me - lane // seq_loc + cp_size) % cp_size) * seq_loc + lane % seq_loc
        inv_freq = 1.0 / (ROPE_BASE ** (jnp.arange(0, HEAD_DIM, 2, dtype=F32) / HEAD_DIM))
        angles = inv_freq[:, None] * positions.astype(F32)[None, :]
        cos_t, sin_t = jnp.cos(angles), jnp.sin(angles)
        me_arr = me.reshape(1).astype(jnp.int32)

        S = SEQ
        dma = pltpu.SemaphoreType.DMA
        vmem = pl.BlockSpec(memory_space=pltpu.VMEM)
        hbm = pl.BlockSpec(memory_space=pl.ANY)
        n_arr = len(shards)
        kept = [0] + list(range(2, n_arr))
        g_shape = (cp_size, n_seq, seq_loc, D)
        per_feature = per_seq(D, S)
        table = whole(8, S)
        tok = tokens.reshape(cp_size, n_seq, seq_loc)
        outs = call(
            functools.partial(attn_fwd_kernel, n_seq, cp_size, seq_loc, n_arr), n_seq,
            [SMEM, whole(D, VOCAB_PAD), table, table, vmem, hbm] + [vmem] * n_arr,
            [hbm] * len(kept) + [per_seq(1, S), hbm, whole(D, SM_ROWS), whole(D, 3 * D), per_feature, per_feature, per_seq(8, S), per_seq(3 * D, S), per_seq(N_HEADS, 1, S), per_feature],
            [sds(full[i], shards[i].dtype) for i in kept] + [sds((n_seq, 1, S), jnp.int32), sds(g_shape, BF), sds((D, SM_ROWS), F32), sds((D, 3 * D), BF), sds((n_seq, D, S), BF), sds((n_seq, D, S), F32), sds((n_seq, 8, S), F32), sds((n_seq, 3 * D, S), BF), sds((n_seq, N_HEADS, 1, S), F32), sds((n_seq, D, S), F32)],
            [pltpu.VMEM((3 * D, D), BF), pltpu.VMEM((N_TILES, S, LANES), BF), pltpu.VMEM((N_TILES * LANES, S), BF), pltpu.VMEM((S, LANES), F32), pltpu.VMEM((5, D, LANES), F32), pltpu.VMEM(tok.shape, jnp.int32), dma((len(kept),))] + [pltpu.VMEM(sh, arr.dtype) for sh, arr in zip(full, shards)] + [
             dma((n_arr, 7)), dma((n_arr, fs_size)), dma((cp_size,)), dma((cp_size,)), dma((cp_size,)), dma((cp_size,)), dma],
            FLOPS, 'attn_fwd', collective_id=0, has_side_effects=True,
        )(lengths, emb_t, cos_t, sin_t, tok, grad_out, *shards)
        small_p, out_p, up_p, down_p, tok_w, g_w, vecs_t, qkv_w, h, xhat1, stat, qkv, lse, attn = outs

        outs = call(
            functools.partial(ffn_kernel, n_seq, cp_size, seq_loc), n_seq,
            [per_seq(1, S), per_seq(8, S), per_feature, pl.BlockSpec((cp_size, 1, seq_loc, D), lambda b: (0, b, 0, 0)), whole(D, VOCAB_PAD), whole(*full[0]), whole(*full[2]), whole(*full[3]), whole(F, D)],
            [hbm, pl.BlockSpec((1, S, D), lambda b: (jnp.maximum(b - EARLY_SEQS, 0), 0, 0)), per_feature, per_feature, whole(F, D), whole(D, UO_PAD), whole(8, N_TILES * LANES)],
            [sds((cp_size, EARLY_SEQS, seq_loc, D), BF), sds((n_seq - EARLY_SEQS, S, D), BF), sds((n_seq, D, S), F32), sds((n_seq, D, S), F32), sds((F, D), F32), sds((D, UO_PAD), F32), sds((8, N_TILES * LANES), F32)],
            [pltpu.VMEM((D, D), BF), pltpu.VMEM((D, F), BF), pltpu.VMEM((D, D), BF), pltpu.VMEM((F, D), BF), pltpu.VMEM((D, F), BF), pltpu.VMEM((4, D, LANES), F32), pltpu.VMEM((F, LANES), F32),
             pltpu.VMEM((F, S), BF), pltpu.VMEM((F, S), BF), pltpu.VMEM((F, LANES), F32), pltpu.VMEM((4, D, LANES), F32), pltpu.VMEM((EARLY_SEQS, S, D), BF), dma((EARLY_SEQS, cp_size)), dma((EARLY_SEQS, cp_size))],
            FLOPS, 'ffn', collective_id=2, has_side_effects=True,
        )(tok_w, stat, attn, g_w, emb_t, small_p, out_p, up_p, down_p.reshape(F, D))
        out_a, out_rest, dres, dattn, dw_down, dw_uo, dvec2 = outs

        rows = D // fs_size
        shapes = [(F // fs_size, D), (rows, UO_PAD), (rows, QKV_HALF), (rows, QKV_HALF)]
        small_shape = (SMALL_ROWS, N_TILES * LANES)
        results = [shapes[0], (rows, F), (rows, D), (rows, 3 * D), small_shape]
        acc_q = pltpu.VMEM((fs_size, rows, QKV_HALF), F32)
        r_down, r_up, r_out, r_qkv, packed, out_b = call(
            functools.partial(attn_bwd_kernel, n_seq, cp_size, seq_loc), n_seq,
            [SMEM, SMEM, per_seq(1, S), whole(D, SM_ROWS), whole(D, 3 * D), table, table, per_seq(3 * D, S), per_seq(N_HEADS, 1, S), per_seq(D, S), per_seq(D, S), per_seq(D, S), per_seq(D, S), per_seq(D, S), per_seq(8, S),
             whole(fs_size, *shapes[0]), whole(fs_size, *shapes[1]), whole(8, N_TILES * LANES), hbm],
            [whole(*sh) for sh in results] + [hbm],
            [sds(sh, F32) for sh in results] + [sds((cp_size, n_seq - EARLY_SEQS, seq_loc, D), BF)],
            [pltpu.VMEM(sh, F32) for sh in shapes[1:]] + [*[dma((1, cp_size))] * 2, pltpu.VMEM((N_TILES, S, LANES), BF), pltpu.VMEM((N_TILES, S, LANES), BF), pltpu.VMEM((N_TILES * LANES, S), BF), pltpu.VMEM((N_TILES * LANES, S), BF), pltpu.VMEM((S, LANES), F32),
             *[pltpu.VMEM((D, S), F32)] * 3, pltpu.VMEM((3, D, LANES), F32), pltpu.VMEM((2, D, LANES), F32), acc_q, acc_q, pltpu.VMEM((VOCAB_PAD, D), F32)] + sum_scratch(cp_size, shapes, small_shape),
            FLOPS, 'attn_bwd', collective_id=1, has_side_effects=True,
        )(lengths, me_arr, tok_w, vecs_t, qkv_w, cos_t, sin_t, qkv, lse, attn, dattn, dres, xhat1, h, stat, dw_down.reshape(fs_size, *shapes[0]), dw_uo.reshape(fs_size, *shapes[1]), dvec2, out_rest)
        layer_out = jnp.concatenate([out_a, out_b], axis=1).reshape(grad_out.shape)

        vocab = embed_table.shape[0]
        d_vecs = stack_rows([packed[EMB_ROWS:EMB_ROWS + 5], packed[EMB_ROWS + 8:EMB_ROWS + 12]])
        d_vecs = lax.dynamic_slice_in_dim(d_vecs, fs * (D // fs_size), D // fs_size, 1)
        d_bup = packed[EMB_ROWS + 12:EMB_ROWS + 16, :D].reshape(F)
        d_bup = lax.dynamic_slice_in_dim(d_bup, fs * (F // fs_size), F // fs_size, 0)
        return (layer_out, packed[:vocab, :D], d_vecs, r_qkv.reshape(w_qkv.shape), r_out, r_up, d_bup, r_down)

    in_specs = (P('fsdp', 'cp'), P('fsdp'), P(), P(None, 'fsdp'), P('fsdp', None, None, None), P('fsdp', None), P('fsdp', None), P('fsdp'), P('fsdp', None), P('fsdp', 'cp', None))
    out_specs = (P('fsdp', 'cp', None), P(), P(None, 'fsdp'), P('fsdp', None, None, None), P('fsdp', None), P('fsdp', None), P('fsdp'), P('fsdp', None))
    return jax.shard_map(local_step, mesh=mesh, in_specs=in_specs, out_specs=out_specs, check_vma=False)
```

```python
import functools

import jax
import jax.numpy as jnp
from jax import lax
from jax.experimental import pallas as pl
from jax.experimental.pallas import tpu as pltpu
from jax.sharding import PartitionSpec as P

MASK_ID = 32
LN_EPS = 1e-5
ROPE_BASE = 10000.0
TRAIN_RATIO = 0.15 * 0.8
NEG_BIG = -1e30
VOCAB_PAD = 128
HEAD_DIM = 16
N_HEADS = 20
D = 320
F = 1280
SEQ = 256
LANES = 128
HEADS_PER_TILE = LANES // HEAD_DIM
N_TILES = -(-D // LANES)
HEAD_UNROLL = 4
QKV_HALF = 512
UO_PAD = 1664
EARLY_SEQS = 5
FLOPS = 9_000_000_000
SM_ROWS = 16
BF = jnp.bfloat16
F32 = jnp.float32
SQRT_HALF = 0.7071067811865476
INV_SQRT_2PI = 0.3989422804014327

NN = (((1,), (0,)), ((), ()))
NT = (((1,), (1,)), ((), ()))


def stack_rows(parts):
    return jnp.concatenate(parts, axis=0)


def col_sum(z):
    return jnp.sum(z, axis=0, keepdims=True)


def col_mean(z):
    return jnp.mean(z, axis=0, keepdims=True)


def dot(a, b, dims=NN):
    return lax.dot_general(a, b, dims, preferred_element_type=F32)


def col(vecs_t, j):
    return vecs_t[:, j:j + 1]


def rope(z, cos_t, sin_t):
    z4 = z.reshape(N_HEADS, 2, HEAD_DIM // 2, SEQ)
    lower, upper = z4[:, 0], z4[:, 1]
    new_l = lower * cos_t - upper * sin_t
    new_u = upper * cos_t + lower * sin_t
    return jnp.stack([new_l, new_u], axis=1).reshape(D, SEQ)


def key_bias(shift_base, cp_size, seq_loc, length):
    row = lax.broadcasted_iota(jnp.int32, (SEQ, LANES), 0)
    src = (shift_base - row // seq_loc + cp_size) % cp_size
    pos = src * seq_loc + row % seq_loc
    return jnp.where(pos < length, 0.0, NEG_BIG).astype(F32)


def feature_tiles(z_t):
    pad = stack_rows([z_t, jnp.zeros((N_TILES * LANES - D, SEQ), F32)])
    return [pad[t * LANES:(t + 1) * LANES].T.astype(BF) for t in range(N_TILES)]


def store_token_major(dst_ref, z_t):
    for t, part in enumerate(feature_tiles(z_t)):
        dst_ref[t] = part


def head_rows(ref, hd):
    slot = hd % HEADS_PER_TILE
    rows = ref[hd * HEAD_DIM:(hd + 1) * HEAD_DIM, :]
    before, after = slot * HEAD_DIM, LANES - (slot + 1) * HEAD_DIM
    parts = [jnp.zeros((before, SEQ), BF)] * (before > 0) + [rows] + [jnp.zeros((after, SEQ), BF)] * (after > 0)
    return stack_rows(parts)


def pipeline(n, stages):
    held = {}
    for turn in range(n + len(stages) - 1):
        for j in range(len(stages)):
            i = turn - j
            if 0 <= i < n:
                held[i] = stages[j](held[i], i) if j else stages[j](i)


def token_scale(tok, length, seq_loc, cp_size, me):
    lane = lax.broadcasted_iota(jnp.int32, (1, SEQ), 1)
    src = (me - lane // seq_loc + cp_size) % cp_size
    pos = src * seq_loc + lane % seq_loc
    is_mask = tok == MASK_ID
    n_mask = jnp.sum(is_mask.astype(F32), axis=1, keepdims=True)
    drop = (1.0 - TRAIN_RATIO) / (1.0 - n_mask / length.astype(F32))
    return jnp.where(is_mask | (pos >= length), 0.0, drop)


def one_hot_rows(tok):
    row = lax.broadcasted_iota(jnp.int32, (VOCAB_PAD, SEQ), 0)
    return jnp.where(row == tok, 1.0, 0.0).astype(BF)


def join_rows(ref):
    return stack_rows([ref[i].astype(F32) for i in range(ref.shape[0])]).astype(BF)


def wide(z):
    return jnp.concatenate([z, z], axis=1)


def spread_vectors(sm_ref, rows_of, dst_ref):
    pieces = sm_ref.shape[0]
    rows = D // pieces
    for i in range(pieces):
        sm_t = sm_ref[i].T
        for n, j in enumerate(rows_of):
            dst_ref[n, i * rows:(i + 1) * rows] = jnp.broadcast_to(sm_t[:rows, j:j + 1], (rows, LANES))


def normalize(z):
    cent = z - col_mean(z)
    rstd = lax.rsqrt(col_mean(cent * cent) + LN_EPS)
    return cent * rstd, rstd


class Gather:
    def __init__(self, cp_size, n_seq, ins, outs, tok_in, tok_out, g_in, g_out, sems):
        self.ins, self.outs, self.tok_in, self.tok_out, self.g_in, self.g_out = ins, outs, tok_in, tok_out, g_in, g_out
        self.send, self.recv, self.tok_send, self.tok_recv, self.g_send, self.g_recv, self.own = sems
        self.cp_size, self.n_seq = cp_size, n_seq
        self.me = lax.axis_index('cp')
        fs = self.fs = lax.axis_index('fsdp')
        y, x, c = place(fs)
        self.near, self.xn, self.yn = neighbours(fs)
        self.dg = neighbours(self.xn)[2]
        self.first = self.xn * (1 - c) + self.yn * c
        self.other = self.yn * (1 - c) + self.xn * c
        self.flip = 1 - 2 * c
        self.cps = [lax.rem(self.me + k, cp_size) for k in range(1, cp_size)]

    def enter(self):
        enter([device(self.me, f) for f in (self.near, self.xn, self.yn)] + [device(z, self.fs) for z in self.cps])

    def routes(self):
        return [(self.fs, self.xn), (self.fs, self.yn), (self.fs, self.near), (self.first, self.other), (self.first, self.near), (self.other, self.near), (self.dg, self.near)]

    def copy(self, a, lane):
        slot, peer = self.routes()[lane]
        src = self.ins[a] if lane < 3 else self.outs[a].at[slot]
        return remote(src, self.outs[a].at[slot], self.send.at[a, lane], self.recv.at[a, slot], device(self.me, peer))

    def push(self, arrays, lanes):
        for a in arrays:
            for lane in lanes:
                self.copy(a, lane).start()

    def arrived(self, arrays, slots):
        for a in arrays:
            for slot in slots:
                remote(self.ins[a], self.outs[a].at[slot], self.send.at[a, 0], self.recv.at[a, slot], device(self.me, self.near)).wait_recv()

    def begin(self, arrays):
        self.push(arrays, (0, 1, 2))
        for a in arrays:
            self.outs[a][self.fs] = self.ins[a][...]

    def relay(self, arrays):
        self.arrived(arrays, [self.first])
        self.push(arrays, (3, 4))
        self.arrived(arrays, [self.other])
        self.push(arrays, (5,))

    def relay_last(self, arrays):
        self.arrived(arrays, [self.dg])
        self.push(arrays, (6,))

    def complete(self, arrays):
        self.arrived(arrays, [self.near] + [slot + self.flip for slot in (self.xn, self.yn, self.dg)])

    def sent(self, arrays):
        for a in arrays:
            for lane in range(7):
                self.copy(a, lane).wait_send()

    def blocks(self, z):
        return self.g_in.at[pl.ds(z * self.n_seq, self.n_seq)]

    def tok_copy(self, k):
        z = self.cps[k - 1]
        return remote(self.tok_in.at[z], self.tok_out.at[k], self.tok_send.at[k], self.tok_recv.at[k], device(z, self.fs))

    def g_copy(self, k):
        z = self.cps[k - 1]
        return remote(self.blocks(z), self.g_out.at[k], self.g_send.at[k], self.g_recv.at[k], device(z, self.fs))

    def own_block(self):
        return pltpu.make_async_copy(self.blocks(self.me), self.g_out.at[0], self.own)


def attn_fwd_kernel(n_steps, cp_size, seq_loc, n_arr, len_ref, emb_ref, cos_ref, sin_ref, tok_in, g_in, *refs):
    ins, refs = refs[:n_arr], refs[n_arr:]
    saved, refs = refs[:n_arr - 1], refs[n_arr - 1:]
    tok_ref, g_out, gain_ref, wqkv_n, h_ref, xhat1_ref, stat_ref, qkv_ref, lse_ref, attn_ref, wqkv_t, k_tm, q_pad, bias, vec_b, tok_s, save_sem, *refs = refs
    outs = refs[:n_arr]
    gather = Gather(cp_size, n_steps, ins, outs, tok_in, tok_s, g_in, g_out, refs[n_arr:])
    kept = outs[:1] + outs[2:]
    saves = [pltpu.make_async_copy(src, dst, save_sem.at[i]) for i, (src, dst) in enumerate(zip(kept, saved))]
    early, late = (0, 1), tuple(range(2, n_arr))
    others = range(1, cp_size)
    step = pl.program_id(0)
    me = lax.axis_index('cp')

    @pl.when(step == 0)
    def _():
        gather.enter()
        for k in others:
            gather.tok_copy(k).start()
        gather.begin(early)
        for k in others:
            gather.g_copy(k).start()
        gather.own_block().start()
        tok_s[0] = tok_in[me]
        q_pad[...] = jnp.zeros_like(q_pad)
        gather.relay(early)
        gather.begin(late)
        gather.relay_last(early)
        gather.complete(early)
        joined = join_rows(outs[1])
        wqkv_n[...] = joined
        wqkv_t[...] = joined.T
        pieces = outs[0].shape[0]
        rows = D // pieces
        for i in range(pieces):
            gain_ref[i * rows:(i + 1) * rows] = outs[0][i].T[:rows]
        spread_vectors(outs[0], range(5), vec_b)
        for k in others:
            gather.tok_copy(k).wait()

    @pl.when(step == 2)
    def _():
        gather.relay(late)

    @pl.when(step == 4)
    def _():
        gather.relay_last(late)

    @pl.when(step == 6)
    def _():
        gather.complete(late)
        for copy in saves:
            copy.start()

    length = len_ref[lax.axis_index('cp') * n_steps + step]
    tok = jnp.concatenate([tok_s[k, pl.ds(step, 1), :] for k in range(cp_size)], axis=1)
    tok_ref[0] = tok
    keep = token_scale(tok, length, seq_loc, cp_size, me)
    e = dot(emb_ref[...], one_hot_rows(tok)) * keep
    xhat1, rstd1 = normalize(e)
    xhat1_ref[0] = xhat1
    h = (xhat1 * wide(vec_b[0]) + wide(vec_b[1])).astype(BF)
    h_ref[0] = h
    stat_ref[0] = stack_rows([rstd1, keep, jnp.zeros((6, SEQ), F32)])
    cos_t, sin_t = cos_ref[...], sin_ref[...]
    q = (dot(wqkv_t[0:D], h) + wide(vec_b[2])) * HEAD_DIM ** -0.5
    q = rope(q, cos_t, sin_t).astype(BF)
    qkv_ref[0, 0:D] = q
    q_pad[0:D] = q
    k = rope(dot(wqkv_t[D:2 * D], h) + wide(vec_b[3]), cos_t, sin_t)
    qkv_ref[0, D:2 * D] = k.astype(BF)
    store_token_major(k_tm, k)
    qkv_ref[0, 2 * D:3 * D] = (dot(wqkv_t[2 * D:3 * D], h) + wide(vec_b[4])).astype(BF)
    bias[...] = key_bias(me, cp_size, seq_loc, length)

    def scores(hd):
        return dot(k_tm[hd // HEADS_PER_TILE], head_rows(q_pad, hd))

    def weights(s, hd):
        s = s + wide(bias[...])
        m = jnp.max(s, axis=0, keepdims=True)
        p = jnp.exp(s - m)
        l = col_sum(p)
        lse_ref[0, hd] = m + jnp.log(l)
        return p.astype(BF), l

    def attend(pair, hd):
        p, l = pair
        lo = hd * HEAD_DIM
        attn_ref[0, lo:lo + HEAD_DIM] = dot(qkv_ref[0, 2 * D + lo:2 * D + lo + HEAD_DIM, :], p) / l

    pipeline(N_HEADS, (scores, weights, attend))

    @pl.when(step == n_steps - 1)
    def _():
        gather.sent(early + late)
        for copy in saves:
            copy.wait()
        for k in others:
            gather.g_copy(k).wait()
        gather.own_block().wait()


def to_token_major(z_t):
    return jnp.concatenate(feature_tiles(z_t), axis=1)[:, :D]


def to_feature_major(z):
    z32 = z.astype(F32)
    pad = jnp.concatenate([z32, jnp.zeros((SEQ, N_TILES * LANES - D), F32)], axis=1)
    return stack_rows([pad[:, t * LANES:(t + 1) * LANES].T for t in range(N_TILES)])[:D]


def lane_part(z):
    return z[:, :LANES] + z[:, LANES:]


def ln_grad(dn, xhat, rstd, gain):
    dxh = dn * gain
    m1 = col_mean(dxh)
    m2 = col_mean(dxh * xhat)
    return rstd * (dxh - m1 - xhat * m2)


def row_sum(acc):
    return col_sum(acc.T)


class Homeward:
    def __init__(self, cp_size, seq_loc, send, recv):
        self.cp_size, self.seq_loc, self.send, self.recv = cp_size, seq_loc, send, recv
        self.me = lax.axis_index('cp')
        self.fs = lax.axis_index('fsdp')
        self.others = range(1, cp_size)

    def enter(self):
        enter([device(lax.rem(self.me + k, self.cp_size), self.fs) for k in self.others])

    def block(self, k):
        return pl.ds(k * self.seq_loc, self.seq_loc)

    def copies(self, item, srcs, dst):
        local = pltpu.make_async_copy(srcs[0], dst, self.send.at[item, 0])
        return [local] + [remote(srcs[k], dst, self.send.at[item, k], self.recv.at[item, k], device(lax.rem(self.me + self.cp_size - k, self.cp_size), self.fs)) for k in self.others]


def ffn_kernel(n_steps, cp_size, seq_loc, tok_ref, stat_ref, attn_ref, g_ref, emb_ref, sm_ref, wout_ref, wup_ref, wdown_ref,
               out_ref, rest_ref, dres_ref, dattn_ref, dwdown_ref, dwuo_ref, dvec_ref,
               wout_n, wup_n, wout_t, wup_t, wdown_t, vec_b, bup_b, dup_s, gelu_s, acc_bup, acc_vec, out_s, out_send, out_recv):
    step = pl.program_id(0)
    home = Homeward(cp_size, seq_loc, out_send, out_recv)

    def leaving(item):
        return home.copies(item, [out_s.at[item, home.block(k)] for k in range(cp_size)], out_ref.at[home.me, item])


    @pl.when(step == 0)
    def _():
        home.enter()
        for src, nat, tr in ((wout_ref, wout_n, wout_t), (wup_ref, wup_n, wup_t)):
            joined = join_rows(src)
            nat[...] = joined
            tr[...] = joined.T
        wdown_t[...] = wdown_ref[...].T
        spread_vectors(sm_ref, range(5, 9), vec_b)
        pieces = sm_ref.shape[0]
        rows = D // pieces
        for i in range(pieces):
            sm_t = sm_ref[i].T
            for r in range(F // D):
                lo = i * (F // pieces) + r * rows
                bup_b[lo:lo + rows] = jnp.broadcast_to(sm_t[:rows, 9 + r:10 + r], (rows, LANES))
        for acc in (dwdown_ref, dwuo_ref, acc_bup, acc_vec):
            acc[...] = jnp.zeros_like(acc)

    e = dot(emb_ref[...], one_hot_rows(tok_ref[0])) * stat_ref[0, 1:2]
    o = attn_ref[0].astype(BF)
    x1 = e + dot(wout_t[...], o) + wide(vec_b[0])
    xhat2, rstd2 = normalize(x1)
    a = (xhat2 * wide(vec_b[1]) + wide(vec_b[2])).astype(BF)
    g = stack_rows([g_ref[k, 0] for k in range(g_ref.shape[0])])
    for c in range(F // D):
        rows = slice(c * D, (c + 1) * D)
        u = dot(wup_t[rows], a) + wide(bup_b[rows])
        cdf = 0.5 * (1.0 + lax.erf(u * SQRT_HALF))
        gelu = (u * cdf).astype(BF)
        gelu_s[rows] = gelu
        dup = dot(wdown_ref[rows], g, NT) * (cdf + u * (INV_SQRT_2PI * jnp.exp(-0.5 * u * u)))
        acc_bup[rows] += lane_part(dup)
        dup_s[rows] = dup.astype(BF)
        dwdown_ref[rows] += dot(gelu, g)
    out_tm = to_token_major(x1 + wide(vec_b[3]) + dot(wdown_t[...], gelu_s[...]))
    rest_ref[0] = out_tm

    @pl.when(step < EARLY_SEQS)
    def _():
        out_s[step] = out_tm
        for copy in leaving(step):
            copy.start()

    dup_b = dup_s[...]
    dwuo_ref[:, 0:F] += dot(a, dup_b, NT)
    dn2 = dot(wup_n[...], dup_b)
    g_t = to_feature_major(g)
    dres = g_t + ln_grad(dn2, xhat2, rstd2, wide(vec_b[1]))
    for j, part in enumerate((dres, dn2 * xhat2, dn2, g_t)):
        acc_vec[j] += lane_part(part)
    dres_ref[0] = dres
    dres_b = dres.astype(BF)
    dwuo_ref[:, F:F + D] += dot(o, dres_b, NT)
    dattn_ref[0] = dot(wout_n[...], dres_b)

    @pl.when(step == n_steps - 1)
    def _():
        rows = [row_sum(pad_rows(acc_vec[j])) for j in range(4)] + [row_sum(pad_rows(acc_bup[j * D:(j + 1) * D])) for j in range(F // D)]
        dvec_ref[...] = stack_rows(rows)
        for item in range(EARLY_SEQS):
            for copy in leaving(item):
                copy.wait()


def pad_rows(z):
    return stack_rows([z, jnp.zeros((N_TILES * LANES - D, LANES), F32)])


def attn_bwd_kernel(n_steps, cp_size, seq_loc, len_ref, me_ref, tok_ref, vec_ref, wqkv_ref, cos_ref, sin_ref, qkv_ref, lse_ref, attn_ref, dattn_ref, dres_ref, xhat1_ref, h_ref, stat_ref, dwdown_ref, dwuo_ref, dvec2_ref, rest_ref,
                    rdown_ref, rup_ref, rout_ref, rqkv_ref, rsmall_ref, outb_ref,
                    ruo_ref, rqa_ref, rqb_ref, out_send, out_recv, k_tm, v_tm, q_pad, do_pad, bias, dq_s, dk_s, dv_s, acc_b, acc_vec, acc_qa, acc_qb, acc_emb, *red):
    step = pl.program_id(0)
    summer = GradSum(cp_size, (dwdown_ref, dwuo_ref, acc_qa, acc_qb), (rdown_ref, ruo_ref, rqa_ref, rqb_ref), rsmall_ref, red)

    home = Homeward(cp_size, seq_loc, out_send, out_recv)
    leaving = home.copies(0, [rest_ref.at[:, home.block(k)] for k in range(cp_size)], outb_ref.at[home.me])

    @pl.when(step == 0)
    def _():
        summer.enter()
        for copy in leaving:
            copy.start()
        for i in (0, 1):
            summer.start(0, i)
        acc_qa[...] = jnp.zeros_like(acc_qa)
        acc_qb[...] = jnp.zeros_like(acc_qb)
        acc_emb[...] = jnp.zeros_like(acc_emb)
        acc_b[...] = jnp.zeros_like(acc_b)
        acc_vec[...] = jnp.zeros_like(acc_vec)
        q_pad[...] = jnp.zeros_like(q_pad)
        do_pad[...] = jnp.zeros_like(do_pad)

    for phase, at in enumerate(PHASE_STEPS):
        @pl.when(step == at)
        def _(phase=phase):
            for i in (0, 1):
                summer.finish(phase, i)
                summer.start(phase + 1, i)

    length = len_ref[lax.axis_index('cp') * n_steps + step]
    me = me_ref[0]
    vecs = vec_ref[...]
    q_pad[0:D] = qkv_ref[0, 0:D]
    do_pad[0:D] = dattn_ref[0].astype(BF)
    store_token_major(k_tm, qkv_ref[0, D:2 * D].astype(F32))
    store_token_major(v_tm, qkv_ref[0, 2 * D:3 * D].astype(F32))
    bias[...] = key_bias(me, cp_size, seq_loc, length)

    def products(hd):
        tile = hd // HEADS_PER_TILE
        return dot(k_tm[tile], head_rows(q_pad, hd)), dot(v_tm[tile], head_rows(do_pad, hd))

    def weights(pair, hd):
        s, dp = pair
        rows = slice(hd * HEAD_DIM, (hd + 1) * HEAD_DIM)
        delta = col_sum(dattn_ref[0, rows, :] * attn_ref[0, rows, :])
        p = jnp.exp((s + wide(bias[...])) - lse_ref[0, hd])
        return p.astype(BF), (p * (dp - delta)).astype(BF)

    def gradients(pair, hd):
        p, ds = pair
        rows = slice(hd * HEAD_DIM, (hd + 1) * HEAD_DIM)
        dq_s[rows, :] = dot(qkv_ref[0, D + hd * HEAD_DIM:D + (hd + 1) * HEAD_DIM, :], ds)
        dk_s[rows, :] = dot(q_pad[rows, :], ds, NT)
        dv_s[rows, :] = dot(do_pad[rows, :], p, NT)

    pipeline(N_HEADS, (products, weights, gradients))

    cos_t, sin_t = cos_ref[...], sin_ref[...]
    h = h_ref[0]
    dq = rope(dq_s[...], cos_t, -sin_t) * HEAD_DIM ** -0.5
    dk = rope(dk_s[...], cos_t, -sin_t)
    dv = dv_s[...]
    dn1 = jnp.zeros((D, SEQ), F32)
    parts = []
    for j, dz in enumerate((dq, dk, dv)):
        acc_b[j] += lane_part(dz)
        parts.append(dz.astype(BF))
    dz_b = stack_rows(parts)
    acc_qa[...] += dot(h, dz_b[:QKV_HALF], NT).reshape(acc_qa.shape)
    acc_qb[:, :, :3 * D - QKV_HALF] += dot(h, dz_b[QKV_HALF:], NT).reshape(acc_qb.shape[0], acc_qb.shape[1], 3 * D - QKV_HALF)
    dn1 = dot(wqkv_ref[...], dz_b)
    xhat1 = xhat1_ref[0]
    acc_vec[0] += lane_part(dn1 * xhat1)
    acc_vec[1] += lane_part(dn1)
    de = dres_ref[0] + ln_grad(dn1, xhat1, stat_ref[0, 0:1], col(vecs, 0))
    de = (de * stat_ref[0, 1:2]).astype(BF)
    acc_emb[...] += dot(one_hot_rows(tok_ref[0]), de, NT)

    @pl.when(step == n_steps - 1)
    def _():
        for i in (2, 3):
            summer.start(0, i)
        rows = [row_sum(pad_rows(acc_vec[j])) for j in range(2)] + [row_sum(pad_rows(acc_b[j])) for j in range(3)]
        small = summer.small
        small[...] = jnp.zeros_like(small)
        small[:EMB_ROWS, :D] = acc_emb[:EMB_ROWS]
        small[EMB_ROWS:EMB_ROWS + len(rows)] = stack_rows(rows)
        small[EMB_ROWS + 8:EMB_ROWS + 16] = dvec2_ref[...]
        summer.start_small(0)
        for phase in range(5):
            for i in (2, 3):
                summer.finish(phase, i)
                if phase < 4:
                    summer.start(phase + 1, i)
            summer.finish_small(phase)
            if phase < 4:
                summer.start_small(phase + 1)
        for i in (0, 1):
            summer.finish(4, i)
        rup_ref[...] = ruo_ref[:, :F]
        rout_ref[...] = ruo_ref[:, F:F + D]
        rqkv_ref[:, :QKV_HALF] = rqa_ref[...]
        rqkv_ref[:, QKV_HALF:] = rqb_ref[:, :3 * D - QKV_HALF]
        for copy in leaving:
            copy.wait()


MESH = pl.DeviceIdType.MESH
EMB_ROWS = 40
SMALL_ROWS = 64
PHASE_STEPS = (1, 3, 4, 7)
STREAMS = (('xy', (0, 40, 40)), ('yx', (1, 512, 384)), ('xy', (1, 128, 128)), ('yx', (1, 128, 128)))
SMALL_SPEC = (0, SMALL_ROWS // 4, SMALL_ROWS // 4)


def neighbours(fs):
    y, x, c = place(fs)
    return fs + 1 - 2 * c, fs + 2 - 4 * x, fs + 4 - 8 * y


def place(fs):
    return fs // 4, (fs // 2) % 2, fs % 2


def device(cp, fs):
    return {'cp': cp, 'fsdp': fs}


def enter(peers):
    barrier = pltpu.get_barrier_semaphore()
    for peer in peers:
        pl.semaphore_signal(barrier, inc=1, device_id=peer, device_id_type=MESH)
    pl.semaphore_wait(barrier, len(peers))


def remote(src, dst, send_sem, recv_sem, peer):
    return pltpu.make_async_remote_copy(src_ref=src, dst_ref=dst, send_sem=send_sem, recv_sem=recv_sem, device_id=peer, device_id_type=MESH)


def piece_of(ref, spec, p):
    axis, size, stride = spec
    start = pl.multiple_of(p * stride, stride)
    return ref.at[pl.ds(start, size), :] if axis == 0 else ref.at[:, pl.ds(start, size)]


class GradSum:
    def __init__(self, cp_size, big, outs, small_out, refs):
        n = len(STREAMS)
        self.cp_size, self.big, self.outs, self.small_out = cp_size, big, outs, small_out
        self.r0, self.acc, self.r1, self.r2, self.rz, self.rg = (refs[i * n:(i + 1) * n] for i in range(6))
        self.small, self.er, self.ez, self.eg = refs[6 * n:6 * n + 4]
        sems = refs[6 * n + 4:]
        self.sends, self.recvs = sems[0:5], sems[5:10]
        self.small_send, self.small_recv = sems[10], sems[11]
        self.me = lax.axis_index('cp')
        self.fs = lax.axis_index('fsdp')
        self.y, self.x, self.c = place(self.fs)
        fs, y, x, c = self.fs, self.y, self.x, self.c
        self.cps = [lax.rem(self.me + k, cp_size) for k in range(1, cp_size)]
        self.hops = [device(self.me, f) for f in neighbours(fs)]
        self.peers = [device(z, fs) for z in self.cps]

    def enter(self):
        enter(self.hops + self.peers)

    def copies(self, phase, i):
        path, spec = STREAMS[i]
        xy = path == 'xy'
        s, v = self.sends[phase], self.recvs[phase]
        x, y, c, me = self.x, self.y, self.c, self.me
        if phase == 0:
            return [remote(self.big[i].at[2 * j + 1 - c], self.r0[i].at[j], s.at[i, j], v.at[i, j], self.hops[0]) for j in range(4)]
        if phase == 1:
            give = [2 * k + 1 - x if xy else 2 * (1 - y) + k for k in range(2)]
            return [remote(self.acc[i].at[give[k]], self.r1[i].at[k], s.at[i, k], v.at[i, k], self.hops[1 if xy else 2]) for k in range(2)]
        if phase == 2:
            return [remote(self.r1[i].at[1 - y if xy else 1 - x], self.r2[i], s.at[i, 0], v.at[i, 0], self.hops[2 if xy else 1])]
        if phase == 3:
            return [remote(piece_of(self.outs[i], spec, self.cps[k]), self.rz[i].at[k], s.at[i, k], v.at[i, k], self.peers[k]) for k in range(self.cp_size - 1)]
        return [remote(self.rg[i].at[me], self.rg[i].at[me], s.at[i, k], v.at[i, k], self.peers[k]) for k in range(self.cp_size - 1)]

    def start(self, phase, i):
        for copy in self.copies(phase, i):
            copy.start()

    def finish(self, phase, i):
        for copy in self.copies(phase, i):
            copy.wait()
        path, spec = STREAMS[i]
        xy = path == 'xy'
        big, r0, acc, r1, r2, out = self.big[i], self.r0[i], self.acc[i], self.r1[i], self.r2[i], self.outs[i]
        rz, rg = self.rz[i], self.rg[i]
        if phase == 0:
            for j in range(4):
                acc[j] = big[2 * j + self.c] + r0[j]
        elif phase == 1:
            for k in range(2):
                r1[k] = acc[2 * k + self.x if xy else 2 * self.y + k] + r1[k]
        elif phase == 2:
            out[...] = r1[self.y if xy else self.x] + r2[...]
        elif phase == 3:
            rg[self.me] = ((piece_of(out, spec, self.me)[...] + rz[0]) + rz[1]) + rz[2]
        else:
            axis, size, stride = spec
            for p in range(self.cp_size):
                lo = p * stride
                if axis == 0:
                    out[lo:lo + size, :] = rg[p]
                else:
                    out[:, lo:lo + size] = rg[p]

    def small_copies(self, phase):
        s, v = self.small_send, self.small_recv
        if phase < 3:
            return [remote(self.small, self.er.at[phase], s.at[phase], v.at[phase], self.hops[phase])]
        if phase == 3:
            return [remote(piece_of(self.small, SMALL_SPEC, self.cps[k]), self.ez.at[k], s.at[3 + k], v.at[3 + k], self.peers[k]) for k in range(self.cp_size - 1)]
        return [remote(self.eg.at[self.me], self.eg.at[self.me], s.at[6 + k], v.at[6 + k], self.peers[k]) for k in range(self.cp_size - 1)]

    def start_small(self, phase):
        for copy in self.small_copies(phase):
            copy.start()

    def finish_small(self, phase):
        for copy in self.small_copies(phase):
            copy.wait()
        if phase < 3:
            self.small[...] += self.er[phase]
        elif phase == 3:
            self.eg[self.me] = ((piece_of(self.small, SMALL_SPEC, self.me)[...] + self.ez[0]) + self.ez[1]) + self.ez[2]
        else:
            size = SMALL_SPEC[1]
            for p in range(self.cp_size):
                self.small_out[p * size:(p + 1) * size, :] = self.eg[p]


def sum_scratch(cp_size, shapes, small_shape):
    dma = pltpu.SemaphoreType.DMA
    n = len(shapes)
    cut = [((size, sh[1]) if axis == 0 else (sh[0], size)) for sh, (_, (axis, size, _)) in zip(shapes, STREAMS)]
    lanes = small_shape[1]
    scratch = [pltpu.VMEM((4,) + sh, F32) for sh in shapes] * 2 + [pltpu.VMEM((2,) + sh, F32) for sh in shapes] + [pltpu.VMEM(sh, F32) for sh in shapes]
    scratch += [pltpu.VMEM((cp_size - 1,) + sh, F32) for sh in cut] + [pltpu.VMEM((cp_size,) + sh, F32) for sh in cut]
    scratch += [pltpu.VMEM(small_shape, F32), pltpu.VMEM((3,) + small_shape, F32), pltpu.VMEM((cp_size - 1, SMALL_SPEC[1], lanes), F32), pltpu.VMEM((cp_size, SMALL_SPEC[1], lanes), F32)]
    scratch += [dma(shape) for shape in ((n, 4), (n, 2), (n, 1), (n, cp_size - 1), (n, cp_size - 1))] * 2 + [dma((3 + 2 * (cp_size - 1),))] * 2
    return scratch


def per_seq(*shape):
    return pl.BlockSpec((1,) + shape, lambda b: (b,) + (0,) * len(shape))


def whole(*shape):
    return pl.BlockSpec(shape, lambda b: (0,) * len(shape))


SMEM = pl.BlockSpec(memory_space=pltpu.SMEM)


def sds(shape, dtype):
    return jax.ShapeDtypeStruct(shape, dtype)


def call(kernel, grid, in_specs, out_specs, out_shape, scratch, flops, name, **params):
    return pl.pallas_call(
        kernel, grid=(grid,), in_specs=in_specs, out_specs=out_specs, out_shape=out_shape, scratch_shapes=scratch, name=name,
        cost_estimate=pl.CostEstimate(flops=flops, bytes_accessed=50_000_000, transcendentals=10_000_000),
        compiler_params=pltpu.CompilerParams(dimension_semantics=('arbitrary',), vmem_limit_bytes=58 * 1024 * 1024, **params))


def solution(mesh):
    cp_size = mesh.shape['cp']
    fs_size = mesh.shape['fsdp']

    def local_step(tokens, lengths, embed_table, layer_vecs, w_qkv, w_out, w_up, b_up, w_down, grad_out):
        n_loc, seq_loc = tokens.shape
        n_seq = n_loc // cp_size
        me = lax.axis_index('cp')
        fs = lax.axis_index('fsdp')

        small = stack_rows([layer_vecs, b_up.reshape(F // D, D // fs_size)])
        small = jnp.pad(small, ((0, SM_ROWS - small.shape[0]), (0, LANES - small.shape[1])))
        shards = [small, w_qkv.reshape(-1, 3 * D), w_out, w_up, w_down]
        full = [(fs_size,) + arr.shape for arr in shards]
        emb_t = jnp.pad(embed_table, ((0, VOCAB_PAD - embed_table.shape[0]), (0, 0))).T

        lane = jnp.arange(SEQ)
        positions = ((me - lane // seq_loc + cp_size) % cp_size) * seq_loc + lane % seq_loc
        inv_freq = 1.0 / (ROPE_BASE ** (jnp.arange(0, HEAD_DIM, 2, dtype=F32) / HEAD_DIM))
        angles = inv_freq[:, None] * positions.astype(F32)[None, :]
        cos_t, sin_t = jnp.cos(angles), jnp.sin(angles)
        me_arr = me.reshape(1).astype(jnp.int32)

        S = SEQ
        dma = pltpu.SemaphoreType.DMA
        vmem = pl.BlockSpec(memory_space=pltpu.VMEM)
        hbm = pl.BlockSpec(memory_space=pl.ANY)
        n_arr = len(shards)
        kept = [0] + list(range(2, n_arr))
        g_shape = (cp_size, n_seq, seq_loc, D)
        per_feature = per_seq(D, S)
        table = whole(8, S)
        tok = tokens.reshape(cp_size, n_seq, seq_loc)
        outs = call(
            functools.partial(attn_fwd_kernel, n_seq, cp_size, seq_loc, n_arr), n_seq,
            [SMEM, whole(D, VOCAB_PAD), table, table, vmem, hbm] + [vmem] * n_arr,
            [hbm] * len(kept) + [per_seq(1, S), hbm, whole(D, SM_ROWS), whole(D, 3 * D), per_feature, per_feature, per_seq(8, S), per_seq(3 * D, S), per_seq(N_HEADS, 1, S), per_feature],
            [sds(full[i], shards[i].dtype) for i in kept] + [sds((n_seq, 1, S), jnp.int32), sds(g_shape, BF), sds((D, SM_ROWS), F32), sds((D, 3 * D), BF), sds((n_seq, D, S), BF), sds((n_seq, D, S), F32), sds((n_seq, 8, S), F32), sds((n_seq, 3 * D, S), BF), sds((n_seq, N_HEADS, 1, S), F32), sds((n_seq, D, S), F32)],
            [pltpu.VMEM((3 * D, D), BF), pltpu.VMEM((N_TILES, S, LANES), BF), pltpu.VMEM((N_TILES * LANES, S), BF), pltpu.VMEM((S, LANES), F32), pltpu.VMEM((5, D, LANES), F32), pltpu.VMEM(tok.shape, jnp.int32), dma((len(kept),))] + [pltpu.VMEM(sh, arr.dtype) for sh, arr in zip(full, shards)] + [
             dma((n_arr, 7)), dma((n_arr, fs_size)), dma((cp_size,)), dma((cp_size,)), dma((cp_size,)), dma((cp_size,)), dma],
            FLOPS, 'attn_fwd', collective_id=0, has_side_effects=True,
        )(lengths, emb_t, cos_t, sin_t, tok, grad_out, *shards)
        small_p, out_p, up_p, down_p, tok_w, g_w, vecs_t, qkv_w, h, xhat1, stat, qkv, lse, attn = outs

        outs = call(
            functools.partial(ffn_kernel, n_seq, cp_size, seq_loc), n_seq,
            [per_seq(1, S), per_seq(8, S), per_feature, pl.BlockSpec((cp_size, 1, seq_loc, D), lambda b: (0, b, 0, 0)), whole(D, VOCAB_PAD), whole(*full[0]), whole(*full[2]), whole(*full[3]), whole(F, D)],
            [hbm, pl.BlockSpec((1, S, D), lambda b: (jnp.maximum(b - EARLY_SEQS, 0), 0, 0)), per_feature, per_feature, whole(F, D), whole(D, UO_PAD), whole(8, N_TILES * LANES)],
            [sds((cp_size, EARLY_SEQS, seq_loc, D), BF), sds((n_seq - EARLY_SEQS, S, D), BF), sds((n_seq, D, S), F32), sds((n_seq, D, S), F32), sds((F, D), F32), sds((D, UO_PAD), F32), sds((8, N_TILES * LANES), F32)],
            [pltpu.VMEM((D, D), BF), pltpu.VMEM((D, F), BF), pltpu.VMEM((D, D), BF), pltpu.VMEM((F, D), BF), pltpu.VMEM((D, F), BF), pltpu.VMEM((4, D, LANES), F32), pltpu.VMEM((F, LANES), F32),
             pltpu.VMEM((F, S), BF), pltpu.VMEM((F, S), BF), pltpu.VMEM((F, LANES), F32), pltpu.VMEM((4, D, LANES), F32), pltpu.VMEM((EARLY_SEQS, S, D), BF), dma((EARLY_SEQS, cp_size)), dma((EARLY_SEQS, cp_size))],
            FLOPS, 'ffn', collective_id=2, has_side_effects=True,
        )(tok_w, stat, attn, g_w, emb_t, small_p, out_p, up_p, down_p.reshape(F, D))
        out_a, out_rest, dres, dattn, dw_down, dw_uo, dvec2 = outs

        rows = D // fs_size
        shapes = [(F // fs_size, D), (rows, UO_PAD), (rows, QKV_HALF), (rows, QKV_HALF)]
        small_shape = (SMALL_ROWS, N_TILES * LANES)
        results = [shapes[0], (rows, F), (rows, D), (rows, 3 * D), small_shape]
        acc_q = pltpu.VMEM((fs_size, rows, QKV_HALF), F32)
        r_down, r_up, r_out, r_qkv, packed, out_b = call(
            functools.partial(attn_bwd_kernel, n_seq, cp_size, seq_loc), n_seq,
            [SMEM, SMEM, per_seq(1, S), whole(D, SM_ROWS), whole(D, 3 * D), table, table, per_seq(3 * D, S), per_seq(N_HEADS, 1, S), per_seq(D, S), per_seq(D, S), per_seq(D, S), per_seq(D, S), per_seq(D, S), per_seq(8, S),
             whole(fs_size, *shapes[0]), whole(fs_size, *shapes[1]), whole(8, N_TILES * LANES), hbm],
            [whole(*sh) for sh in results] + [hbm],
            [sds(sh, F32) for sh in results] + [sds((cp_size, n_seq - EARLY_SEQS, seq_loc, D), BF)],
            [pltpu.VMEM(sh, F32) for sh in shapes[1:]] + [*[dma((1, cp_size))] * 2, pltpu.VMEM((N_TILES, S, LANES), BF), pltpu.VMEM((N_TILES, S, LANES), BF), pltpu.VMEM((N_TILES * LANES, S), BF), pltpu.VMEM((N_TILES * LANES, S), BF), pltpu.VMEM((S, LANES), F32),
             *[pltpu.VMEM((D, S), F32)] * 3, pltpu.VMEM((3, D, LANES), F32), pltpu.VMEM((2, D, LANES), F32), acc_q, acc_q, pltpu.VMEM((VOCAB_PAD, D), F32)] + sum_scratch(cp_size, shapes, small_shape),
            FLOPS, 'attn_bwd', collective_id=1, has_side_effects=True,
        )(lengths, me_arr, tok_w, vecs_t, qkv_w, cos_t, sin_t, qkv, lse, attn, dattn, dres, xhat1, h, stat, dw_down.reshape(fs_size, *shapes[0]), dw_uo.reshape(fs_size, *shapes[1]), dvec2, out_rest)
        layer_out = jnp.concatenate([out_a, out_b], axis=1).reshape(grad_out.shape)

        vocab = embed_table.shape[0]
        d_vecs = stack_rows([packed[EMB_ROWS:EMB_ROWS + 5], packed[EMB_ROWS + 8:EMB_ROWS + 12]])
        d_vecs = lax.dynamic_slice_in_dim(d_vecs, fs * (D // fs_size), D // fs_size, 1)
        d_bup = packed[EMB_ROWS + 12:EMB_ROWS + 16, :D].reshape(F)
        d_bup = lax.dynamic_slice_in_dim(d_bup, fs * (F // fs_size), F // fs_size, 0)
        return (layer_out, packed[:vocab, :D], d_vecs, r_qkv.reshape(w_qkv.shape), r_out, r_up, d_bup, r_down)

    in_specs = (P('fsdp', 'cp'), P('fsdp'), P(), P(None, 'fsdp'), P('fsdp', None, None, None), P('fsdp', None), P('fsdp', None), P('fsdp'), P('fsdp', None), P('fsdp', 'cp', None))
    out_specs = (P('fsdp', 'cp', None), P(), P(None, 'fsdp'), P('fsdp', None, None, None), P('fsdp', None), P('fsdp', None), P('fsdp'), P('fsdp', None))
    return jax.shard_map(local_step, mesh=mesh, in_specs=in_specs, out_specs=out_specs, check_vma=False)
```

```python
import functools

import jax
import jax.numpy as jnp
from jax import lax
from jax.experimental import pallas as pl
from jax.experimental.pallas import tpu as pltpu
from jax.sharding import PartitionSpec as P

MASK_ID = 32
LN_EPS = 1e-5
ROPE_BASE = 10000.0
TRAIN_RATIO = 0.15 * 0.8
NEG_BIG = -1e30
VOCAB_PAD = 128
HEAD_DIM = 16
N_HEADS = 20
D = 320
F = 1280
SEQ = 256
LANES = 128
HEADS_PER_TILE = LANES // HEAD_DIM
N_TILES = -(-D // LANES)
HEAD_UNROLL = 4
QKV_HALF = 512
UO_PAD = 1664
EARLY_SEQS = 5
FLOPS = 9_000_000_000
SM_ROWS = 16
BF = jnp.bfloat16
F32 = jnp.float32
SQRT_HALF = 0.7071067811865476
INV_SQRT_2PI = 0.3989422804014327

NN = (((1,), (0,)), ((), ()))
NT = (((1,), (1,)), ((), ()))


def stack_rows(parts):
    return jnp.concatenate(parts, axis=0)


def col_sum(z):
    return jnp.sum(z, axis=0, keepdims=True)


def col_mean(z):
    return jnp.mean(z, axis=0, keepdims=True)


def dot(a, b, dims=NN):
    return lax.dot_general(a, b, dims, preferred_element_type=F32)


def col(vecs_t, j):
    return vecs_t[:, j:j + 1]


def rope(z, cos_t, sin_t):
    z4 = z.reshape(N_HEADS, 2, HEAD_DIM // 2, SEQ)
    lower, upper = z4[:, 0], z4[:, 1]
    new_l = lower * cos_t - upper * sin_t
    new_u = upper * cos_t + lower * sin_t
    return jnp.stack([new_l, new_u], axis=1).reshape(D, SEQ)


def key_bias(shift_base, cp_size, seq_loc, length):
    row = lax.broadcasted_iota(jnp.int32, (SEQ, LANES), 0)
    src = (shift_base - row // seq_loc + cp_size) % cp_size
    pos = src * seq_loc + row % seq_loc
    return jnp.where(pos < length, 0.0, NEG_BIG).astype(F32)


def feature_tiles(z_t):
    pad = stack_rows([z_t, jnp.zeros((N_TILES * LANES - D, SEQ), F32)])
    return [pad[t * LANES:(t + 1) * LANES].T.astype(BF) for t in range(N_TILES)]


def store_token_major(dst_ref, z_t):
    for t, part in enumerate(feature_tiles(z_t)):
        dst_ref[t] = part


def head_rows(ref, hd):
    slot = hd % HEADS_PER_TILE
    rows = ref[hd * HEAD_DIM:(hd + 1) * HEAD_DIM, :]
    before, after = slot * HEAD_DIM, LANES - (slot + 1) * HEAD_DIM
    parts = [jnp.zeros((before, SEQ), BF)] * (before > 0) + [rows] + [jnp.zeros((after, SEQ), BF)] * (after > 0)
    return stack_rows(parts)


def pipeline(n, stages):
    held = {}
    for turn in range(n + len(stages) - 1):
        for j in range(len(stages)):
            i = turn - j
            if 0 <= i < n:
                held[i] = stages[j](held[i], i) if j else stages[j](i)


def token_scale(tok, length, seq_loc, cp_size, me):
    lane = lax.broadcasted_iota(jnp.int32, (1, SEQ), 1)
    src = (me - lane // seq_loc + cp_size) % cp_size
    pos = src * seq_loc + lane % seq_loc
    is_mask = tok == MASK_ID
    n_mask = jnp.sum(is_mask.astype(F32), axis=1, keepdims=True)
    drop = (1.0 - TRAIN_RATIO) / (1.0 - n_mask / length.astype(F32))
    return jnp.where(is_mask | (pos >= length), 0.0, drop)


def one_hot_rows(tok):
    row = lax.broadcasted_iota(jnp.int32, (VOCAB_PAD, SEQ), 0)
    return jnp.where(row == tok, 1.0, 0.0).astype(BF)


def join_rows(ref):
    return stack_rows([ref[i].astype(F32) for i in range(ref.shape[0])]).astype(BF)


def wide(z):
    return jnp.concatenate([z, z], axis=1)


def spread_vectors(sm_ref, rows_of, dst_ref):
    pieces = sm_ref.shape[0]
    rows = D // pieces
    for i in range(pieces):
        sm_t = sm_ref[i].T
        for n, j in enumerate(rows_of):
            dst_ref[n, i * rows:(i + 1) * rows] = jnp.broadcast_to(sm_t[:rows, j:j + 1], (rows, LANES))


def normalize(z):
    cent = z - col_mean(z)
    rstd = lax.rsqrt(col_mean(cent * cent) + LN_EPS)
    return cent * rstd, rstd


class Gather:
    def __init__(self, cp_size, n_seq, ins, outs, tok_in, tok_out, g_in, g_out, sems):
        self.ins, self.outs, self.tok_in, self.tok_out, self.g_in, self.g_out = ins, outs, tok_in, tok_out, g_in, g_out
        self.send, self.recv, self.tok_send, self.tok_recv, self.g_send, self.g_recv, self.own = sems
        self.cp_size, self.n_seq = cp_size, n_seq
        self.me = lax.axis_index('cp')
        fs = self.fs = lax.axis_index('fsdp')
        y, x, c = place(fs)
        self.near, self.xn, self.yn = neighbours(fs)
        self.dg = neighbours(self.xn)[2]
        self.first = self.xn * (1 - c) + self.yn * c
        self.other = self.yn * (1 - c) + self.xn * c
        self.flip = 1 - 2 * c
        self.cps = [lax.rem(self.me + k, cp_size) for k in range(1, cp_size)]

    def enter(self):
        enter([device(self.me, f) for f in (self.near, self.xn, self.yn)] + [device(z, self.fs) for z in self.cps])

    def routes(self):
        return [(self.fs, self.xn), (self.fs, self.yn), (self.fs, self.near), (self.first, self.other), (self.first, self.near), (self.other, self.near), (self.dg, self.near)]

    def copy(self, a, lane):
        slot, peer = self.routes()[lane]
        src = self.ins[a] if lane < 3 else self.outs[a].at[slot]
        return remote(src, self.outs[a].at[slot], self.send.at[a, lane], self.recv.at[a, slot], device(self.me, peer))

    def push(self, arrays, lanes):
        for a in arrays:
            for lane in lanes:
                self.copy(a, lane).start()

    def arrived(self, arrays, slots):
        for a in arrays:
            for slot in slots:
                remote(self.ins[a], self.outs[a].at[slot], self.send.at[a, 0], self.recv.at[a, slot], device(self.me, self.near)).wait_recv()

    def begin(self, arrays):
        self.push(arrays, (0, 1, 2))
        for a in arrays:
            self.outs[a][self.fs] = self.ins[a][...]

    def relay(self, arrays):
        self.arrived(arrays, [self.first])
        self.push(arrays, (3, 4))
        self.arrived(arrays, [self.other])
        self.push(arrays, (5,))

    def relay_last(self, arrays):
        self.arrived(arrays, [self.dg])
        self.push(arrays, (6,))

    def complete(self, arrays):
        self.arrived(arrays, [self.near] + [slot + self.flip for slot in (self.xn, self.yn, self.dg)])

    def sent(self, arrays):
        for a in arrays:
            for lane in range(7):
                self.copy(a, lane).wait_send()

    def blocks(self, z):
        return self.g_in.at[pl.ds(z * self.n_seq, self.n_seq)]

    def tok_copy(self, k):
        z = self.cps[k - 1]
        return remote(self.tok_in.at[z], self.tok_out.at[k], self.tok_send.at[k], self.tok_recv.at[k], device(z, self.fs))

    def g_copy(self, k):
        z = self.cps[k - 1]
        return remote(self.blocks(z), self.g_out.at[k], self.g_send.at[k], self.g_recv.at[k], device(z, self.fs))

    def own_block(self):
        return pltpu.make_async_copy(self.blocks(self.me), self.g_out.at[0], self.own)


def attn_fwd_kernel(n_steps, cp_size, seq_loc, n_arr, len_ref, emb_ref, cos_ref, sin_ref, tok_in, g_in, *refs):
    ins, refs = refs[:n_arr], refs[n_arr:]
    saved, refs = refs[:n_arr - 1], refs[n_arr - 1:]
    tok_ref, g_out, gain_ref, wqkv_n, h_ref, xhat1_ref, stat_ref, qkv_ref, lse_ref, attn_ref, wqkv_t, k_tm, q_pad, bias, vec_b, tok_s, save_sem, *refs = refs
    outs = refs[:n_arr]
    gather = Gather(cp_size, n_steps, ins, outs, tok_in, tok_s, g_in, g_out, refs[n_arr:])
    kept = outs[:1] + outs[2:]
    saves = [pltpu.make_async_copy(src, dst, save_sem.at[i]) for i, (src, dst) in enumerate(zip(kept, saved))]
    early, late = (0, 1), tuple(range(2, n_arr))
    others = range(1, cp_size)
    step = pl.program_id(0)
    me = lax.axis_index('cp')

    @pl.when(step == 0)
    def _():
        gather.enter()
        for k in others:
            gather.tok_copy(k).start()
        gather.begin(early)
        for k in others:
            gather.g_copy(k).start()
        gather.own_block().start()
        tok_s[0] = tok_in[me]
        q_pad[...] = jnp.zeros_like(q_pad)
        gather.relay(early)
        gather.begin(late)
        gather.relay_last(early)
        gather.complete(early)
        joined = join_rows(outs[1])
        wqkv_n[...] = joined
        wqkv_t[...] = joined.T
        pieces = outs[0].shape[0]
        rows = D // pieces
        for i in range(pieces):
            gain_ref[i * rows:(i + 1) * rows] = outs[0][i].T[:rows]
        spread_vectors(outs[0], range(5), vec_b)
        for k in others:
            gather.tok_copy(k).wait()

    @pl.when(step == 2)
    def _():
        gather.relay(late)

    @pl.when(step == 4)
    def _():
        gather.relay_last(late)

    @pl.when(step == 6)
    def _():
        gather.complete(late)
        for copy in saves:
            copy.start()

    length = len_ref[lax.axis_index('cp') * n_steps + step]
    tok = jnp.concatenate([tok_s[k, pl.ds(step, 1), :] for k in range(cp_size)], axis=1)
    tok_ref[0] = tok
    keep = token_scale(tok, length, seq_loc, cp_size, me)
    e = dot(emb_ref[...], one_hot_rows(tok)) * keep
    xhat1, rstd1 = normalize(e)
    xhat1_ref[0] = xhat1
    h = (xhat1 * wide(vec_b[0]) + wide(vec_b[1])).astype(BF)
    h_ref[0] = h
    stat_ref[0] = stack_rows([rstd1, keep, jnp.zeros((6, SEQ), F32)])
    cos_t, sin_t = cos_ref[...], sin_ref[...]
    q = (dot(wqkv_t[0:D], h) + wide(vec_b[2])) * HEAD_DIM ** -0.5
    q = rope(q, cos_t, sin_t).astype(BF)
    qkv_ref[0, 0:D] = q
    q_pad[0:D] = q
    k = rope(dot(wqkv_t[D:2 * D], h) + wide(vec_b[3]), cos_t, sin_t)
    qkv_ref[0, D:2 * D] = k.astype(BF)
    store_token_major(k_tm, k)
    qkv_ref[0, 2 * D:3 * D] = (dot(wqkv_t[2 * D:3 * D], h) + wide(vec_b[4])).astype(BF)
    bias[...] = key_bias(me, cp_size, seq_loc, length)

    def scores(hd):
        return dot(k_tm[hd // HEADS_PER_TILE], head_rows(q_pad, hd))

    def weights(s, hd):
        s = s + wide(bias[...])
        m = jnp.max(s, axis=0, keepdims=True)
        p = jnp.exp(s - m)
        l = col_sum(p)
        lse_ref[0, hd] = m + jnp.log(l)
        return p.astype(BF), l

    def attend(pair, hd):
        p, l = pair
        lo = hd * HEAD_DIM
        attn_ref[0, lo:lo + HEAD_DIM] = dot(qkv_ref[0, 2 * D + lo:2 * D + lo + HEAD_DIM, :], p) / l

    pipeline(N_HEADS, (scores, weights, attend))

    @pl.when(step == n_steps - 1)
    def _():
        gather.sent(early + late)
        for copy in saves:
            copy.wait()
        for k in others:
            gather.g_copy(k).wait()
        gather.own_block().wait()


def to_token_major(z_t):
    return jnp.concatenate(feature_tiles(z_t), axis=1)[:, :D]


def to_feature_major(z):
    z32 = z.astype(F32)
    pad = jnp.concatenate([z32, jnp.zeros((SEQ, N_TILES * LANES - D), F32)], axis=1)
    return stack_rows([pad[:, t * LANES:(t + 1) * LANES].T for t in range(N_TILES)])[:D]


def lane_part(z):
    return z[:, :LANES] + z[:, LANES:]


def ln_grad(dn, xhat, rstd, gain):
    dxh = dn * gain
    m1 = col_mean(dxh)
    m2 = col_mean(dxh * xhat)
    return rstd * (dxh - m1 - xhat * m2)


def row_sum(acc):
    return col_sum(acc.T)


class Homeward:
    def __init__(self, cp_size, seq_loc, send, recv):
        self.cp_size, self.seq_loc, self.send, self.recv = cp_size, seq_loc, send, recv
        self.me = lax.axis_index('cp')
        self.fs = lax.axis_index('fsdp')
        self.others = range(1, cp_size)

    def enter(self):
        enter([device(lax.rem(self.me + k, self.cp_size), self.fs) for k in self.others])

    def block(self, k):
        return pl.ds(k * self.seq_loc, self.seq_loc)

    def copies(self, item, srcs, dst):
        local = pltpu.make_async_copy(srcs[0], dst, self.send.at[item, 0])
        return [local] + [remote(srcs[k], dst, self.send.at[item, k], self.recv.at[item, k], device(lax.rem(self.me + self.cp_size - k, self.cp_size), self.fs)) for k in self.others]


def ffn_kernel(n_steps, cp_size, seq_loc, tok_ref, stat_ref, attn_ref, g_ref, emb_ref, sm_ref, wout_ref, wup_ref, wdown_ref,
               out_ref, rest_ref, dres_ref, dattn_ref, dwdown_ref, dwuo_ref, dvec_ref,
               wout_n, wup_n, wout_t, wup_t, wdown_t, vec_b, bup_b, dup_s, gelu_s, acc_bup, acc_vec, out_s, out_send, out_recv):
    step = pl.program_id(0)
    home = Homeward(cp_size, seq_loc, out_send, out_recv)

    def leaving(item):
        return home.copies(item, [out_s.at[item, home.block(k)] for k in range(cp_size)], out_ref.at[home.me, item])


    @pl.when(step == 0)
    def _():
        home.enter()
        for src, nat, tr in ((wout_ref, wout_n, wout_t), (wup_ref, wup_n, wup_t)):
            joined = join_rows(src)
            nat[...] = joined
            tr[...] = joined.T
        wdown_t[...] = wdown_ref[...].T
        spread_vectors(sm_ref, range(5, 9), vec_b)
        pieces = sm_ref.shape[0]
        rows = D // pieces
        for i in range(pieces):
            sm_t = sm_ref[i].T
            for r in range(F // D):
                lo = i * (F // pieces) + r * rows
                bup_b[lo:lo + rows] = jnp.broadcast_to(sm_t[:rows, 9 + r:10 + r], (rows, LANES))
        for acc in (dwdown_ref, dwuo_ref, acc_bup, acc_vec):
            acc[...] = jnp.zeros_like(acc)

    e = dot(emb_ref[...], one_hot_rows(tok_ref[0])) * stat_ref[0, 1:2]
    o = attn_ref[0].astype(BF)
    x1 = e + dot(wout_t[...], o) + wide(vec_b[0])
    xhat2, rstd2 = normalize(x1)
    a = (xhat2 * wide(vec_b[1]) + wide(vec_b[2])).astype(BF)
    g = stack_rows([g_ref[k, 0] for k in range(g_ref.shape[0])])
    for c in range(F // D):
        rows = slice(c * D, (c + 1) * D)
        u = dot(wup_t[rows], a) + wide(bup_b[rows])
        cdf = 0.5 * (1.0 + lax.erf(u * SQRT_HALF))
        gelu = (u * cdf).astype(BF)
        gelu_s[rows] = gelu
        dup = dot(wdown_ref[rows], g, NT) * (cdf + u * (INV_SQRT_2PI * jnp.exp(-0.5 * u * u)))
        acc_bup[rows] += lane_part(dup)
        dup_s[rows] = dup.astype(BF)
        dwdown_ref[rows] += dot(gelu, g)
    out_tm = to_token_major(x1 + wide(vec_b[3]) + dot(wdown_t[...], gelu_s[...]))
    rest_ref[0] = out_tm

    @pl.when(step < EARLY_SEQS)
    def _():
        out_s[step] = out_tm
        for copy in leaving(step):
            copy.start()

    dup_b = dup_s[...]
    dwuo_ref[:, 0:F] += dot(a, dup_b, NT)
    dn2 = dot(wup_n[...], dup_b)
    g_t = to_feature_major(g)
    dres = g_t + ln_grad(dn2, xhat2, rstd2, wide(vec_b[1]))
    for j, part in enumerate((dres, dn2 * xhat2, dn2, g_t)):
        acc_vec[j] += lane_part(part)
    dres_ref[0] = dres
    dres_b = dres.astype(BF)
    dwuo_ref[:, F:F + D] += dot(o, dres_b, NT)
    dattn_ref[0] = dot(wout_n[...], dres_b)

    @pl.when(step == n_steps - 1)
    def _():
        rows = [row_sum(pad_rows(acc_vec[j])) for j in range(4)] + [row_sum(pad_rows(acc_bup[j * D:(j + 1) * D])) for j in range(F // D)]
        dvec_ref[...] = stack_rows(rows)
        for item in range(EARLY_SEQS):
            for copy in leaving(item):
                copy.wait()


def pad_rows(z):
    return stack_rows([z, jnp.zeros((N_TILES * LANES - D, LANES), F32)])


def attn_bwd_kernel(n_steps, cp_size, seq_loc, len_ref, me_ref, tok_ref, vec_ref, wqkv_ref, cos_ref, sin_ref, qkv_ref, lse_ref, attn_ref, dattn_ref, dres_ref, xhat1_ref, h_ref, stat_ref, dwdown_ref, dwuo_ref, dvec2_ref, rest_ref,
                    rdown_ref, rup_ref, rout_ref, rqkv_ref, rsmall_ref, outb_ref,
                    ruo_ref, rqa_ref, rqb_ref, out_send, out_recv, k_tm, v_tm, q_pad, do_pad, bias, dq_s, dk_s, dv_s, acc_b, acc_vec, acc_qa, acc_qb, acc_emb, *red):
    step = pl.program_id(0)
    summer = GradSum(cp_size, (dwdown_ref, dwuo_ref, acc_qa, acc_qb), (rdown_ref, ruo_ref, rqa_ref, rqb_ref), rsmall_ref, red)

    home = Homeward(cp_size, seq_loc, out_send, out_recv)
    leaving = home.copies(0, [rest_ref.at[:, home.block(k)] for k in range(cp_size)], outb_ref.at[home.me])

    @pl.when(step == 0)
    def _():
        summer.enter()
        for copy in leaving:
            copy.start()
        for i in FFN_STREAMS:
            summer.start(0, i)
        acc_qa[...] = jnp.zeros_like(acc_qa)
        acc_qb[...] = jnp.zeros_like(acc_qb)
        acc_emb[...] = jnp.zeros_like(acc_emb)
        acc_b[...] = jnp.zeros_like(acc_b)
        acc_vec[...] = jnp.zeros_like(acc_vec)
        q_pad[...] = jnp.zeros_like(q_pad)
        do_pad[...] = jnp.zeros_like(do_pad)

    for phase, at in enumerate(PHASE_STEPS):
        @pl.when(step == at)
        def _(phase=phase):
            for i in FFN_STREAMS:
                summer.finish(phase, i)
                summer.start(phase + 1, i)

    length = len_ref[lax.axis_index('cp') * n_steps + step]
    me = me_ref[0]
    vecs = vec_ref[...]
    q_pad[0:D] = qkv_ref[0, 0:D]
    do_pad[0:D] = dattn_ref[0].astype(BF)
    store_token_major(k_tm, qkv_ref[0, D:2 * D].astype(F32))
    store_token_major(v_tm, qkv_ref[0, 2 * D:3 * D].astype(F32))
    bias[...] = key_bias(me, cp_size, seq_loc, length)

    def products(hd):
        tile = hd // HEADS_PER_TILE
        return dot(k_tm[tile], head_rows(q_pad, hd)), dot(v_tm[tile], head_rows(do_pad, hd))

    def weights(pair, hd):
        s, dp = pair
        rows = slice(hd * HEAD_DIM, (hd + 1) * HEAD_DIM)
        delta = col_sum(dattn_ref[0, rows, :] * attn_ref[0, rows, :])
        p = jnp.exp((s + wide(bias[...])) - lse_ref[0, hd])
        return p.astype(BF), (p * (dp - delta)).astype(BF)

    def gradients(pair, hd):
        p, ds = pair
        rows = slice(hd * HEAD_DIM, (hd + 1) * HEAD_DIM)
        dq_s[rows, :] = dot(qkv_ref[0, D + hd * HEAD_DIM:D + (hd + 1) * HEAD_DIM, :], ds)
        dk_s[rows, :] = dot(q_pad[rows, :], ds, NT)
        dv_s[rows, :] = dot(do_pad[rows, :], p, NT)

    pipeline(N_HEADS, (products, weights, gradients))

    cos_t, sin_t = cos_ref[...], sin_ref[...]
    h = h_ref[0]
    dq = rope(dq_s[...], cos_t, -sin_t) * HEAD_DIM ** -0.5
    dk = rope(dk_s[...], cos_t, -sin_t)
    dv = dv_s[...]
    dn1 = jnp.zeros((D, SEQ), F32)
    parts = []
    for j, dz in enumerate((dq, dk, dv)):
        acc_b[j] += lane_part(dz)
        parts.append(dz.astype(BF))
    dz_b = stack_rows(parts)
    acc_qa[...] += dot(h, dz_b[:QKV_HALF], NT).reshape(acc_qa.shape)
    acc_qb[:, :, :3 * D - QKV_HALF] += dot(h, dz_b[QKV_HALF:], NT).reshape(acc_qb.shape[0], acc_qb.shape[1], 3 * D - QKV_HALF)
    dn1 = dot(wqkv_ref[...], dz_b)
    xhat1 = xhat1_ref[0]
    acc_vec[0] += lane_part(dn1 * xhat1)
    acc_vec[1] += lane_part(dn1)
    de = dres_ref[0] + ln_grad(dn1, xhat1, stat_ref[0, 0:1], col(vecs, 0))
    de = (de * stat_ref[0, 1:2]).astype(BF)
    acc_emb[...] += dot(one_hot_rows(tok_ref[0]), de, NT)

    @pl.when(step == n_steps - 1)
    def _():
        for i in QKV_STREAMS:
            summer.start(0, i)
        for i in FFN_STREAMS:
            summer.finish(3, i)
            summer.start(4, i)
        rows = [row_sum(pad_rows(acc_vec[j])) for j in range(2)] + [row_sum(pad_rows(acc_b[j])) for j in range(3)]
        small = summer.small
        small[...] = jnp.zeros_like(small)
        small[:EMB_ROWS, :D] = acc_emb[:EMB_ROWS]
        small[EMB_ROWS:EMB_ROWS + len(rows)] = stack_rows(rows)
        small[EMB_ROWS + 8:EMB_ROWS + 16] = dvec2_ref[...]
        summer.start_small(0)
        for phase in range(5):
            for i in QKV_STREAMS:
                summer.finish(phase, i)
                if phase < 4:
                    summer.start(phase + 1, i)
            summer.finish_small(phase)
            if phase < 4:
                summer.start_small(phase + 1)
        for i in FFN_STREAMS:
            summer.finish(4, i)
        rup_ref[...] = ruo_ref[:, :F]
        rout_ref[...] = ruo_ref[:, F:F + D]
        rqkv_ref[:, :QKV_HALF] = rqa_ref[...]
        rqkv_ref[:, QKV_HALF:] = rqb_ref[:, :3 * D - QKV_HALF]
        for copy in leaving:
            copy.wait()


MESH = pl.DeviceIdType.MESH
EMB_ROWS = 40
SMALL_ROWS = 64
PHASE_STEPS = (1, 4, 5)
FFN_STREAMS = (0, 1)
QKV_STREAMS = (2, 3)
STREAMS = (('xy', (0, 40, 40)), ('yx', (1, 512, 384)), ('xy', (1, 128, 128)), ('yx', (1, 128, 128)))
SMALL_SPEC = (0, SMALL_ROWS // 4, SMALL_ROWS // 4)


def neighbours(fs):
    y, x, c = place(fs)
    return fs + 1 - 2 * c, fs + 2 - 4 * x, fs + 4 - 8 * y


def place(fs):
    return fs // 4, (fs // 2) % 2, fs % 2


def device(cp, fs):
    return {'cp': cp, 'fsdp': fs}


def enter(peers):
    barrier = pltpu.get_barrier_semaphore()
    for peer in peers:
        pl.semaphore_signal(barrier, inc=1, device_id=peer, device_id_type=MESH)
    pl.semaphore_wait(barrier, len(peers))


def remote(src, dst, send_sem, recv_sem, peer):
    return pltpu.make_async_remote_copy(src_ref=src, dst_ref=dst, send_sem=send_sem, recv_sem=recv_sem, device_id=peer, device_id_type=MESH)


def piece_of(ref, spec, p):
    axis, size, stride = spec
    start = pl.multiple_of(p * stride, stride)
    return ref.at[pl.ds(start, size), :] if axis == 0 else ref.at[:, pl.ds(start, size)]


class GradSum:
    def __init__(self, cp_size, big, outs, small_out, refs):
        n = len(STREAMS)
        self.cp_size, self.big, self.outs, self.small_out = cp_size, big, outs, small_out
        self.r0, self.acc, self.r1, self.r2, self.rz, self.rg = (refs[i * n:(i + 1) * n] for i in range(6))
        self.small, self.er, self.ez, self.eg = refs[6 * n:6 * n + 4]
        sems = refs[6 * n + 4:]
        self.sends, self.recvs = sems[0:5], sems[5:10]
        self.small_send, self.small_recv = sems[10], sems[11]
        self.me = lax.axis_index('cp')
        self.fs = lax.axis_index('fsdp')
        self.y, self.x, self.c = place(self.fs)
        fs, y, x, c = self.fs, self.y, self.x, self.c
        self.cps = [lax.rem(self.me + k, cp_size) for k in range(1, cp_size)]
        self.hops = [device(self.me, f) for f in neighbours(fs)]
        self.peers = [device(z, fs) for z in self.cps]

    def enter(self):
        enter(self.hops + self.peers)

    def copies(self, phase, i):
        path, spec = STREAMS[i]
        xy = path == 'xy'
        s, v = self.sends[phase], self.recvs[phase]
        x, y, c, me = self.x, self.y, self.c, self.me
        if phase == 0:
            return [remote(self.big[i].at[2 * j + 1 - c], self.r0[i].at[j], s.at[i, j], v.at[i, j], self.hops[0]) for j in range(4)]
        if phase == 1:
            give = [2 * k + 1 - x if xy else 2 * (1 - y) + k for k in range(2)]
            return [remote(self.acc[i].at[give[k]], self.r1[i].at[k], s.at[i, k], v.at[i, k], self.hops[1 if xy else 2]) for k in range(2)]
        if phase == 2:
            return [remote(self.r1[i].at[1 - y if xy else 1 - x], self.r2[i], s.at[i, 0], v.at[i, 0], self.hops[2 if xy else 1])]
        if phase == 3:
            return [remote(piece_of(self.outs[i], spec, self.cps[k]), self.rz[i].at[k], s.at[i, k], v.at[i, k], self.peers[k]) for k in range(self.cp_size - 1)]
        return [remote(self.rg[i].at[me], self.rg[i].at[me], s.at[i, k], v.at[i, k], self.peers[k]) for k in range(self.cp_size - 1)]

    def start(self, phase, i):
        for copy in self.copies(phase, i):
            copy.start()

    def finish(self, phase, i):
        for copy in self.copies(phase, i):
            copy.wait()
        path, spec = STREAMS[i]
        xy = path == 'xy'
        big, r0, acc, r1, r2, out = self.big[i], self.r0[i], self.acc[i], self.r1[i], self.r2[i], self.outs[i]
        rz, rg = self.rz[i], self.rg[i]
        if phase == 0:
            for j in range(4):
                acc[j] = big[2 * j + self.c] + r0[j]
        elif phase == 1:
            for k in range(2):
                r1[k] = acc[2 * k + self.x if xy else 2 * self.y + k] + r1[k]
        elif phase == 2:
            out[...] = r1[self.y if xy else self.x] + r2[...]
        elif phase == 3:
            rg[self.me] = ((piece_of(out, spec, self.me)[...] + rz[0]) + rz[1]) + rz[2]
        else:
            axis, size, stride = spec
            for p in range(self.cp_size):
                lo = p * stride
                if axis == 0:
                    out[lo:lo + size, :] = rg[p]
                else:
                    out[:, lo:lo + size] = rg[p]

    def small_copies(self, phase):
        s, v = self.small_send, self.small_recv
        if phase < 3:
            return [remote(self.small, self.er.at[phase], s.at[phase], v.at[phase], self.hops[phase])]
        if phase == 3:
            return [remote(piece_of(self.small, SMALL_SPEC, self.cps[k]), self.ez.at[k], s.at[3 + k], v.at[3 + k], self.peers[k]) for k in range(self.cp_size - 1)]
        return [remote(self.eg.at[self.me], self.eg.at[self.me], s.at[6 + k], v.at[6 + k], self.peers[k]) for k in range(self.cp_size - 1)]

    def start_small(self, phase):
        for copy in self.small_copies(phase):
            copy.start()

    def finish_small(self, phase):
        for copy in self.small_copies(phase):
            copy.wait()
        if phase < 3:
            self.small[...] += self.er[phase]
        elif phase == 3:
            self.eg[self.me] = ((piece_of(self.small, SMALL_SPEC, self.me)[...] + self.ez[0]) + self.ez[1]) + self.ez[2]
        else:
            size = SMALL_SPEC[1]
            for p in range(self.cp_size):
                self.small_out[p * size:(p + 1) * size, :] = self.eg[p]


def sum_scratch(cp_size, shapes, small_shape):
    dma = pltpu.SemaphoreType.DMA
    n = len(shapes)
    cut = [((size, sh[1]) if axis == 0 else (sh[0], size)) for sh, (_, (axis, size, _)) in zip(shapes, STREAMS)]
    lanes = small_shape[1]
    scratch = [pltpu.VMEM((4,) + sh, F32) for sh in shapes] * 2 + [pltpu.VMEM((2,) + sh, F32) for sh in shapes] + [pltpu.VMEM(sh, F32) for sh in shapes]
    scratch += [pltpu.VMEM((cp_size - 1,) + sh, F32) for sh in cut] + [pltpu.VMEM((cp_size,) + sh, F32) for sh in cut]
    scratch += [pltpu.VMEM(small_shape, F32), pltpu.VMEM((3,) + small_shape, F32), pltpu.VMEM((cp_size - 1, SMALL_SPEC[1], lanes), F32), pltpu.VMEM((cp_size, SMALL_SPEC[1], lanes), F32)]
    scratch += [dma(shape) for shape in ((n, 4), (n, 2), (n, 1), (n, cp_size - 1), (n, cp_size - 1))] * 2 + [dma((3 + 2 * (cp_size - 1),))] * 2
    return scratch


def per_seq(*shape):
    return pl.BlockSpec((1,) + shape, lambda b: (b,) + (0,) * len(shape))


def whole(*shape):
    return pl.BlockSpec(shape, lambda b: (0,) * len(shape))


SMEM = pl.BlockSpec(memory_space=pltpu.SMEM)


def sds(shape, dtype):
    return jax.ShapeDtypeStruct(shape, dtype)


def call(kernel, grid, in_specs, out_specs, out_shape, scratch, flops, name, **params):
    return pl.pallas_call(
        kernel, grid=(grid,), in_specs=in_specs, out_specs=out_specs, out_shape=out_shape, scratch_shapes=scratch, name=name,
        cost_estimate=pl.CostEstimate(flops=flops, bytes_accessed=50_000_000, transcendentals=10_000_000),
        compiler_params=pltpu.CompilerParams(dimension_semantics=('arbitrary',), vmem_limit_bytes=58 * 1024 * 1024, **params))


def solution(mesh):
    cp_size = mesh.shape['cp']
    fs_size = mesh.shape['fsdp']

    def local_step(tokens, lengths, embed_table, layer_vecs, w_qkv, w_out, w_up, b_up, w_down, grad_out):
        n_loc, seq_loc = tokens.shape
        n_seq = n_loc // cp_size
        me = lax.axis_index('cp')
        fs = lax.axis_index('fsdp')

        small = stack_rows([layer_vecs, b_up.reshape(F // D, D // fs_size)])
        small = jnp.pad(small, ((0, SM_ROWS - small.shape[0]), (0, LANES - small.shape[1])))
        shards = [small, w_qkv.reshape(-1, 3 * D), w_out, w_up, w_down]
        full = [(fs_size,) + arr.shape for arr in shards]
        emb_t = jnp.pad(embed_table, ((0, VOCAB_PAD - embed_table.shape[0]), (0, 0))).T

        lane = jnp.arange(SEQ)
        positions = ((me - lane // seq_loc + cp_size) % cp_size) * seq_loc + lane % seq_loc
        inv_freq = 1.0 / (ROPE_BASE ** (jnp.arange(0, HEAD_DIM, 2, dtype=F32) / HEAD_DIM))
        angles = inv_freq[:, None] * positions.astype(F32)[None, :]
        cos_t, sin_t = jnp.cos(angles), jnp.sin(angles)
        me_arr = me.reshape(1).astype(jnp.int32)

        S = SEQ
        dma = pltpu.SemaphoreType.DMA
        vmem = pl.BlockSpec(memory_space=pltpu.VMEM)
        hbm = pl.BlockSpec(memory_space=pl.ANY)
        n_arr = len(shards)
        kept = [0] + list(range(2, n_arr))
        g_shape = (cp_size, n_seq, seq_loc, D)
        per_feature = per_seq(D, S)
        table = whole(8, S)
        tok = tokens.reshape(cp_size, n_seq, seq_loc)
        outs = call(
            functools.partial(attn_fwd_kernel, n_seq, cp_size, seq_loc, n_arr), n_seq,
            [SMEM, whole(D, VOCAB_PAD), table, table, vmem, hbm] + [vmem] * n_arr,
            [hbm] * len(kept) + [per_seq(1, S), hbm, whole(D, SM_ROWS), whole(D, 3 * D), per_feature, per_feature, per_seq(8, S), per_seq(3 * D, S), per_seq(N_HEADS, 1, S), per_feature],
            [sds(full[i], shards[i].dtype) for i in kept] + [sds((n_seq, 1, S), jnp.int32), sds(g_shape, BF), sds((D, SM_ROWS), F32), sds((D, 3 * D), BF), sds((n_seq, D, S), BF), sds((n_seq, D, S), F32), sds((n_seq, 8, S), F32), sds((n_seq, 3 * D, S), BF), sds((n_seq, N_HEADS, 1, S), F32), sds((n_seq, D, S), F32)],
            [pltpu.VMEM((3 * D, D), BF), pltpu.VMEM((N_TILES, S, LANES), BF), pltpu.VMEM((N_TILES * LANES, S), BF), pltpu.VMEM((S, LANES), F32), pltpu.VMEM((5, D, LANES), F32), pltpu.VMEM(tok.shape, jnp.int32), dma((len(kept),))] + [pltpu.VMEM(sh, arr.dtype) for sh, arr in zip(full, shards)] + [
             dma((n_arr, 7)), dma((n_arr, fs_size)), dma((cp_size,)), dma((cp_size,)), dma((cp_size,)), dma((cp_size,)), dma],
            FLOPS, 'attn_fwd', collective_id=0, has_side_effects=True,
        )(lengths, emb_t, cos_t, sin_t, tok, grad_out, *shards)
        small_p, out_p, up_p, down_p, tok_w, g_w, vecs_t, qkv_w, h, xhat1, stat, qkv, lse, attn = outs

        outs = call(
            functools.partial(ffn_kernel, n_seq, cp_size, seq_loc), n_seq,
            [per_seq(1, S), per_seq(8, S), per_feature, pl.BlockSpec((cp_size, 1, seq_loc, D), lambda b: (0, b, 0, 0)), whole(D, VOCAB_PAD), whole(*full[0]), whole(*full[2]), whole(*full[3]), whole(F, D)],
            [hbm, pl.BlockSpec((1, S, D), lambda b: (jnp.maximum(b - EARLY_SEQS, 0), 0, 0)), per_feature, per_feature, whole(F, D), whole(D, UO_PAD), whole(8, N_TILES * LANES)],
            [sds((cp_size, EARLY_SEQS, seq_loc, D), BF), sds((n_seq - EARLY_SEQS, S, D), BF), sds((n_seq, D, S), F32), sds((n_seq, D, S), F32), sds((F, D), F32), sds((D, UO_PAD), F32), sds((8, N_TILES * LANES), F32)],
            [pltpu.VMEM((D, D), BF), pltpu.VMEM((D, F), BF), pltpu.VMEM((D, D), BF), pltpu.VMEM((F, D), BF), pltpu.VMEM((D, F), BF), pltpu.VMEM((4, D, LANES), F32), pltpu.VMEM((F, LANES), F32),
             pltpu.VMEM((F, S), BF), pltpu.VMEM((F, S), BF), pltpu.VMEM((F, LANES), F32), pltpu.VMEM((4, D, LANES), F32), pltpu.VMEM((EARLY_SEQS, S, D), BF), dma((EARLY_SEQS, cp_size)), dma((EARLY_SEQS, cp_size))],
            FLOPS, 'ffn', collective_id=2, has_side_effects=True,
        )(tok_w, stat, attn, g_w, emb_t, small_p, out_p, up_p, down_p.reshape(F, D))
        out_a, out_rest, dres, dattn, dw_down, dw_uo, dvec2 = outs

        rows = D // fs_size
        shapes = [(F // fs_size, D), (rows, UO_PAD), (rows, QKV_HALF), (rows, QKV_HALF)]
        small_shape = (SMALL_ROWS, N_TILES * LANES)
        results = [shapes[0], (rows, F), (rows, D), (rows, 3 * D), small_shape]
        acc_q = pltpu.VMEM((fs_size, rows, QKV_HALF), F32)
        r_down, r_up, r_out, r_qkv, packed, out_b = call(
            functools.partial(attn_bwd_kernel, n_seq, cp_size, seq_loc), n_seq,
            [SMEM, SMEM, per_seq(1, S), whole(D, SM_ROWS), whole(D, 3 * D), table, table, per_seq(3 * D, S), per_seq(N_HEADS, 1, S), per_seq(D, S), per_seq(D, S), per_seq(D, S), per_seq(D, S), per_seq(D, S), per_seq(8, S),
             whole(fs_size, *shapes[0]), whole(fs_size, *shapes[1]), whole(8, N_TILES * LANES), hbm],
            [whole(*sh) for sh in results] + [hbm],
            [sds(sh, F32) for sh in results] + [sds((cp_size, n_seq - EARLY_SEQS, seq_loc, D), BF)],
            [pltpu.VMEM(sh, F32) for sh in shapes[1:]] + [*[dma((1, cp_size))] * 2, pltpu.VMEM((N_TILES, S, LANES), BF), pltpu.VMEM((N_TILES, S, LANES), BF), pltpu.VMEM((N_TILES * LANES, S), BF), pltpu.VMEM((N_TILES * LANES, S), BF), pltpu.VMEM((S, LANES), F32),
             *[pltpu.VMEM((D, S), F32)] * 3, pltpu.VMEM((3, D, LANES), F32), pltpu.VMEM((2, D, LANES), F32), acc_q, acc_q, pltpu.VMEM((VOCAB_PAD, D), F32)] + sum_scratch(cp_size, shapes, small_shape),
            FLOPS, 'attn_bwd', collective_id=1, has_side_effects=True,
        )(lengths, me_arr, tok_w, vecs_t, qkv_w, cos_t, sin_t, qkv, lse, attn, dattn, dres, xhat1, h, stat, dw_down.reshape(fs_size, *shapes[0]), dw_uo.reshape(fs_size, *shapes[1]), dvec2, out_rest)
        layer_out = jnp.concatenate([out_a, out_b], axis=1).reshape(grad_out.shape)

        vocab = embed_table.shape[0]
        d_vecs = stack_rows([packed[EMB_ROWS:EMB_ROWS + 5], packed[EMB_ROWS + 8:EMB_ROWS + 12]])
        d_vecs = lax.dynamic_slice_in_dim(d_vecs, fs * (D // fs_size), D // fs_size, 1)
        d_bup = packed[EMB_ROWS + 12:EMB_ROWS + 16, :D].reshape(F)
        d_bup = lax.dynamic_slice_in_dim(d_bup, fs * (F // fs_size), F // fs_size, 0)
        return (layer_out, packed[:vocab, :D], d_vecs, r_qkv.reshape(w_qkv.shape), r_out, r_up, d_bup, r_down)

    in_specs = (P('fsdp', 'cp'), P('fsdp'), P(), P(None, 'fsdp'), P('fsdp', None, None, None), P('fsdp', None), P('fsdp', None), P('fsdp'), P('fsdp', None), P('fsdp', 'cp', None))
    out_specs = (P('fsdp', 'cp', None), P(), P(None, 'fsdp'), P('fsdp', None, None, None), P('fsdp', None), P('fsdp', None), P('fsdp'), P('fsdp', None))
    return jax.shard_map(local_step, mesh=mesh, in_specs=in_specs, out_specs=out_specs, check_vma=False)
```
